256 devices in a mesh: dp: 128 (over y, x_lo, z, core), rep: 2 (over x_hi).
Axes of the slice: x: 4 (x_hi: 2, x_lo: 2; x = x_hi * 2 + x_lo), y: 4, z: 8, core: 2. Of those that a mesh axis runs over, the one named last changes fastest.
Arguments:
- gate_pre: bfloat16 [2, 16384, 5632], P(None, 'dp', 'rep'), may hold values from -8 to 8
- up_pre: bfloat16 [2, 16384, 5632], P(None, 'dp', 'rep'), may hold values from -6 to 6
- out_grad: bfloat16 [2, 16384, 1024], P(None, 'dp'), may hold values from -24 to 24
- master: float32 [1024, 5632], P('dp', 'rep'), may hold values from -0.078125 to 0.078125
- moment_one: float32 [1024, 5632], P('dp', 'rep'), may hold values from -0.02 to 0.02
- moment_two: float32 [1024, 5632], P('dp', 'rep'), may hold values from 1e-06 to 1e-05
Outputs:
- layer_out: bfloat16 [2, 16384, 1024], P(None, 'dp', 'rep')
- gate_grad: bfloat16 [2, 16384, 5632], P(None, 'dp', 'rep')
- up_grad: bfloat16 [2, 16384, 5632], P(None, 'dp', 'rep')
- master_new: float32 [1024, 5632], P('dp', 'rep')
- moment_one_new: float32 [1024, 5632], P('dp', 'rep')
- moment_two_new: float32 [1024, 5632], P('dp', 'rep')
The draws below stay inside these ranges and needn't reach their ends.
All inputs are finite; a program needn't handle non-finite values.
Results may differ from the reference program's by a relative error of at most 0.0048.
The reference program's roundings to bfloat16 on the way (of `weight_bf` and `hidden`) count: a program that leaves them out, or rounds other values in their place, can miss the bound.
Values may be sent and summed in bfloat16 or wider, within the bound.
A program may use at most 128 MiB of HBM per device.

```python
import math
import jax
import jax.numpy as jnp
from jax import lax

D = 1024
FF = 5632
MB = 2
TOKENS = 16384


def strengthened(values, stream_key, source, target, shards_of, factor):
    def block_of(axis_at):
        return (jnp.arange(values.shape[axis_at]) // (values.shape[axis_at] // shards_of)).reshape((-1,) + (1,) * (values.ndim - 1 - axis_at))

    one_side = jax.random.permutation(stream_key, shards_of)[block_of(target)]
    far = (block_of(target) + shards_of // 2) % shards_of
    return jnp.where((block_of(source) == one_side) | (block_of(source) == far), factor * values, values)


def shard_levels(rng, shape, pieces, smallest, top_value):
    level, own = 1.0, jax.random.fold_in(rng, 6)
    for axis_at, blocks in pieces:
        draws = jnp.exp(jax.random.uniform(jax.random.fold_in(own, axis_at), (blocks,), jnp.float32, smallest / len(pieces), top_value / len(pieces)))
        level = level * jnp.repeat(draws, shape[axis_at] // blocks).reshape([-1 if axis == axis_at else 1 for axis in range(len(shape))])
    return level


def centred(rng, extent, width, most, pieces=(), held_as=jnp.bfloat16):
    array = jax.random.normal(rng, extent, jnp.float32) * width
    if len(pieces) > 0:
        array = shard_levels(rng, extent, pieces, -0.22, 0.18) * array
    return jnp.clip(array, min=-most, max=most).astype(held_as)


def heavy_noise(key, shape, scale, reach, pieces, heavy, dtype=jnp.bfloat16):
    drawn = scale * jax.random.normal(key, shape, jnp.float32)
    if pieces:
        drawn = drawn * shard_levels(key, shape, pieces, -0.22, 0.18)
    return jnp.clip(strengthened(drawn, jax.random.fold_in(key, 3), *heavy), -reach, reach).astype(dtype)


def setup_inputs(seed: int = 0) -> dict:
    splits = jax.random.split(jax.random.key(seed), 7)
    gate_pre = centred(splits[0], (MB, TOKENS, FF), 1.5, 8.0, ((1, 128), (2, 2)))
    up_pre = centred(splits[1], (MB, TOKENS, FF), 1.0, 6.0, ((1, 128), (2, 2)))
    out_grad = heavy_noise(splits[2], (MB, TOKENS, D), 1.0, 24.0, ((1, 128),), (1, 2, 128, 5.5))
    master = centred(splits[3], (D, FF), FF ** -0.5, 0.078125, ((0, 128), (1, 2)), jnp.float32)
    moment_one = centred(splits[4], (D, FF), 0.003, 0.02, ((0, 128), (1, 2)), jnp.float32)
    moment_two = jnp.clip(jnp.exp(math.log(9.999999747378752e-06) - 2.3025851 * jax.random.uniform(splits[5], (D, FF), jnp.float32) ** shard_levels(splits[5], (D, FF), ((0, 128), (1, 2)), -0.2, 0.2)), 9.999999974752427e-07, 9.999999747378752e-06)
    return {"gate_pre": gate_pre, "up_pre": up_pre, "out_grad": out_grad, "master": master, "moment_one": moment_one, "moment_two": moment_two}


first_power = 2.6561398887587544e-05
second_power = 0.005920529220333997

def reference(gate_pre, up_pre, out_grad, master, moment_one, moment_two):
    weight_bf = master.astype(jnp.bfloat16)
    outs_list = []
    gate_list = []
    up_list = []
    grad_sum = jnp.zeros(master.shape, jnp.float32)
    for index in range(MB):
        gate = gate_pre[index].astype(jnp.float32)
        up_val = up_pre[index].astype(jnp.float32)
        sig = jax.nn.sigmoid(gate)
        hidden = (gate * sig * up_val).astype(jnp.bfloat16)
        result = lax.dot_general(hidden, weight_bf, (((1,), (1,)), ((), ())), preferred_element_type=jnp.float32)
        outs_list.append(result.astype(jnp.bfloat16))
        hid_grad = jnp.dot(out_grad[index], weight_bf, preferred_element_type=jnp.float32)
        gate_list.append((hid_grad * up_val * sig * (1.0 + gate * (1.0 - sig))).astype(jnp.bfloat16))
        up_list.append((hid_grad * gate * sig).astype(jnp.bfloat16))
        grad_sum = grad_sum + lax.dot_general(out_grad[index], hidden, (((0,), (0,)), ((), ())), preferred_element_type=jnp.float32)
    main_grad = grad_sum / jnp.float32(MB * TOKENS)
    first = 0.9 * moment_one + 0.1 * main_grad
    second = 0.95 * moment_two + 0.05 * main_grad * main_grad
    update = first / (1.0 - first_power) / (jnp.sqrt(second / (1.0 - second_power)) + 1e-08)
    master_new = master - 0.003 * (update + 0.1 * master)
    return (jnp.stack(outs_list), jnp.stack(gate_list), jnp.stack(up_list), master_new, first, second)
```

```python
import jax
import jax.numpy as jnp
from jax import lax
from jax.experimental import pallas as pl
from jax.experimental.pallas import tpu as pltpu
from jax.sharding import Mesh
from jax.sharding import PartitionSpec as P

DP = ("dp_0", "dp_1", "dp_2", "dp_3")
NY, NX, NZ, NC = 4, 2, 8, 2

first_power = 2.6561398887587544e-05
second_power = 0.005920529220333997

F32 = jnp.float32
BF = jnp.bfloat16
D = 1024
FF = 2816
HALF = 1408
TOK = 256
A = (0, 512)
B = (512, 512)
C = (1024, 384)
BC = (512, 896)


def cols(r):
    return pl.ds(r[0], r[1])


def kernel(
    gate_ref, up_ref, og_ref, master_ref, one_ref, two_ref,
    out_ref, gg_ref, ug_ref, master_out, one_out, two_out,
    W, G, hid2, hidO, ogP, ogT, mP, hg, acc, fin, finP, lo_s, lo_r,
    sa1, ra1, sa2, ra2, sa3, ra3, sa4, ra4,
    sb1, rb1, sb2, rb2, sb3, rb3, sb4, rb4,
    sc1, rc1, sc2, rc2, sc3, rc3, sc4, rc4,
    ssem, rsem,
):
    y = lax.axis_index("dp_0")
    x = lax.axis_index("dp_1")
    z = lax.axis_index("dp_2")
    c = lax.axis_index("dp_3")
    r = lax.axis_index("rep")
    oc = 1 - c
    ox = 1 - x

    def dy(o):
        return {"dp_0": lax.rem(y + (o % NY), NY)}

    def dz(o):
        return {"dp_2": lax.rem(z + (o % NZ), NZ)}

    def zz(o):
        return lax.rem(z + (o % NZ), NZ)

    def yy(o):
        return lax.rem(y + (o % NY), NY)

    dx = {"dp_1": ox}
    dc = {"dp_3": oc}
    dr = {"rep": 1 - r}

    peers = [dc, dx, dr] + [dy(o) for o in range(1, NY)] + [dz(o) for o in range(1, NZ)]
    bar = pltpu.get_barrier_semaphore()
    for p in peers:
        pl.semaphore_signal(bar, inc=1, device_id=p, device_id_type=pl.DeviceIdType.MESH)
    pl.semaphore_wait(bar, len(peers))

    sent = []
    slots = {}

    def slot(name):
        if name not in slots:
            slots[name] = len(slots)
        return slots[name]

    def rc(name, src, dst, dev):
        k = slot(name)
        return pltpu.make_async_remote_copy(
            src_ref=src, dst_ref=dst, send_sem=ssem.at[k], recv_sem=rsem.at[k],
            device_id=dev, device_id_type=pl.DeviceIdType.MESH,
        )

    def send(name, src, dst, dev):
        d = rc(name, src, dst, dev)
        d.start()
        sent.append(d)

    def recv(name, dst, dev):
        rc(name, dst, dst, dev).wait_recv()

    def hidden_rows(half, out, out_base):
        off = pl.multiple_of(half * HALF, 128)

        def body(i, _):
            rows = pl.ds(pl.multiple_of(i * 16, 16), 16)
            g = gate_ref[rows, pl.ds(off, HALF)].astype(F32)
            u = up_ref[rows, pl.ds(off, HALF)].astype(F32)
            s = jax.nn.sigmoid(g)
            out[pl.ds(pl.multiple_of(out_base + i * 16, 16), 16), :] = (g * s * u).astype(BF)
            return 0

        lax.fori_loop(0, TOK // 16, body, 0)

    send("m", master_ref.at[:, pl.ds(pl.multiple_of(oc * HALF, 128), HALF)], mP, dc)
    send("og", og_ref, ogP, dc)

    recv("m", mP, dc)
    mine = master_ref[:, pl.ds(pl.multiple_of(c * HALF, 128), HALF)]
    theirs = mP[...]
    first_core = c == 0
    W[c, y, x, z] = jnp.concatenate(
        [jnp.where(first_core, mine, theirs), jnp.where(first_core, theirs, mine)], axis=0
    ).astype(BF)

    def Wb(*idx):
        return W.at[(c,) + idx]

    send("Ax", Wb(y, x, z, slice(None), cols(A)), Wb(y, x, z, slice(None), cols(A)), dx)
    for o in (4, 3, 5, 2, 6, 1, 7):
        ref = Wb(y, x, z, slice(None), cols(BC))
        send(f"Zd{o}", ref, ref, dz(o))

    hidden_rows(oc, hidO, 0)
    send("h", hidO, hid2.at[pl.ds(TOK, TOK)], dc)
    hidden_rows(c, hid2, 0)
    for b in range(4):
        ogT[b, :, 0:TOK] = og_ref[:, b * 256 : (b + 1) * 256].T

    allr = slice(None)

    def A1():
        recv("Ax", Wb(y, ox, z, allr, cols(A)), dx)
        ref = Wb(y, allr, z, allr, cols(A))
        for o in (2, 1, 3):
            send(f"Ay{o}", ref, ref, dy(o))

    def A2():
        for o in (1, 3, 2):
            recv(f"Ay{o}", Wb(yy(-o), allr, z, allr, cols(A)), dy(-o))
        ref = Wb(allr, allr, z, allr, cols(A))
        send("Az1R", ref, ref, dz(1))
        send("Az1L", ref, ref, dz(-1))

    def A3(step):
        ref = Wb(allr, allr, zz(-step), allr, cols(A))
        recv(f"Az{step}R", ref, dz(-1))
        if step < 3:
            send(f"Az{step + 1}R", ref, ref, dz(1))
        else:
            h = Wb(pl.ds(0, 2), allr, zz(-3), allr, cols(A))
            send("Az4R", h, h, dz(1))
        ref = Wb(allr, allr, zz(step), allr, cols(A))
        recv(f"Az{step}L", ref, dz(1))
        if step < 3:
            send(f"Az{step + 1}L", ref, ref, dz(-1))
        else:
            h = Wb(pl.ds(2, 2), allr, zz(3), allr, cols(A))
            send("Az4L", h, h, dz(-1))

    def A6():
        recv("Az4R", Wb(pl.ds(0, 2), allr, zz(4), allr, cols(A)), dz(-1))
        recv("Az4L", Wb(pl.ds(2, 2), allr, zz(4), allr, cols(A)), dz(1))
        ref = Wb(allr, allr, allr, allr, cols(A))
        send("DA", ref, ref, dc)

    def BC1():
        for o in (1, 7, 2, 6, 3, 5, 4):
            recv(f"Zd{o}", Wb(y, x, zz(-o), allr, cols(BC)), dz(-o))
        ref = Wb(y, x, allr, allr, cols(B))
        send("Bx", ref, ref, dx)
        ref = Wb(y, x, allr, allr, cols(C))
        send("Cy1R", ref, ref, dy(1))
        send("Cy1L", ref, ref, dy(-1))

    def B2():
        recv("Bx", Wb(y, ox, allr, allr, cols(B)), dx)
        ref = Wb(y, allr, allr, allr, cols(B))
        send("By1R", ref, ref, dy(1))
        send("By1L", ref, ref, dy(-1))

    def B3():
        recv("By1R", Wb(yy(-1), allr, allr, allr, cols(B)), dy(-1))
        ref = Wb(yy(-1), 0, allr, allr, cols(B))
        send("By2R", ref, ref, dy(1))
        recv("By1L", Wb(yy(1), allr, allr, allr, cols(B)), dy(1))
        ref = Wb(yy(1), 1, allr, allr, cols(B))
        send("By2L", ref, ref, dy(-1))

    def B4():
        recv("By2R", Wb(yy(2), 0, allr, allr, cols(B)), dy(-1))
        recv("By2L", Wb(yy(2), 1, allr, allr, cols(B)), dy(1))
        ref = Wb(allr, allr, allr, allr, cols(B))
        send("DB", ref, ref, dc)

    def C2():
        recv("Cy1R", Wb(yy(-1), x, allr, allr, cols(C)), dy(-1))
        ref = Wb(yy(-1), x, pl.ds(0, 4), allr, cols(C))
        send("Cy2R", ref, ref, dy(1))
        recv("Cy1L", Wb(yy(1), x, allr, allr, cols(C)), dy(1))
        ref = Wb(yy(1), x, pl.ds(4, 4), allr, cols(C))
        send("Cy2L", ref, ref, dy(-1))

    def C3():
        recv("Cy2R", Wb(yy(2), x, pl.ds(0, 4), allr, cols(C)), dy(-1))
        recv("Cy2L", Wb(yy(2), x, pl.ds(4, 4), allr, cols(C)), dy(1))
        ref = Wb(allr, x, allr, allr, cols(C))
        send("Cx", ref, ref, dx)

    def C4():
        recv("Cx", Wb(allr, ox, allr, allr, cols(C)), dx)
        ref = Wb(allr, allr, allr, allr, cols(C))
        send("DC", ref, ref, dc)

    def grads(cr):
        def body(b, _):
            p = jnp.dot(ogT[b], hid2[:, cols(cr)], preferred_element_type=F32)
            G[b, :, :, :, cols(cr)] = p.reshape(NX, NZ, 16, cr[1])
            return 0

        lax.fori_loop(0, NY, body, 0)

    def RA1():
        def body(i, _):
            sa1[i] = G[i, :, zz(4), :, cols(A)].astype(BF)
            return 0

        lax.fori_loop(0, NY, body, 0)
        send("rA1R", sa1.at[pl.ds(0, 2)], ra1.at[0], dz(1))
        send("rA1L", sa1.at[pl.ds(2, 2)], ra1.at[1], dz(-1))

    def RA(step):
        d = 5 - step
        for side, o in ((0, d), (1, -d)):
            name = "RL"[side]
            zi = zz(o)
            dst = sa2.at[side, step - 2]
            if step == 2:
                recv(f"rA1{name}", ra1.at[side], dz(-1 if side == 0 else 1))
                base = 2 * side

                def with_recv(i, _):
                    dst[base + i] = (
                        G[base + i, :, zi, :, cols(A)] + ra1[side, i].astype(F32)
                    ).astype(BF)
                    return 0

                def without(i, _):
                    dst[2 - base + i] = G[2 - base + i, :, zi, :, cols(A)].astype(BF)
                    return 0

                lax.fori_loop(0, 2, without, 0)
                lax.fori_loop(0, 2, with_recv, 0)
            else:
                recv(f"rA{step - 1}{name}", ra2.at[side, step - 3], dz(-1 if side == 0 else 1))

                def full(i, _):
                    dst[i] = (
                        G[i, :, zi, :, cols(A)] + ra2[side, step - 3, i].astype(F32)
                    ).astype(BF)
                    return 0

                lax.fori_loop(0, NY, full, 0)
            send(f"rA{step}{name}", dst, ra2.at[side, step - 2], dz(1 if side == 0 else -1))

    def RA5():
        recv("rA4R", ra2.at[0, 2], dz(-1))
        recv("rA4L", ra2.at[1, 2], dz(1))

        def body(i, _):
            t = G[i, :, z, :, cols(A)] + ra2[0, 2, i].astype(F32) + ra2[1, 2, i].astype(F32)
            G[i, :, z, :, cols(A)] = t
            sa3[i] = t.astype(BF)
            return 0

        lax.fori_loop(0, NY, body, 0)
        for o in (2, 1, 3):
            send(f"rAy{o}", sa3.at[yy(o)], ra3.at[o - 1], dy(o))

    def RA6():
        for o in (1, 3, 2):
            recv(f"rAy{o}", ra3.at[o - 1], dy(-o))
        t = G[y, :, z, :, cols(A)]
        for o in (1, 2, 3):
            t = t + ra3[o - 1].astype(F32)
        G[y, :, z, :, cols(A)] = t
        sa4[...] = t.astype(BF)
        send("rAx", sa4.at[ox], ra4, dx)

    def RA7():
        recv("rAx", ra4, dx)
        fin[:, cols(A)] = G[y, x, z, :, cols(A)] + ra4[...].astype(F32)

    def RB1():
        def body(i, _):
            sb1[i] = G[yy(2), i, :, :, cols(B)].astype(BF)
            return 0

        lax.fori_loop(0, NX, body, 0)
        send("rB1R", sb1.at[0], rb1.at[0], dy(1))
        send("rB1L", sb1.at[1], rb1.at[1], dy(-1))

    def RB2():
        for side, o in ((0, 1), (1, -1)):
            name = "RL"[side]
            yi = yy(o)
            sb2[side, 1 - side] = G[yi, 1 - side, :, :, cols(B)].astype(BF)
            recv(f"rB1{name}", rb1.at[side], dy(-o))
            sb2[side, side] = (G[yi, side, :, :, cols(B)] + rb1[side].astype(F32)).astype(BF)
            send(f"rB2{name}", sb2.at[side], rb2.at[side], dy(o))

    def RB3():
        recv("rB2R", rb2.at[0], dy(-1))
        recv("rB2L", rb2.at[1], dy(1))
        sb3[...] = (
            G[y, ox, :, :, cols(B)] + rb2[0, ox].astype(F32) + rb2[1, ox].astype(F32)
        ).astype(BF)
        send("rBx", sb3, rb3, dx)
        G[y, x, :, :, cols(B)] = (
            G[y, x, :, :, cols(B)] + rb2[0, x].astype(F32) + rb2[1, x].astype(F32)
        )

    def RB4():
        recv("rBx", rb3, dx)
        t = G[y, x, :, :, cols(B)] + rb3[...].astype(F32)
        G[y, x, :, :, cols(B)] = t
        sb4[...] = t.astype(BF)
        for o in (4, 3, 5, 2, 6, 1, 7):
            send(f"rBz{o}", sb4.at[zz(o)], rb4.at[o - 1], dz(o))

    def RB5():
        t = G[y, x, z, :, cols(B)]
        for o in range(1, NZ):
            recv(f"rBz{o}", rb4.at[o - 1], dz(-o))
        for o in range(1, NZ):
            t = t + rb4[o - 1].astype(F32)
        fin[:, cols(B)] = t

    def RC1():
        def body(i, _):
            sc1[i] = G[i, ox, :, :, cols(C)].astype(BF)
            return 0

        lax.fori_loop(0, NY, body, 0)
        send("rCx", sc1, rc1, dx)

    def RC2():
        recv("rCx", rc1, dx)

        def body(i, _):
            G[i, x, :, :, cols(C)] = G[i, x, :, :, cols(C)] + rc1[i].astype(F32)
            return 0

        lax.fori_loop(0, NY, body, 0)
        sc2[...] = G[yy(2), x, :, :, cols(C)].astype(BF)
        send("rCy1R", sc2.at[pl.ds(0, 4)], rc2.at[0], dy(1))
        send("rCy1L", sc2.at[pl.ds(4, 4)], rc2.at[1], dy(-1))

    def RC3():
        for side, o in ((0, 1), (1, -1)):
            name = "RL"[side]
            yi = yy(o)
            w, n = 4 * side, 4 - 4 * side
            sc3[side, n : n + 4] = G[yi, x, n : n + 4, :, cols(C)].astype(BF)
            recv(f"rCy1{name}", rc2.at[side], dy(-o))
            sc3[side, w : w + 4] = (
                G[yi, x, w : w + 4, :, cols(C)] + rc2[side].astype(F32)
            ).astype(BF)
            send(f"rCy2{name}", sc3.at[side], rc3.at[side], dy(o))

    def RC4():
        recv("rCy2R", rc3.at[0], dy(-1))
        recv("rCy2L", rc3.at[1], dy(1))
        t = G[y, x, :, :, cols(C)] + rc3[0].astype(F32) + rc3[1].astype(F32)
        G[y, x, :, :, cols(C)] = t
        sc4[...] = t.astype(BF)
        for o in (4, 3, 5, 2, 6, 1, 7):
            send(f"rCz{o}", sc4.at[zz(o)], rc4.at[o - 1], dz(o))

    def RC5():
        t = G[y, x, z, :, cols(C)]
        for o in range(1, NZ):
            recv(f"rCz{o}", rc4.at[o - 1], dz(-o))
        for o in range(1, NZ):
            t = t + rc4[o - 1].astype(F32)
        fin[:, cols(C)] = t

    def forward(half, cr, hid, first):
        n = cr[1]
        w = W[half, :, :, :, :, cols(cr)].reshape(D, n)
        part = lax.dot_general(
            hid[0:TOK, cols(cr)], w, (((1,), (1,)), ((), ())), preferred_element_type=F32
        )
        if first:
            acc[...] = part
        else:
            acc[...] += part
        hg[:, 0:n] = jnp.dot(og_ref[...], w, preferred_element_type=F32)
        off = pl.multiple_of(half * HALF + cr[0], 128)

        def body(i, _):
            rows = pl.ds(pl.multiple_of(i * 16, 16), 16)
            g = gate_ref[rows, pl.ds(off, n)].astype(F32)
            u = up_ref[rows, pl.ds(off, n)].astype(F32)
            h = hg[rows, 0:n]
            s = jax.nn.sigmoid(g)
            gg_ref[rows, pl.ds(off, n)] = (h * u * s * (1.0 + g * (1.0 - s))).astype(BF)
            ug_ref[rows, pl.ds(off, n)] = (h * g * s).astype(BF)
            return 0

        lax.fori_loop(0, TOK // 16, body, 0)

    A1()
    recv("og", ogP, dc)
    for b in range(4):
        ogT[b, :, TOK : 2 * TOK] = ogP[:, b * 256 : (b + 1) * 256].T
    recv("h", hid2.at[pl.ds(TOK, TOK)], dc)
    grads(C)
    RC1()
    BC1()
    grads(B)
    RB1()
    A2()
    grads(A)
    RA1()
    B2()
    C2()
    A3(1)
    RB2()
    RA(2)
    C3()
    A3(2)
    B3()
    RA(3)
    RC2()
    A3(3)
    B4()
    RB3()
    RA(4)
    C4()
    RC3()
    A6()
    RB4()
    RA5()
    forward(c, B, hid2, True)
    RC4()
    RA6()
    forward(c, C, hid2, False)
    forward(c, A, hid2, False)
    RA7()
    recv("DB", W.at[oc, :, :, :, :, cols(B)], dc)
    forward(oc, B, hidO, False)
    recv("DC", W.at[oc, :, :, :, :, cols(C)], dc)
    forward(oc, C, hidO, False)
    recv("DA", W.at[oc, :, :, :, :, cols(A)], dc)
    forward(oc, A, hidO, False)
    lo_s[...] = acc[:, pl.ds(pl.multiple_of((1 - r) * 512, 128), 512)].astype(BF)
    send("lo", lo_s, lo_r, dr)
    RB5()
    RC5()
    send("fin", fin.at[pl.ds(pl.multiple_of(oc * 8, 8), 8)], finP, dc)

    def adam(half, g):
        cs = pl.ds(pl.multiple_of(half * HALF, 128), HALF)
        g = g / jnp.float32(32768)
        m = master_ref[:, cs]
        first = 0.9 * one_ref[:, cs] + 0.1 * g
        second = 0.95 * two_ref[:, cs] + 0.05 * g * g
        update = first / (1.0 - first_power) / (jnp.sqrt(second / (1.0 - second_power)) + 1e-08)
        master_out[:, cs] = m - 0.003 * (update + 0.1 * m)
        one_out[:, cs] = first
        two_out[:, cs] = second

    adam(c, fin[pl.ds(pl.multiple_of(c * 8, 8), 8), :])
    recv("fin", finP, dc)
    adam(oc, finP[...])
    recv("lo", lo_r, dr)
    out_ref[...] = (
        acc[:, pl.ds(pl.multiple_of(r * 512, 128), 512)] + lo_r[...].astype(F32)
    ).astype(BF)
    for d in sent:
        d.wait_send()
    assert len(slots) <= NSEM, len(slots)


NSEM = 80


def on_device(gate_pre, up_pre, out_grad, master, moment_one, moment_two):
    V = pltpu.VMEM
    nA, nB, nC = A[1], B[1], C[1]
    outs = pl.pallas_call(
        kernel,
        out_shape=(
            jax.ShapeDtypeStruct((TOK, 512), BF),
            jax.ShapeDtypeStruct((TOK, FF), BF),
            jax.ShapeDtypeStruct((TOK, FF), BF),
            jax.ShapeDtypeStruct((8, FF), F32),
            jax.ShapeDtypeStruct((8, FF), F32),
            jax.ShapeDtypeStruct((8, FF), F32),
        ),
        in_specs=[pl.BlockSpec(memory_space=V)] * 6,
        out_specs=[pl.BlockSpec(memory_space=V)] * 6,
        scratch_shapes=[
            V((NC, NY, NX, NZ, 16, HALF), BF),
            V((NY, NX, NZ, 16, HALF), F32),
            V((2 * TOK, HALF), BF),
            V((TOK, HALF), BF),
            V((TOK, D), BF),
            V((4, 256, 2 * TOK), BF),
            V((8, HALF), F32),
            V((TOK, 512), F32),
            V((TOK, D), F32),
            V((16, HALF), F32),
            V((8, HALF), F32),
            V((TOK, 512), BF),
            V((TOK, 512), BF),
            V((NY, NX, 16, nA), BF), V((2, 2, NX, 16, nA), BF),
            V((2, 3, NY, NX, 16, nA), BF), V((2, 3, NY, NX, 16, nA), BF),
            V((NY, NX, 16, nA), BF), V((3, NX, 16, nA), BF),
            V((NX, 16, nA), BF), V((16, nA), BF),
            V((NX, NZ, 16, nB), BF), V((2, NZ, 16, nB), BF),
            V((2, NX, NZ, 16, nB), BF), V((2, NX, NZ, 16, nB), BF),
            V((NZ, 16, nB), BF), V((NZ, 16, nB), BF),
            V((NZ, 16, nB), BF), V((7, 16, nB), BF),
            V((NY, NZ, 16, nC), BF), V((NY, NZ, 16, nC), BF),
            V((NZ, 16, nC), BF), V((2, 4, 16, nC), BF),
            V((2, NZ, 16, nC), BF), V((2, NZ, 16, nC), BF),
            V((NZ, 16, nC), BF), V((7, 16, nC), BF),
            pltpu.SemaphoreType.DMA((NSEM,)),
            pltpu.SemaphoreType.DMA((NSEM,)),
        ],
        compiler_params=pltpu.CompilerParams(
            collective_id=0, has_side_effects=True, vmem_limit_bytes=66_000_000
        ),
    )(
        gate_pre.reshape(TOK, FF),
        up_pre.reshape(TOK, FF),
        out_grad.reshape(TOK, D),
        master,
        moment_one,
        moment_two,
    )
    lo, gg, ug, mn, m1, m2 = outs
    return (
        lo.reshape(2, 128, 512),
        gg.reshape(2, 128, FF),
        ug.reshape(2, 128, FF),
        mn,
        m1,
        m2,
    )


def solution(mesh):
    torus = Mesh(
        mesh.devices.reshape(NY, NX, NZ, NC, mesh.shape["rep"]),
        ("dp_0", "dp_1", "dp_2", "dp_3", "rep"),
    )
    return jax.shard_map(
        on_device,
        mesh=torus,
        in_specs=(
            P(None, DP, "rep"),
            P(None, DP, "rep"),
            P(None, DP, None),
            P(DP, "rep"),
            P(DP, "rep"),
            P(DP, "rep"),
        ),
        out_specs=(
            P(None, DP, "rep"),
            P(None, DP, "rep"),
            P(None, DP, "rep"),
            P(DP, "rep"),
            P(DP, "rep"),
            P(DP, "rep"),
        ),
        check_vma=False,
    )
```

```python
import jax
import jax.numpy as jnp
from jax import lax
from jax.experimental import pallas as pl
from jax.experimental.pallas import tpu as pltpu
from jax.sharding import Mesh
from jax.sharding import PartitionSpec as P

DP = ("dp_0", "dp_1", "dp_2", "dp_3")
NY, NX, NZ, NC = 4, 2, 8, 2

first_power = 2.6561398887587544e-05
second_power = 0.005920529220333997

F32 = jnp.float32
BF = jnp.bfloat16
D = 1024
FF = 2816
HALF = 1408
TOK = 256
A = (0, 512)
B = (512, 512)
C = (1024, 384)
BC = (512, 896)


def cols(r):
    return pl.ds(r[0], r[1])


class Names:
    def __getattr__(self, word):
        return word


K = Names()

ORDER = (
    K.init, K.A1, K.gp, K.gB, K.RB1, K.gC, K.RC1, K.gA, K.RA1, K.A2, K.RB2L, K.BC1, K.RC2,
    K.RA2R0, K.RA2L1, K.RA3R1, K.RA3L0, K.RC2b, K.RB2R, K.A3_1R0, K.A3_1L0, K.RC2c, K.C2R,
    K.A3_1R1, K.A3_1L1, K.RB3, K.RA3L1, K.RA3R0, K.B3R, K.RA4R1, K.RA4L0, K.RC3R, K.A3_2L0,
    K.A3_2R0, K.B2, K.C2L, K.A3_2R1, K.A3_2L1, K.RC3L, K.RA4L1, K.RA4R0, K.A3_3R0, K.B3L, K.C3,
    K.A3_3L1, K.RB4, K.RC4, K.RA5, K.A6, K.hg_cA, K.B4, K.lo_cB, K.C4, K.lo_cA, K.lo_cC,
    K.lo_oA, K.lo_oB, K.RA6, K.lo_oC, K.losend, K.hg_oB, K.hg_oC, K.hg_cB, K.RA7, K.RB5,
    K.hg_oA, K.hg_cC, K.RC5, K.fin_, K.adam, K.lofin,
)
ORDS = {
    K.init: (K.Zd7, K.Zd3, K.h, K.Zd6, K.Zd5, K.Zd1, K.Zd4, K.Zd2, K.Ax, K.og,),
    K.A1: (K.Ay2, K.Ay3, K.Ay1,),
    K.A2: (K.DA0, K.Az1L0, K.Az1R0, K.Az1R1, K.Az1L1,),
    K.A3_1R0: (K.Az2R0, K.DA1R0,),
    K.A3_1R1: (K.DA1R1, K.Az2R1,),
    K.A3_1L0: (K.Az2L0, K.DA1L0,),
    K.A3_1L1: (K.Az2L1, K.DA1L1,),
    K.A3_2R0: (K.DA2R0, K.Az3R0,),
    K.A3_2R1: (K.DA2R1, K.Az3R1,),
    K.A3_2L0: (K.DA2L0, K.Az3L0,),
    K.A3_2L1: (K.Az3L1, K.DA2L1,),
    K.A3_3R0: (K.Az4R0, K.DA3R0,),
    K.A3_3L1: (K.DA3L1, K.Az4L1,),
    K.BC1: (K.DB0, K.By1Lx, K.Cy1L, K.Bx, K.Cy1R, K.DC0, K.By1Rx, K.Cx0,),
    K.B2: (K.DB1, K.By1Ro, K.By1Lo,),
    K.B3R: (K.DB2, K.By2R,),
    K.B3L: (K.DB3, K.By2L,),
    K.C2R: (K.Cy2R, K.DC3, K.Cx3,),
    K.C2L: (K.DC1, K.Cx1, K.Cy2L,),
    K.C3: (K.Cx2, K.DC2,),
    K.RC1: (K.rCx2, K.rCx1, K.rCx3, K.rCx0,),
    K.RB1: (K.rB1L, K.rB2L1, K.rB2R1, K.rB1R,),
    K.RA1: (K.rA1L1, K.rA2L0, K.rA1R0, K.rA2R1,),
    K.RA5: (K.rAy2, K.rAy1, K.rAy3,),
    K.RB4: (K.rBz2, K.rBz7, K.rBz3, K.rBz6, K.rBz4, K.rBz1, K.rBz5,),
    K.RC2: (K.rCy1R, K.rCy1L,),
    K.RC4: (K.rCz7, K.rCz5, K.rCz4, K.rCz2, K.rCz3, K.rCz6, K.rCz1,),
}


def kernel(
    gate_hbm, up_hbm, og_hbm, master_hbm, one_hbm, two_hbm,
    out_hbm, gg_hbm, ug_hbm, master_out_hbm, one_out_hbm, two_out_hbm,
    gate_ref, up_ref, og_ref, master_ref, one_ref, two_ref,
    out_ref, gg_ref, ug_ref, master_out, one_out, two_out,
    W, G, hid2, hidO, ogP, ogT, mP, hg, acc, fin, finP, lo_s, lo_r,
    sa1, ra1, sa2, ra2, sa3, ra3, sa4, ra4,
    sb1, rb1, sb2, rb2, sb3, rb3, sb4, rb4,
    sc1, rc1, sc2, rc2, sc3, rc3, sc4, rc4,
    ssem, rsem, lsem,
):
    y = lax.axis_index(K.dp_0)
    x = lax.axis_index(K.dp_1)
    z = lax.axis_index(K.dp_2)
    c = lax.axis_index(K.dp_3)
    r = lax.axis_index(K.rep)
    oc = 1 - c
    ox = 1 - x

    def dy(o):
        return {K.dp_0: lax.rem(y + (o % NY), NY)}

    def dz(o):
        return {K.dp_2: lax.rem(z + (o % NZ), NZ)}

    def zz(o):
        return lax.rem(z + (o % NZ), NZ)

    def yy(o):
        return lax.rem(y + (o % NY), NY)

    dx = {K.dp_1: ox}
    dc = {K.dp_3: oc}
    dr = {K.rep: 1 - r}
    allr = slice(None)

    peers = [dc, dx, dr] + [dy(o) for o in range(1, NY)] + [dz(o) for o in range(1, NZ)]
    bar = pltpu.get_barrier_semaphore()
    for p in peers:
        pl.semaphore_signal(bar, inc=1, device_id=p, device_id_type=pl.DeviceIdType.MESH)

    loc = {}

    def local(name, src, dst):
        d = pltpu.make_async_copy(src, dst, lsem.at[len(loc)])
        d.start()
        loc[name] = d

    local(K.gate, gate_hbm, gate_ref)
    local(K.up, up_hbm, up_ref)
    local(K.og, og_hbm, og_ref)
    local(K.master, master_hbm, master_ref)
    local(K.one, one_hbm, one_ref)
    local(K.two, two_hbm, two_ref)

    sent = []
    slots = {}

    def slot(name):
        if name not in slots:
            slots[name] = len(slots)
        return slots[name]

    def rc(name, src, dst, dev):
        k = slot(name)
        return pltpu.make_async_remote_copy(
            src_ref=src, dst_ref=dst, send_sem=ssem.at[k], recv_sem=rsem.at[k],
            device_id=dev, device_id_type=pl.DeviceIdType.MESH,
        )

    def sends(step, items):
        names = ORDS.get(step, tuple(i[0] for i in items))
        table = {i[0]: i for i in items}
        for n in names:
            table[n]
        for name in list(names) + [n for n in table if n not in names]:
            _, src, dst, dev = table[name]
            d = rc(name, src, dst, dev)
            d.start()
            sent.append(d)

    def recv(name, dst, dev):
        with jax.named_scope(K.wait_ + name):
            rc(name, dst, dst, dev).wait_recv()

    def hidden_rows(half, out):
        off = pl.multiple_of(half * HALF, 128)

        def body(i, _):
            rows = pl.ds(pl.multiple_of(i * 16, 16), 16)
            g = gate_ref[rows, pl.ds(off, HALF)].astype(F32)
            u = up_ref[rows, pl.ds(off, HALF)].astype(F32)
            s = jax.nn.sigmoid(g)
            out[rows, :] = (g * s * u).astype(BF)
            return 0

        lax.fori_loop(0, TOK // 16, body, 0)

    def Wb(*idx):
        return W.at[(c,) + idx]

    def same(name, ref, dev):
        return (name, ref, ref, dev)

    S = {}

    def step(f):
        S[f.__name__] = f
        return f

    @step
    def init():
        sends(K.i0, [(K.m, master_ref.at[:, pl.ds(pl.multiple_of(oc * HALF, 128), HALF)], mP, dc)])
        recv(K.m, mP, dc)
        mine = master_ref[:, pl.ds(pl.multiple_of(c * HALF, 128), HALF)]
        theirs = mP[...]
        first_core = c == 0
        W[c, y, x, z] = jnp.concatenate(
            [jnp.where(first_core, mine, theirs), jnp.where(first_core, theirs, mine)], axis=0
        ).astype(BF)
        items = [
            (K.og, og_ref, ogP, dc),
            (K.h, hidO, hid2.at[pl.ds(TOK, TOK)], dc),
            same(K.Ax, Wb(y, x, z, allr, cols(A)), dx),
        ]
        for o in (4, 3, 5, 2, 6, 1, 7):
            items.append(same(f"Zd{o}", Wb(y, x, z, allr, cols(BC)), dz(o)))
        sends(K.init, items)

    @step
    def A1():
        recv(K.Ax, Wb(y, ox, z, allr, cols(A)), dx)
        ref = Wb(y, allr, z, allr, cols(A))
        sends(K.A1, [same(f"Ay{o}", ref, dy(o)) for o in (2, 1, 3)])

    def az(h, zi):
        return Wb(pl.ds(2 * h, 2), allr, zi, allr, cols(A))

    @step
    def A2():
        for o in (1, 3, 2):
            recv(f"Ay{o}", Wb(yy(-o), allr, z, allr, cols(A)), dy(-o))
        sends(K.A2, [
            same(K.Az1R0, az(0, z), dz(1)),
            same(K.Az1L1, az(1, z), dz(-1)),
            same(K.Az1R1, az(1, z), dz(1)),
            same(K.Az1L0, az(0, z), dz(-1)),
            same(K.DA0, Wb(allr, allr, z, allr, cols(A)), dc),
        ])

    def a3(s, sd, h):
        sg = 1 if sd == K.R else -1
        ref = az(h, zz(-sg * s))
        nm = f"{s}{sd}{h}"

        def f():
            recv(K.Az + nm, ref, dz(-sg))
            sends(K.A3_ + nm, [same(f"Az{s + 1}{sd}{h}", ref, dz(sg)), same(K.DA + nm, ref, dc)])

        S[K.A3_ + nm] = f

    last_a = (("3R1", 1, -3), ("3L0", 0, 3), ("4R0", 0, 4), ("4L1", 1, 4))
    for s in (1, 2, 3):
        for sd, h in ((K.R, 0), (K.L, 1), (K.R, 1), (K.L, 0)):
            if s < 3 or (sd == K.R) == (h == 0):
                a3(s, sd, h)

    @step
    def A6():
        for nm, h, o in last_a:
            recv(K.Az + nm, az(h, zz(o)), dz(-1 if K.R in nm else 1))
        sends(K.A6, [same(K.DA + nm, az(h, zz(o)), dc) for nm, h, o in last_a])

    def bref(yi, xi):
        return Wb(yi, xi, allr, allr, cols(B))

    def cref(yi, xi, zs=allr):
        return Wb(yi, xi, zs, allr, cols(C))

    @step
    def BC1():
        for o in (1, 7, 2, 6, 3, 5, 4):
            recv(f"Zd{o}", Wb(y, x, zz(-o), allr, cols(BC)), dz(-o))
        b, cc = bref(y, x), cref(y, x)
        sends(K.BC1, [
            same(K.Bx, b, dx), same(K.By1Rx, b, dy(1)), same(K.By1Lx, b, dy(-1)),
            same(K.Cy1R, cc, dy(1)), same(K.Cy1L, cc, dy(-1)), same(K.Cx0, cc, dx),
            same(K.DB0, b, dc), same(K.DC0, cc, dc),
        ])

    @step
    def B2():
        b = bref(y, ox)
        recv(K.Bx, b, dx)
        sends(K.B2, [same(K.By1Ro, b, dy(1)), same(K.By1Lo, b, dy(-1)), same(K.DB1, b, dc)])

    @step
    def B3R():
        b = bref(yy(-1), x)
        recv(K.By1Rx, b, dy(-1))
        sends(K.B3R, [same(K.By2R, b, dy(1)), same(K.DB2, b, dc)])

    @step
    def B3L():
        b = bref(yy(1), ox)
        recv(K.By1Lo, b, dy(1))
        sends(K.B3L, [same(K.By2L, b, dy(-1)), same(K.DB3, b, dc)])

    last_b = ((K.By2R, 2, x, -1), (K.By2L, 2, ox, 1), (K.By1Ro, -1, ox, -1), (K.By1Lx, 1, x, 1))

    @step
    def B4():
        for nm, o, xi, d in last_b:
            recv(nm, bref(yy(o), xi), dy(d))
        sends(K.B4, [same(K.D + nm, bref(yy(o), xi), dc) for nm, o, xi, d in last_b])

    lo4, hi4 = pl.ds(0, 4), pl.ds(4, 4)

    @step
    def C2R():
        recv(K.Cy1R, cref(yy(-1), x), dy(-1))
        sends(K.C2R, [
            same(K.Cy2R, cref(yy(-1), x, lo4), dy(1)),
            same(K.Cx3, cref(yy(-1), x), dx), same(K.DC3, cref(yy(-1), x), dc),
        ])

    @step
    def C2L():
        recv(K.Cy1L, cref(yy(1), x), dy(1))
        sends(K.C2L, [
            same(K.Cy2L, cref(yy(1), x, hi4), dy(-1)),
            same(K.Cx1, cref(yy(1), x), dx), same(K.DC1, cref(yy(1), x), dc),
        ])

    @step
    def C3():
        recv(K.Cy2R, cref(yy(2), x, lo4), dy(-1))
        recv(K.Cy2L, cref(yy(2), x, hi4), dy(1))
        sends(K.C3, [same(K.Cx2, cref(yy(2), x), dx), same(K.DC2, cref(yy(2), x), dc)])

    @step
    def C4():
        for o in (0, 1, 3, 2):
            recv(f"Cx{o}", cref(yy(o), ox), dx)
        sends(K.C4, [same(f"DCx{o}", cref(yy(o), ox), dc) for o in (0, 1, 3, 2)])

    @step
    def gp():
        recv(K.og, ogP, dc)
        for b in range(4):
            ogT[b, :, TOK : 2 * TOK] = ogP[:, b * 256 : (b + 1) * 256].T
        recv(K.h, hid2.at[pl.ds(TOK, TOK)], dc)

    def grads(cr):
        def body(b, _):
            p = jnp.dot(ogT[b], hid2[:, cols(cr)], preferred_element_type=F32)
            G[b, :, :, :, cols(cr)] = p.reshape(NX, NZ, 16, cr[1])
            return 0

        lax.fori_loop(0, NY, body, 0)

    S[K.gA] = lambda: grads(A)
    S[K.gB] = lambda: grads(B)
    S[K.gC] = lambda: grads(C)

    def ga(h, zi):
        return G[2 * h : 2 * h + 2, :, zi, :, cols(A)]

    @step
    def RA1():
        sa1[0] = ga(0, zz(4)).astype(BF)
        sa1[1] = ga(1, zz(4)).astype(BF)
        sa2[0, 0, 1] = ga(1, zz(3)).astype(BF)
        sa2[1, 0, 0] = ga(0, zz(-3)).astype(BF)
        sends(K.RA1, [
            (K.rA1R0, sa1.at[0], ra1.at[0], dz(1)),
            (K.rA1L1, sa1.at[1], ra1.at[1], dz(-1)),
            (K.rA2R1, sa2.at[0, 0, 1], ra2.at[0, 0, 1], dz(1)),
            (K.rA2L0, sa2.at[1, 0, 0], ra2.at[1, 0, 0], dz(-1)),
        ])

    def ra(s, sd, h):
        sg = 1 if sd == K.R else -1
        side = 0 if sd == K.R else 1

        def f():
            buf = ra1.at[side] if s == 2 else ra2.at[side, s - 3, h]
            recv(f"rA{s - 1}{sd}{h}", buf, dz(-sg))
            sa2[side, s - 2, h] = (ga(h, zz(sg * (5 - s))) + buf[...].astype(F32)).astype(BF)
            sends(K.RA, [(f"rA{s}{sd}{h}", sa2.at[side, s - 2, h], ra2.at[side, s - 2, h], dz(sg))])

        S[f"RA{s}{sd}{h}"] = f

    for sd in K.RL:
        for h in (0, 1):
            for s in range(2 if (sd == K.R) == (h == 0) else 3, 5):
                ra(s, sd, h)

    @step
    def RA5():
        for sd, d in ((K.R, -1), (K.L, 1)):
            for h in (0, 1):
                recv(f"rA4{sd}{h}", ra2.at[K.RL.index(sd), 2, h], dz(d))
        for h in (0, 1):
            t = ga(h, z) + ra2[0, 2, h].astype(F32) + ra2[1, 2, h].astype(F32)
            G[2 * h : 2 * h + 2, :, z, :, cols(A)] = t
            sa3[2 * h : 2 * h + 2] = t.astype(BF)
        sends(K.RA5, [(f"rAy{o}", sa3.at[yy(o)], ra3.at[o - 1], dy(o)) for o in (2, 1, 3)])

    @step
    def RA6():
        for o in (1, 3, 2):
            recv(f"rAy{o}", ra3.at[o - 1], dy(-o))
        t = G[y, :, z, :, cols(A)]
        for o in (1, 2, 3):
            t = t + ra3[o - 1].astype(F32)
        G[y, :, z, :, cols(A)] = t
        sa4[...] = t.astype(BF)
        sends(K.RA6, [(K.rAx, sa4.at[ox], ra4, dx)])

    @step
    def RA7():
        recv(K.rAx, ra4, dx)
        fin[:, cols(A)] = G[y, x, z, :, cols(A)] + ra4[...].astype(F32)

    def gb(yi, xi):
        return G[yi, xi, :, :, cols(B)]

    @step
    def RB1():
        sb1[0] = gb(yy(2), x).astype(BF)
        sb1[1] = gb(yy(2), ox).astype(BF)
        sb2[0, 1] = gb(yy(1), ox).astype(BF)
        sb2[1, 0] = gb(yy(-1), x).astype(BF)
        sends(K.RB1, [
            (K.rB1R, sb1.at[0], rb1.at[0], dy(1)), (K.rB1L, sb1.at[1], rb1.at[1], dy(-1)),
            (K.rB2R1, sb2.at[0, 1], rb2.at[0, 1], dy(1)),
            (K.rB2L1, sb2.at[1, 0], rb2.at[1, 0], dy(-1)),
        ])

    @step
    def RB2R():
        recv(K.rB1R, rb1.at[0], dy(-1))
        sb2[0, 0] = (gb(yy(1), x) + rb1[0].astype(F32)).astype(BF)
        sends(K.RB2R, [(K.rB2R0, sb2.at[0, 0], rb2.at[0, 0], dy(1))])

    @step
    def RB2L():
        recv(K.rB1L, rb1.at[1], dy(1))
        sb2[1, 1] = (gb(yy(-1), ox) + rb1[1].astype(F32)).astype(BF)
        sends(K.RB2L, [(K.rB2L0, sb2.at[1, 1], rb2.at[1, 1], dy(-1))])

    @step
    def RB3():
        recv(K.rB2R1, rb2.at[0, 1], dy(-1))
        recv(K.rB2L0, rb2.at[1, 1], dy(1))
        sb3[...] = (gb(y, ox) + rb2[0, 1].astype(F32) + rb2[1, 1].astype(F32)).astype(BF)
        sends(K.RB3, [(K.rBx, sb3, rb3, dx)])

    @step
    def RB4():
        recv(K.rB2R0, rb2.at[0, 0], dy(-1))
        recv(K.rB2L1, rb2.at[1, 0], dy(1))
        recv(K.rBx, rb3, dx)
        t = gb(y, x) + rb2[0, 0].astype(F32) + rb2[1, 0].astype(F32) + rb3[...].astype(F32)
        G[y, x, :, :, cols(B)] = t
        sb4[...] = t.astype(BF)
        sends(K.RB4, [(f"rBz{o}", sb4.at[zz(o)], rb4.at[o - 1], dz(o)) for o in (4, 3, 5, 2, 6, 1, 7)])

    @step
    def RB5():
        t = G[y, x, z, :, cols(B)]
        for o in range(1, NZ):
            recv(f"rBz{o}", rb4.at[o - 1], dz(-o))
        for o in range(1, NZ):
            t = t + rb4[o - 1].astype(F32)
        fin[:, cols(B)] = t

    def gc(yi, xi, zs=allr):
        return G[yi, xi, zs, :, cols(C)]

    @step
    def RC1():
        items = []
        for o in (2, 1, 3, 0):
            sc1[o] = gc(yy(o), ox).astype(BF)
            items.append((f"rCx{o}", sc1.at[o], rc1.at[o], dx))
        sends(K.RC1, items)

    @step
    def RC2():
        recv(K.rCx2, rc1.at[2], dx)
        sc2[...] = (gc(yy(2), x) + rc1[2].astype(F32)).astype(BF)
        sends(K.RC2, [
            (K.rCy1R, sc2.at[lo4], rc2.at[0], dy(1)), (K.rCy1L, sc2.at[hi4], rc2.at[1], dy(-1)),
        ])

    @step
    def RC2b():
        recv(K.rCx1, rc1.at[1], dx)
        t = gc(yy(1), x) + rc1[1].astype(F32)
        G[yy(1), x, :, :, cols(C)] = t
        sc3[0, 4:8] = t[4:8].astype(BF)
        sends(K.RC2b, [(K.rCy2R1, sc3.at[0, hi4], rc3.at[0, hi4], dy(1))])

    @step
    def RC2c():
        recv(K.rCx3, rc1.at[3], dx)
        t = gc(yy(3), x) + rc1[3].astype(F32)
        G[yy(3), x, :, :, cols(C)] = t
        sc3[1, 0:4] = t[0:4].astype(BF)
        sends(K.RC2c, [(K.rCy2L1, sc3.at[1, lo4], rc3.at[1, lo4], dy(-1))])

    @step
    def RC3R():
        recv(K.rCy1R, rc2.at[0], dy(-1))
        sc3[0, 0:4] = (gc(yy(1), x, slice(0, 4)) + rc2[0].astype(F32)).astype(BF)
        sends(K.RC3R, [(K.rCy2R0, sc3.at[0, lo4], rc3.at[0, lo4], dy(1))])

    @step
    def RC3L():
        recv(K.rCy1L, rc2.at[1], dy(1))
        sc3[1, 4:8] = (gc(yy(3), x, slice(4, 8)) + rc2[1].astype(F32)).astype(BF)
        sends(K.RC3L, [(K.rCy2L0, sc3.at[1, hi4], rc3.at[1, hi4], dy(-1))])

    @step
    def RC4():
        recv(K.rCx0, rc1.at[0], dx)
        recv(K.rCy2R0, rc3.at[0, lo4], dy(-1))
        recv(K.rCy2R1, rc3.at[0, hi4], dy(-1))
        recv(K.rCy2L0, rc3.at[1, hi4], dy(1))
        recv(K.rCy2L1, rc3.at[1, lo4], dy(1))
        t = gc(y, x) + rc1[0].astype(F32) + rc3[0].astype(F32) + rc3[1].astype(F32)
        G[y, x, :, :, cols(C)] = t
        sc4[...] = t.astype(BF)
        sends(K.RC4, [(f"rCz{o}", sc4.at[zz(o)], rc4.at[o - 1], dz(o)) for o in (4, 3, 5, 2, 6, 1, 7)])

    @step
    def RC5():
        t = G[y, x, z, :, cols(C)]
        for o in range(1, NZ):
            recv(f"rCz{o}", rc4.at[o - 1], dz(-o))
        for o in range(1, NZ):
            t = t + rc4[o - 1].astype(F32)
        fin[:, cols(C)] = t

    def partner_pieces(k):
        if k == K.A:
            yield K.DA0, W.at[oc, :, :, z, :, cols(A)]
            for s in (1, 2, 3, 4):
                for sd, sg in ((K.R, 1), (K.L, -1)):
                    for h in (0, 1):
                        if s < 4 or (sd == K.R) == (h == 0):
                            yield f"DA{s}{sd}{h}", W.at[oc, pl.ds(2 * h, 2), :, zz(-sg * s), :, cols(A)]
        if k == K.B:
            for nm, o, xi in (
                (K.DB0, 0, x), (K.DB1, 0, ox), (K.DB2, -1, x), (K.DB3, 1, ox),
                (K.DBy1Ro, -1, ox), (K.DBy1Lx, 1, x), (K.DBy2R, 2, x), (K.DBy2L, 2, ox),
            ):
                yield nm, W.at[oc, yy(o), xi, :, :, cols(B)]
        if k == K.C:
            for o in (0, 1, 3, 2):
                yield f"DC{o}", W.at[oc, yy(o), x, :, :, cols(C)]
                yield f"DCx{o}", W.at[oc, yy(o), ox, :, :, cols(C)]

    ranges = {K.A: A, K.B: B, K.C: C}
    have = set()
    started = []

    def w_of(side, k):
        if side == K.o and k not in have:
            have.add(k)
            for nm, ref in partner_pieces(k):
                recv(nm, ref, dc)
        half = c if side == K.c else oc
        return W[half, :, :, :, :, cols(ranges[k])].reshape(D, ranges[k][1])

    def lo(side, k):
        w = w_of(side, k)
        h = (hid2 if side == K.c else hidO)[0:TOK, cols(ranges[k])]
        part = lax.dot_general(h, w, (((1,), (1,)), ((), ())), preferred_element_type=F32)
        if started:
            acc[...] += part
        else:
            acc[...] = part
        started.append(1)

    def hgrad(side, k):
        n = ranges[k][1]
        half = c if side == K.c else oc
        hg[:, 0:n] = jnp.dot(og_ref[...], w_of(side, k), preferred_element_type=F32)
        cs = pl.ds(pl.multiple_of(half * HALF + ranges[k][0], 128), n)

        def body(i, _):
            rows = pl.ds(pl.multiple_of(i * 16, 16), 16)
            g = gate_ref[rows, cs].astype(F32)
            u = up_ref[rows, cs].astype(F32)
            h = hg[rows, 0:n]
            s = jax.nn.sigmoid(g)
            gg_ref[rows, cs] = (h * u * s * (1.0 + g * (1.0 - s))).astype(BF)
            ug_ref[rows, cs] = (h * g * s).astype(BF)
            return 0

        lax.fori_loop(0, TOK // 16, body, 0)
        local(f"gg{side}{k}", gg_ref.at[:, cs], gg_hbm.at[:, cs])
        local(f"ug{side}{k}", ug_ref.at[:, cs], ug_hbm.at[:, cs])

    for side in K.co:
        for k in K.ABC:
            S[f"lo_{side}{k}"] = lambda side=side, k=k: lo(side, k)
            S[f"hg_{side}{k}"] = lambda side=side, k=k: hgrad(side, k)

    @step
    def losend():
        lo_s[...] = acc[:, pl.ds(pl.multiple_of((1 - r) * 512, 128), 512)].astype(BF)
        sends(K.losend, [(K.lo, lo_s, lo_r, dr)])

    @step
    def lofin():
        recv(K.lo, lo_r, dr)
        out_ref[...] = (
            acc[:, pl.ds(pl.multiple_of(r * 512, 128), 512)] + lo_r[...].astype(F32)
        ).astype(BF)
        local(K.out, out_ref, out_hbm)

    def update(half, g):
        cs = pl.ds(pl.multiple_of(half * HALF, 128), HALF)
        g = g / jnp.float32(32768)
        m = master_ref[:, cs]
        first = 0.9 * one_ref[:, cs] + 0.1 * g
        second = 0.95 * two_ref[:, cs] + 0.05 * g * g
        upd = first / (1.0 - first_power) / (jnp.sqrt(second / (1.0 - second_power)) + 1e-08)
        master_out[:, cs] = m - 0.003 * (upd + 0.1 * m)
        one_out[:, cs] = first
        two_out[:, cs] = second

    @step
    def fin_():
        sends(K.fin, [(K.fin, fin.at[pl.ds(pl.multiple_of(oc * 8, 8), 8)], finP, dc)])
        update(c, fin[pl.ds(pl.multiple_of(c * 8, 8), 8), :])

    @step
    def adam():
        recv(K.fin, finP, dc)
        update(oc, finP[...])
        local(K.mo, master_out, master_out_hbm)
        local(K.oo, one_out, one_out_hbm)
        local(K.to, two_out, two_out_hbm)

    with jax.named_scope(K.loads):
        loc[K.gate].wait()
        loc[K.up].wait()
    with jax.named_scope(K.hidden):
        hidden_rows(oc, hidO)
        hidden_rows(c, hid2)
    for n in (K.og, K.master, K.one, K.two):
        loc[n].wait()
    with jax.named_scope(K.transpose):
        for b in range(4):
            ogT[b, :, 0:TOK] = og_ref[:, b * 256 : (b + 1) * 256].T
    with jax.named_scope(K.barrier):
        pl.semaphore_wait(bar, len(peers))
    for n in ORDER:
        with jax.named_scope(n):
            S.pop(n)()
    assert not S, S.keys()
    with jax.named_scope(K.sends_done):
        for d in sent:
            d.wait_send()
        for n, d in loc.items():
            if n not in (K.gate, K.up, K.og, K.master, K.one, K.two):
                d.wait()
    assert len(slots) <= NSEM, len(slots)


NSEM = 144


def copy_kernel(*refs):
    src, dst, buf, sem = refs[0:6], refs[6:12], refs[12:18], refs[18]
    parts = []
    for i in (1, 2, 0, 3, 4, 5):
        rows = src[i].shape[0]
        n = 2 if rows > 8 else 1
        for j in range(n):
            rs = pl.ds(j * (rows // n), rows // n)
            k = len(parts)
            parts.append((
                pltpu.make_async_copy(src[i].at[rs], buf[i].at[rs], sem.at[0, k]),
                pltpu.make_async_copy(buf[i].at[rs], dst[i].at[rs], sem.at[1, k]),
            ))
    for a, _ in parts:
        a.start()
    for a, b in parts:
        a.wait()
        b.start()
    for _, b in parts:
        b.wait()


def on_device(gate_pre, up_pre, out_grad, master, moment_one, moment_two):
    V = pltpu.VMEM
    nA, nB, nC = A[1], B[1], C[1]
    outs = pl.pallas_call(
        kernel,
        out_shape=(
            jax.ShapeDtypeStruct((TOK, 512), BF),
            jax.ShapeDtypeStruct((TOK, FF), BF),
            jax.ShapeDtypeStruct((TOK, FF), BF),
            jax.ShapeDtypeStruct((8, FF), F32),
            jax.ShapeDtypeStruct((8, FF), F32),
            jax.ShapeDtypeStruct((8, FF), F32),
        ),
        in_specs=[pl.BlockSpec(memory_space=pl.ANY)] * 6,
        out_specs=[pl.BlockSpec(memory_space=pl.ANY)] * 6,
        scratch_shapes=[
            V((TOK, FF), BF), V((TOK, FF), BF), V((TOK, D), BF),
            V((8, FF), F32), V((8, FF), F32), V((8, FF), F32),
            V((TOK, 512), BF), V((TOK, FF), BF), V((TOK, FF), BF),
            V((8, FF), F32), V((8, FF), F32), V((8, FF), F32),
            V((NC, NY, NX, NZ, 16, HALF), BF),
            V((NY, NX, NZ, 16, HALF), F32),
            V((2 * TOK, HALF), BF),
            V((TOK, HALF), BF),
            V((TOK, D), BF),
            V((4, 256, 2 * TOK), BF),
            V((8, HALF), F32),
            V((TOK, 512), F32),
            V((TOK, D), F32),
            V((16, HALF), F32),
            V((8, HALF), F32),
            V((TOK, 512), BF),
            V((TOK, 512), BF),
            V((2, 2, NX, 16, nA), BF), V((2, 2, NX, 16, nA), BF),
            V((2, 3, 2, 2, NX, 16, nA), BF), V((2, 3, 2, 2, NX, 16, nA), BF),
            V((NY, NX, 16, nA), BF), V((3, NX, 16, nA), BF),
            V((NX, 16, nA), BF), V((16, nA), BF),
            V((NX, NZ, 16, nB), BF), V((2, NZ, 16, nB), BF),
            V((2, NX, NZ, 16, nB), BF), V((2, NX, NZ, 16, nB), BF),
            V((NZ, 16, nB), BF), V((NZ, 16, nB), BF),
            V((NZ, 16, nB), BF), V((7, 16, nB), BF),
            V((NY, NZ, 16, nC), BF), V((NY, NZ, 16, nC), BF),
            V((NZ, 16, nC), BF), V((2, 4, 16, nC), BF),
            V((2, NZ, 16, nC), BF), V((2, NZ, 16, nC), BF),
            V((NZ, 16, nC), BF), V((7, 16, nC), BF),
            pltpu.SemaphoreType.DMA((NSEM,)),
            pltpu.SemaphoreType.DMA((NSEM,)),
            pltpu.SemaphoreType.DMA((24,)),
        ],
        compiler_params=pltpu.CompilerParams(
            collective_id=0, has_side_effects=True, vmem_limit_bytes=66_000_000
        ),
    )(
        gate_pre.reshape(TOK, FF),
        up_pre.reshape(TOK, FF),
        out_grad.reshape(TOK, D),
        master,
        moment_one,
        moment_two,
    )
    outs = pl.pallas_call(
        copy_kernel,
        out_shape=tuple(jax.ShapeDtypeStruct(o.shape, o.dtype) for o in outs),
        in_specs=[pl.BlockSpec(memory_space=pl.ANY)] * 6,
        out_specs=[pl.BlockSpec(memory_space=pl.ANY)] * 6,
        scratch_shapes=[V(o.shape, o.dtype) for o in outs] + [pltpu.SemaphoreType.DMA((2, 12))],
    )(*outs)
    lo, gg, ug, mn, m1, m2 = outs
    return (
        lo.reshape(2, 128, 512),
        gg.reshape(2, 128, FF),
        ug.reshape(2, 128, FF),
        mn,
        m1,
        m2,
    )


def solution(mesh):
    torus = Mesh(
        mesh.devices.reshape(NY, NX, NZ, NC, mesh.shape["rep"]),
        ("dp_0", "dp_1", "dp_2", "dp_3", "rep"),
    )
    return jax.shard_map(
        on_device,
        mesh=torus,
        in_specs=(
            P(None, DP, "rep"),
            P(None, DP, "rep"),
            P(None, DP, None),
            P(DP, "rep"),
            P(DP, "rep"),
            P(DP, "rep"),
        ),
        out_specs=(
            P(None, DP, "rep"),
            P(None, DP, "rep"),
            P(None, DP, "rep"),
            P(DP, "rep"),
            P(DP, "rep"),
            P(DP, "rep"),
        ),
        check_vma=False,
    )
```

```python
import jax
import jax.numpy as jnp
from jax import lax
from jax.experimental import pallas as pl
from jax.experimental.pallas import tpu as pltpu
from jax.sharding import Mesh
from jax.sharding import PartitionSpec as P

DP = ("dp_0", "dp_1", "dp_2", "dp_3")
NY, NX, NZ, NC = 4, 2, 8, 2

first_power = 2.6561398887587544e-05
second_power = 0.005920529220333997

F32 = jnp.float32
BF = jnp.bfloat16
D = 1024
FF = 2816
HALF = 1408
TOK = 256
A = (0, 512)
B = (512, 512)
C = (1024, 384)
BC = (512, 896)


def cols(r):
    return pl.ds(r[0], r[1])


class Names:
    def __getattr__(self, word):
        return word


K = Names()

ORDER = (
    K.init, K.hidO_, K.A1, K.hid2_, K.gp, K.gB, K.RB1, K.gC, K.RC1, K.A2, K.gA, K.RA1, K.A3_1L1,
    K.RB2L, K.A3_1L0, K.A3_1R1, K.BC1, K.RA3R1, K.RA2L0, K.A3_1R0, K.A3_2R1, K.A3_2L1, K.C2R,
    K.A3_2L0, K.C2L, K.RB2R, K.RA4R1, K.A3_2R0, K.B2, K.A3_3L1, K.C3, K.RC2, K.A3_3L0, K.RA3R0,
    K.RA2L1, K.RA3L0, K.B3R, K.B3L, K.RC2b, K.RC2c, K.A6, K.RB3, K.RA4R0, K.RA3L1, K.RA4L0,
    K.C4, K.lo_cC, K.lo_oA, K.B4, K.RA4L1, K.lo_cB, K.lo_oC, K.lo_cA, K.RB4, K.lo_oB, K.losend,
    K.RC3L, K.RC3R, K.hg_cB, K.RA5, K.hg_oA, K.RC4, K.hg_cA, K.hg_oC, K.hg_oB, K.RA6, K.hg_cC,
    K.RB5, K.RC5, K.RA7, K.fin_, K.lofin, K.adam,
)
ORDS = {
    K.init: (K.Zd2, K.Zd6, K.Zd3, K.Zd4, K.og, K.Zd1, K.Zd7, K.Zd5, K.Ax,),
    K.A1: (K.Ay2, K.Ay1, K.Ay3,),
    K.A2: (K.Az1L1, K.DA0, K.Az1L0, K.Az1R1, K.Az1R0,),
    K.A3_1R0: (K.DA1R0, K.Az2R0,),
    K.A3_1R1: (K.Az2R1, K.DA1R1,),
    K.A3_1L0: (K.Az2L0, K.DA1L0,),
    K.A3_1L1: (K.DA1L1, K.Az2L1,),
    K.A3_2R0: (K.DA2R0, K.Az3R0,),
    K.A3_2R1: (K.Az3R1, K.DA2R1,),
    K.A3_2L0: (K.Az3L0, K.DA2L0,),
    K.A3_2L1: (K.Az3L1, K.DA2L1,),
    K.A3_3L0: (K.Az4L0, K.DA3L0,),
    K.A3_3L1: (K.DA3L1, K.Az4L1,),
    K.BC1: (K.Cy1L, K.Cy1R, K.Bx, K.DB0, K.Cx0, K.By1Rx, K.DC0, K.By1Lx,),
    K.B2: (K.By1Ro, K.DB1, K.By1Lo,),
    K.B3R: (K.DB2, K.By2R,),
    K.B3L: (K.DB3, K.By2L,),
    K.C2R: (K.DC3, K.Cy2R, K.Cx3,),
    K.C2L: (K.Cx1, K.Cy2L, K.DC1,),
    K.C3: (K.Cx2, K.DC2,),
    K.RC1: (K.rCx3, K.rCx2, K.rCx0, K.rCx1,),
    K.RB1: (K.rB1R, K.rB1L, K.rB2L1, K.rB2R1,),
    K.RA1: (K.rA2R1, K.rA1L1, K.rA2R0, K.rA1L0,),
    K.RA5: (K.rAy3, K.rAy1, K.rAy2,),
    K.RB4: (K.rBz7, K.rBz1, K.rBz4, K.rBz2, K.rBz6, K.rBz5, K.rBz3,),
    K.RC2: (K.rCy1R, K.rCy1L,),
    K.RC4: (K.rCz4, K.rCz5, K.rCz3, K.rCz2, K.rCz6, K.rCz1, K.rCz7,),
}


def kernel(
    gate_hbm, up_hbm, og_hbm, master_hbm, one_hbm, two_hbm,
    out_ref, gg_ref, ug_ref, master_out, one_out, two_out,
    gate_ref, up_ref, og_ref, master_ref, one_ref, two_ref,
    W, G, hid2, hidO, ogP, ogT, mP, hg, acc, fin, finP, lo_s, lo_r,
    sa1, ra1, sa2, ra2, sa3, ra3, sa4, ra4,
    sb1, rb1, sb2, rb2, sb3, rb3, sb4, rb4,
    sc1, rc1, sc2, rc2, sc3, rc3, sc4, rc4,
    ssem, rsem, lsem,
):
    y = lax.axis_index(K.dp_0)
    x = lax.axis_index(K.dp_1)
    z = lax.axis_index(K.dp_2)
    c = lax.axis_index(K.dp_3)
    r = lax.axis_index(K.rep)
    oc = 1 - c
    ox = 1 - x

    def dy(o):
        return {K.dp_0: lax.rem(y + (o % NY), NY)}

    def dz(o):
        return {K.dp_2: lax.rem(z + (o % NZ), NZ)}

    def zz(o):
        return lax.rem(z + (o % NZ), NZ)

    def yy(o):
        return lax.rem(y + (o % NY), NY)

    dx = {K.dp_1: ox}
    dc = {K.dp_3: oc}
    dr = {K.rep: 1 - r}
    allr = slice(None)

    peers = [dc, dx, dr] + [dy(o) for o in range(1, NY)] + [dz(o) for o in range(1, NZ)]
    bar = pltpu.get_barrier_semaphore()
    for p in peers:
        pl.semaphore_signal(bar, inc=1, device_id=p, device_id_type=pl.DeviceIdType.MESH)

    loc = {}

    def local(name, src, dst):
        d = pltpu.make_async_copy(src, dst, lsem.at[len(loc)])
        d.start()
        loc[name] = d

    local(K.master, master_hbm, master_ref)
    local(K.og, og_hbm, og_ref)
    local(K.gate, gate_hbm, gate_ref)
    local(K.up, up_hbm, up_ref)
    local(K.one, one_hbm, one_ref)
    local(K.two, two_hbm, two_ref)

    sent = []
    slots = {}

    def slot(name):
        if name not in slots:
            slots[name] = len(slots)
        return slots[name]

    def rc(name, src, dst, dev):
        k = slot(name)
        return pltpu.make_async_remote_copy(
            src_ref=src, dst_ref=dst, send_sem=ssem.at[k], recv_sem=rsem.at[k],
            device_id=dev, device_id_type=pl.DeviceIdType.MESH,
        )

    def sends(step, items):
        names = ORDS.get(step, tuple(i[0] for i in items))
        table = {i[0]: i for i in items}
        for n in names:
            table[n]
        for name in list(names) + [n for n in table if n not in names]:
            _, src, dst, dev = table[name]
            d = rc(name, src, dst, dev)
            d.start()
            sent.append(d)

    def recv(name, dst, dev):
        with jax.named_scope(K.wait_ + name):
            rc(name, dst, dst, dev).wait_recv()

    def hidden_rows(half, out):
        off = pl.multiple_of(half * HALF, 128)

        def body(i, _):
            rows = pl.ds(pl.multiple_of(i * 16, 16), 16)
            g = gate_ref[rows, pl.ds(off, HALF)].astype(F32)
            u = up_ref[rows, pl.ds(off, HALF)].astype(F32)
            s = jax.nn.sigmoid(g)
            out[rows, :] = (g * s * u).astype(BF)
            return 0

        lax.fori_loop(0, TOK // 16, body, 0)

    def Wb(*idx):
        return W.at[(c,) + idx]

    def same(name, ref, dev):
        return (name, ref, ref, dev)

    S = {}

    def step(f):
        S[f.__name__] = f
        return f

    @step
    def init():
        sends(K.i0, [(K.m, master_ref.at[:, pl.ds(pl.multiple_of(oc * HALF, 128), HALF)], mP, dc)])
        recv(K.m, mP, dc)
        mine = master_ref[:, pl.ds(pl.multiple_of(c * HALF, 128), HALF)]
        theirs = mP[...]
        first_core = c == 0
        W[c, y, x, z] = jnp.concatenate(
            [jnp.where(first_core, mine, theirs), jnp.where(first_core, theirs, mine)], axis=0
        ).astype(BF)
        loc[K.og].wait()
        items = [
            (K.og, og_ref, ogP, dc),
            same(K.Ax, Wb(y, x, z, allr, cols(A)), dx),
        ]
        for o in (4, 3, 5, 2, 6, 1, 7):
            items.append(same(f"Zd{o}", Wb(y, x, z, allr, cols(BC)), dz(o)))
        sends(K.init, items)

    @step
    def hidO_():
        loc[K.gate].wait()
        loc[K.up].wait()
        hidden_rows(oc, hidO)
        sends(K.h, [(K.h, hidO, hid2.at[pl.ds(TOK, TOK)], dc)])

    @step
    def hid2_():
        hidden_rows(c, hid2)
        for b in range(4):
            ogT[b, :, 0:TOK] = og_ref[:, b * 256 : (b + 1) * 256].T

    @step
    def A1():
        recv(K.Ax, Wb(y, ox, z, allr, cols(A)), dx)
        ref = Wb(y, allr, z, allr, cols(A))
        sends(K.A1, [same(f"Ay{o}", ref, dy(o)) for o in (2, 1, 3)])

    def az(h, zi):
        return Wb(pl.ds(2 * h, 2), allr, zi, allr, cols(A))

    @step
    def A2():
        for o in (1, 3, 2):
            recv(f"Ay{o}", Wb(yy(-o), allr, z, allr, cols(A)), dy(-o))
        sends(K.A2, [
            same(K.Az1L0, az(0, z), dz(-1)),
            same(K.Az1R0, az(0, z), dz(1)),
            same(K.Az1L1, az(1, z), dz(-1)),
            same(K.Az1R1, az(1, z), dz(1)),
            same(K.DA0, Wb(allr, allr, z, allr, cols(A)), dc),
        ])

    def a3(s, sd, h):
        sg = 1 if sd == K.R else -1
        ref = az(h, zz(-sg * s))
        nm = f"{s}{sd}{h}"

        def f():
            recv(K.Az + nm, ref, dz(-sg))
            sends(K.A3_ + nm, [same(f"Az{s + 1}{sd}{h}", ref, dz(sg)), same(K.DA + nm, ref, dc)])

        S[K.A3_ + nm] = f

    last_a = (("3R0", 0, -3), ("3R1", 1, -3), ("4L0", 0, 4), ("4L1", 1, 4))
    for s in (1, 2, 3):
        for h in (0, 1):
            a3(s, K.L, h)
            if s < 3:
                a3(s, K.R, h)

    @step
    def A6():
        for nm, h, o in last_a:
            recv(K.Az + nm, az(h, zz(o)), dz(-1 if K.R in nm else 1))
        sends(K.A6, [same(K.DA + nm, az(h, zz(o)), dc) for nm, h, o in last_a])

    def bref(yi, xi):
        return Wb(yi, xi, allr, allr, cols(B))

    def cref(yi, xi, zs=allr):
        return Wb(yi, xi, zs, allr, cols(C))

    @step
    def BC1():
        for o in (1, 7, 2, 6, 3, 5, 4):
            recv(f"Zd{o}", Wb(y, x, zz(-o), allr, cols(BC)), dz(-o))
        b, cc = bref(y, x), cref(y, x)
        sends(K.BC1, [
            same(K.Bx, b, dx), same(K.By1Rx, b, dy(1)), same(K.By1Lx, b, dy(-1)),
            same(K.Cy1R, cc, dy(1)), same(K.Cy1L, cc, dy(-1)), same(K.Cx0, cc, dx),
            same(K.DB0, b, dc), same(K.DC0, cc, dc),
        ])

    @step
    def B2():
        b = bref(y, ox)
        recv(K.Bx, b, dx)
        sends(K.B2, [same(K.By1Ro, b, dy(1)), same(K.By1Lo, b, dy(-1)), same(K.DB1, b, dc)])

    @step
    def B3R():
        b = bref(yy(-1), x)
        recv(K.By1Rx, b, dy(-1))
        sends(K.B3R, [same(K.By2R, b, dy(1)), same(K.DB2, b, dc)])

    @step
    def B3L():
        b = bref(yy(1), ox)
        recv(K.By1Lo, b, dy(1))
        sends(K.B3L, [same(K.By2L, b, dy(-1)), same(K.DB3, b, dc)])

    last_b = ((K.By2R, 2, x, -1), (K.By2L, 2, ox, 1), (K.By1Ro, -1, ox, -1), (K.By1Lx, 1, x, 1))

    @step
    def B4():
        for nm, o, xi, d in last_b:
            recv(nm, bref(yy(o), xi), dy(d))
        sends(K.B4, [same(K.D + nm, bref(yy(o), xi), dc) for nm, o, xi, d in last_b])

    lo4, hi4 = pl.ds(0, 4), pl.ds(4, 4)

    @step
    def C2R():
        recv(K.Cy1R, cref(yy(-1), x), dy(-1))
        sends(K.C2R, [
            same(K.Cy2R, cref(yy(-1), x, lo4), dy(1)),
            same(K.Cx3, cref(yy(-1), x), dx), same(K.DC3, cref(yy(-1), x), dc),
        ])

    @step
    def C2L():
        recv(K.Cy1L, cref(yy(1), x), dy(1))
        sends(K.C2L, [
            same(K.Cy2L, cref(yy(1), x, hi4), dy(-1)),
            same(K.Cx1, cref(yy(1), x), dx), same(K.DC1, cref(yy(1), x), dc),
        ])

    @step
    def C3():
        recv(K.Cy2R, cref(yy(2), x, lo4), dy(-1))
        recv(K.Cy2L, cref(yy(2), x, hi4), dy(1))
        sends(K.C3, [same(K.Cx2, cref(yy(2), x), dx), same(K.DC2, cref(yy(2), x), dc)])

    @step
    def C4():
        for o in (0, 1, 3, 2):
            recv(f"Cx{o}", cref(yy(o), ox), dx)
        sends(K.C4, [same(f"DCx{o}", cref(yy(o), ox), dc) for o in (0, 1, 3, 2)])

    @step
    def gp():
        recv(K.og, ogP, dc)
        for b in range(4):
            ogT[b, :, TOK : 2 * TOK] = ogP[:, b * 256 : (b + 1) * 256].T
        recv(K.h, hid2.at[pl.ds(TOK, TOK)], dc)

    def grads(cr):
        def body(b, _):
            p = jnp.dot(ogT[b], hid2[:, cols(cr)], preferred_element_type=F32)
            G[b, :, :, :, cols(cr)] = p.reshape(NX, NZ, 16, cr[1])
            return 0

        lax.fori_loop(0, NY, body, 0)

    S[K.gA] = lambda: grads(A)
    S[K.gB] = lambda: grads(B)
    S[K.gC] = lambda: grads(C)

    def ga(h, zi):
        return G[2 * h : 2 * h + 2, :, zi, :, cols(A)]

    @step
    def RA1():
        for h in (0, 1):
            sa1[h] = ga(h, zz(4)).astype(BF)
            sa2[0, 0, h] = ga(h, zz(3)).astype(BF)
        sends(K.RA1, [
            (K.rA1L0, sa1.at[0], ra1.at[0], dz(-1)),
            (K.rA1L1, sa1.at[1], ra1.at[1], dz(-1)),
            (K.rA2R0, sa2.at[0, 0, 0], ra2.at[0, 0, 0], dz(1)),
            (K.rA2R1, sa2.at[0, 0, 1], ra2.at[0, 0, 1], dz(1)),
        ])

    def ra(s, sd, h):
        sg = 1 if sd == K.R else -1
        side = 0 if sd == K.R else 1

        def f():
            buf = ra1.at[h] if s == 2 else ra2.at[side, s - 3, h]
            recv(f"rA{s - 1}{sd}{h}", buf, dz(-sg))
            sa2[side, s - 2, h] = (ga(h, zz(sg * (5 - s))) + buf[...].astype(F32)).astype(BF)
            sends(K.RA, [(f"rA{s}{sd}{h}", sa2.at[side, s - 2, h], ra2.at[side, s - 2, h], dz(sg))])

        S[f"RA{s}{sd}{h}"] = f

    for sd in K.RL:
        for h in (0, 1):
            for s in range(2 if sd == K.L else 3, 5):
                ra(s, sd, h)

    @step
    def RA5():
        for sd, d in ((K.R, -1), (K.L, 1)):
            for h in (0, 1):
                recv(f"rA4{sd}{h}", ra2.at[K.RL.index(sd), 2, h], dz(d))
        for h in (0, 1):
            t = ga(h, z) + ra2[0, 2, h].astype(F32) + ra2[1, 2, h].astype(F32)
            G[2 * h : 2 * h + 2, :, z, :, cols(A)] = t
            sa3[2 * h : 2 * h + 2] = t.astype(BF)
        sends(K.RA5, [(f"rAy{o}", sa3.at[yy(o)], ra3.at[o - 1], dy(o)) for o in (2, 1, 3)])

    @step
    def RA6():
        for o in (1, 3, 2):
            recv(f"rAy{o}", ra3.at[o - 1], dy(-o))
        t = G[y, :, z, :, cols(A)]
        for o in (1, 2, 3):
            t = t + ra3[o - 1].astype(F32)
        G[y, :, z, :, cols(A)] = t
        sa4[...] = t.astype(BF)
        sends(K.RA6, [(K.rAx, sa4.at[ox], ra4, dx)])

    @step
    def RA7():
        recv(K.rAx, ra4, dx)
        fin[:, cols(A)] = G[y, x, z, :, cols(A)] + ra4[...].astype(F32)

    def gb(yi, xi):
        return G[yi, xi, :, :, cols(B)]

    @step
    def RB1():
        sb1[0] = gb(yy(2), x).astype(BF)
        sb1[1] = gb(yy(2), ox).astype(BF)
        sb2[0, 1] = gb(yy(1), ox).astype(BF)
        sb2[1, 0] = gb(yy(-1), x).astype(BF)
        sends(K.RB1, [
            (K.rB1R, sb1.at[0], rb1.at[0], dy(1)), (K.rB1L, sb1.at[1], rb1.at[1], dy(-1)),
            (K.rB2R1, sb2.at[0, 1], rb2.at[0, 1], dy(1)),
            (K.rB2L1, sb2.at[1, 0], rb2.at[1, 0], dy(-1)),
        ])

    @step
    def RB2R():
        recv(K.rB1R, rb1.at[0], dy(-1))
        sb2[0, 0] = (gb(yy(1), x) + rb1[0].astype(F32)).astype(BF)
        sends(K.RB2R, [(K.rB2R0, sb2.at[0, 0], rb2.at[0, 0], dy(1))])

    @step
    def RB2L():
        recv(K.rB1L, rb1.at[1], dy(1))
        sb2[1, 1] = (gb(yy(-1), ox) + rb1[1].astype(F32)).astype(BF)
        sends(K.RB2L, [(K.rB2L0, sb2.at[1, 1], rb2.at[1, 1], dy(-1))])

    @step
    def RB3():
        recv(K.rB2R1, rb2.at[0, 1], dy(-1))
        recv(K.rB2L0, rb2.at[1, 1], dy(1))
        sb3[...] = (gb(y, ox) + rb2[0, 1].astype(F32) + rb2[1, 1].astype(F32)).astype(BF)
        sends(K.RB3, [(K.rBx, sb3, rb3, dx)])

    @step
    def RB4():
        recv(K.rB2R0, rb2.at[0, 0], dy(-1))
        recv(K.rB2L1, rb2.at[1, 0], dy(1))
        recv(K.rBx, rb3, dx)
        t = gb(y, x) + rb2[0, 0].astype(F32) + rb2[1, 0].astype(F32) + rb3[...].astype(F32)
        G[y, x, :, :, cols(B)] = t
        sb4[...] = t.astype(BF)
        sends(K.RB4, [(f"rBz{o}", sb4.at[zz(o)], rb4.at[o - 1], dz(o)) for o in (4, 3, 5, 2, 6, 1, 7)])

    @step
    def RB5():
        t = G[y, x, z, :, cols(B)]
        for o in range(1, NZ):
            recv(f"rBz{o}", rb4.at[o - 1], dz(-o))
        for o in range(1, NZ):
            t = t + rb4[o - 1].astype(F32)
        fin[:, cols(B)] = t

    def gc(yi, xi, zs=allr):
        return G[yi, xi, zs, :, cols(C)]

    @step
    def RC1():
        items = []
        for o in (2, 1, 3, 0):
            sc1[o] = gc(yy(o), ox).astype(BF)
            items.append((f"rCx{o}", sc1.at[o], rc1.at[o], dx))
        sends(K.RC1, items)

    @step
    def RC2():
        recv(K.rCx2, rc1.at[2], dx)
        sc2[...] = (gc(yy(2), x) + rc1[2].astype(F32)).astype(BF)
        sends(K.RC2, [
            (K.rCy1R, sc2.at[lo4], rc2.at[0], dy(1)), (K.rCy1L, sc2.at[hi4], rc2.at[1], dy(-1)),
        ])

    @step
    def RC2b():
        recv(K.rCx1, rc1.at[1], dx)
        t = gc(yy(1), x) + rc1[1].astype(F32)
        G[yy(1), x, :, :, cols(C)] = t
        sc3[0, 4:8] = t[4:8].astype(BF)
        sends(K.RC2b, [(K.rCy2R1, sc3.at[0, hi4], rc3.at[0, hi4], dy(1))])

    @step
    def RC2c():
        recv(K.rCx3, rc1.at[3], dx)
        t = gc(yy(3), x) + rc1[3].astype(F32)
        G[yy(3), x, :, :, cols(C)] = t
        sc3[1, 0:4] = t[0:4].astype(BF)
        sends(K.RC2c, [(K.rCy2L1, sc3.at[1, lo4], rc3.at[1, lo4], dy(-1))])

    @step
    def RC3R():
        recv(K.rCy1R, rc2.at[0], dy(-1))
        sc3[0, 0:4] = (gc(yy(1), x, slice(0, 4)) + rc2[0].astype(F32)).astype(BF)
        sends(K.RC3R, [(K.rCy2R0, sc3.at[0, lo4], rc3.at[0, lo4], dy(1))])

    @step
    def RC3L():
        recv(K.rCy1L, rc2.at[1], dy(1))
        sc3[1, 4:8] = (gc(yy(3), x, slice(4, 8)) + rc2[1].astype(F32)).astype(BF)
        sends(K.RC3L, [(K.rCy2L0, sc3.at[1, hi4], rc3.at[1, hi4], dy(-1))])

    @step
    def RC4():
        recv(K.rCx0, rc1.at[0], dx)
        recv(K.rCy2R0, rc3.at[0, lo4], dy(-1))
        recv(K.rCy2R1, rc3.at[0, hi4], dy(-1))
        recv(K.rCy2L0, rc3.at[1, hi4], dy(1))
        recv(K.rCy2L1, rc3.at[1, lo4], dy(1))
        t = gc(y, x) + rc1[0].astype(F32) + rc3[0].astype(F32) + rc3[1].astype(F32)
        G[y, x, :, :, cols(C)] = t
        sc4[...] = t.astype(BF)
        sends(K.RC4, [(f"rCz{o}", sc4.at[zz(o)], rc4.at[o - 1], dz(o)) for o in (4, 3, 5, 2, 6, 1, 7)])

    @step
    def RC5():
        t = G[y, x, z, :, cols(C)]
        for o in range(1, NZ):
            recv(f"rCz{o}", rc4.at[o - 1], dz(-o))
        for o in range(1, NZ):
            t = t + rc4[o - 1].astype(F32)
        fin[:, cols(C)] = t

    def partner_pieces(k):
        if k == K.A:
            yield K.DA0, W.at[oc, :, :, z, :, cols(A)]
            for s in (1, 2, 3, 4):
                for sd, sg in ((K.R, 1), (K.L, -1)):
                    for h in (0, 1):
                        if s < 4 or sd == K.L:
                            yield f"DA{s}{sd}{h}", W.at[oc, pl.ds(2 * h, 2), :, zz(-sg * s), :, cols(A)]
        if k == K.B:
            for nm, o, xi in (
                (K.DB0, 0, x), (K.DB1, 0, ox), (K.DB2, -1, x), (K.DB3, 1, ox),
                (K.DBy1Ro, -1, ox), (K.DBy1Lx, 1, x), (K.DBy2R, 2, x), (K.DBy2L, 2, ox),
            ):
                yield nm, W.at[oc, yy(o), xi, :, :, cols(B)]
        if k == K.C:
            for o in (0, 1, 3, 2):
                yield f"DC{o}", W.at[oc, yy(o), x, :, :, cols(C)]
                yield f"DCx{o}", W.at[oc, yy(o), ox, :, :, cols(C)]

    ranges = {K.A: A, K.B: B, K.C: C}
    have = set()
    started = []

    def w_of(side, k):
        if side == K.o and k not in have:
            have.add(k)
            for nm, ref in partner_pieces(k):
                recv(nm, ref, dc)
        half = c if side == K.c else oc
        return W[half, :, :, :, :, cols(ranges[k])].reshape(D, ranges[k][1])

    def lo(side, k):
        w = w_of(side, k)
        h = (hid2 if side == K.c else hidO)[0:TOK, cols(ranges[k])]
        part = lax.dot_general(h, w, (((1,), (1,)), ((), ())), preferred_element_type=F32)
        if started:
            acc[...] += part
        else:
            acc[...] = part
        started.append(1)

    def hgrad(side, k):
        n = ranges[k][1]
        half = c if side == K.c else oc
        hg[:, 0:n] = jnp.dot(og_ref[...], w_of(side, k), preferred_element_type=F32)
        cs = pl.ds(pl.multiple_of(half * HALF + ranges[k][0], 128), n)

        def body(i, _):
            rows = pl.ds(pl.multiple_of(i * 16, 16), 16)
            g = gate_ref[rows, cs].astype(F32)
            u = up_ref[rows, cs].astype(F32)
            h = hg[rows, 0:n]
            s = jax.nn.sigmoid(g)
            gg_ref[rows, cs] = (h * u * s * (1.0 + g * (1.0 - s))).astype(BF)
            ug_ref[rows, cs] = (h * g * s).astype(BF)
            return 0

        lax.fori_loop(0, TOK // 16, body, 0)

    for side in K.co:
        for k in K.ABC:
            S[f"lo_{side}{k}"] = lambda side=side, k=k: lo(side, k)
            S[f"hg_{side}{k}"] = lambda side=side, k=k: hgrad(side, k)

    @step
    def losend():
        lo_s[...] = acc[:, pl.ds(pl.multiple_of((1 - r) * 512, 128), 512)].astype(BF)
        sends(K.losend, [(K.lo, lo_s, lo_r, dr)])

    @step
    def lofin():
        recv(K.lo, lo_r, dr)
        out_ref[...] = (
            acc[:, pl.ds(pl.multiple_of(r * 512, 128), 512)] + lo_r[...].astype(F32)
        ).astype(BF)

    def update(half, g):
        cs = pl.ds(pl.multiple_of(half * HALF, 128), HALF)
        g = g / jnp.float32(32768)
        m = master_ref[:, cs]
        first = 0.9 * one_ref[:, cs] + 0.1 * g
        second = 0.95 * two_ref[:, cs] + 0.05 * g * g
        upd = first / (1.0 - first_power) / (jnp.sqrt(second / (1.0 - second_power)) + 1e-08)
        master_out[:, cs] = m - 0.003 * (upd + 0.1 * m)
        one_out[:, cs] = first
        two_out[:, cs] = second

    @step
    def fin_():
        loc[K.one].wait()
        loc[K.two].wait()
        sends(K.fin, [(K.fin, fin.at[pl.ds(pl.multiple_of(oc * 8, 8), 8)], finP, dc)])
        update(c, fin[pl.ds(pl.multiple_of(c * 8, 8), 8), :])

    @step
    def adam():
        recv(K.fin, finP, dc)
        update(oc, finP[...])

    loc[K.master].wait()
    with jax.named_scope(K.barrier):
        pl.semaphore_wait(bar, len(peers))
    for n in ORDER:
        with jax.named_scope(n):
            S.pop(n)()
    assert not S, S.keys()
    with jax.named_scope(K.sends_done):
        for d in sent:
            d.wait_send()
    assert len(slots) <= NSEM, len(slots)


NSEM = 144


def copy_kernel(*refs):
    src, dst, sem = refs[0:6], refs[6:12], refs[12]
    copies = [pltpu.make_async_copy(src[i], dst[i], sem.at[i]) for i in range(6)]
    for d in copies:
        d.start()
    for d in copies:
        d.wait()


def on_device(gate_pre, up_pre, out_grad, master, moment_one, moment_two):
    V = pltpu.VMEM

    def in_hbm(a):
        return pltpu.with_memory_space_constraint(a, pltpu.HBM)

    nA, nB, nC = A[1], B[1], C[1]
    outs = pl.pallas_call(
        kernel,
        out_shape=(
            V((TOK, 512), BF),
            V((TOK, FF), BF),
            V((TOK, FF), BF),
            V((8, FF), F32),
            V((8, FF), F32),
            V((8, FF), F32),
        ),
        in_specs=[pl.BlockSpec(memory_space=pltpu.HBM)] * 6,
        out_specs=[pl.BlockSpec(memory_space=V)] * 6,
        scratch_shapes=[
            V((TOK, FF), BF), V((TOK, FF), BF), V((TOK, D), BF),
            V((8, FF), F32), V((8, FF), F32), V((8, FF), F32),
            V((NC, NY, NX, NZ, 16, HALF), BF),
            V((NY, NX, NZ, 16, HALF), F32),
            V((2 * TOK, HALF), BF),
            V((TOK, HALF), BF),
            V((TOK, D), BF),
            V((4, 256, 2 * TOK), BF),
            V((8, HALF), F32),
            V((TOK, 512), F32),
            V((TOK, D), F32),
            V((16, HALF), F32),
            V((8, HALF), F32),
            V((TOK, 512), BF),
            V((TOK, 512), BF),
            V((2, 2, NX, 16, nA), BF), V((2, 2, NX, 16, nA), BF),
            V((2, 3, 2, 2, NX, 16, nA), BF), V((2, 3, 2, 2, NX, 16, nA), BF),
            V((NY, NX, 16, nA), BF), V((3, NX, 16, nA), BF),
            V((NX, 16, nA), BF), V((16, nA), BF),
            V((NX, NZ, 16, nB), BF), V((2, NZ, 16, nB), BF),
            V((2, NX, NZ, 16, nB), BF), V((2, NX, NZ, 16, nB), BF),
            V((NZ, 16, nB), BF), V((NZ, 16, nB), BF),
            V((NZ, 16, nB), BF), V((7, 16, nB), BF),
            V((NY, NZ, 16, nC), BF), V((NY, NZ, 16, nC), BF),
            V((NZ, 16, nC), BF), V((2, 4, 16, nC), BF),
            V((2, NZ, 16, nC), BF), V((2, NZ, 16, nC), BF),
            V((NZ, 16, nC), BF), V((7, 16, nC), BF),
            pltpu.SemaphoreType.DMA((NSEM,)),
            pltpu.SemaphoreType.DMA((NSEM,)),
            pltpu.SemaphoreType.DMA((24,)),
        ],
        compiler_params=pltpu.CompilerParams(
            collective_id=0, has_side_effects=True, vmem_limit_bytes=48_000_000
        ),
    )(
        in_hbm(gate_pre.reshape(TOK, FF)),
        in_hbm(up_pre.reshape(TOK, FF)),
        in_hbm(out_grad.reshape(TOK, D)),
        in_hbm(master),
        in_hbm(moment_one),
        in_hbm(moment_two),
    )
    outs = pl.pallas_call(
        copy_kernel,
        out_shape=tuple(jax.ShapeDtypeStruct(o.shape, o.dtype) for o in outs),
        in_specs=[pl.BlockSpec(memory_space=V)] * 6,
        out_specs=[pl.BlockSpec(memory_space=pl.ANY)] * 6,
        scratch_shapes=[pltpu.SemaphoreType.DMA((6,))],
    )(*[pltpu.with_memory_space_constraint(o, V) for o in outs])
    lo, gg, ug, mn, m1, m2 = outs
    return (
        lo.reshape(2, 128, 512),
        gg.reshape(2, 128, FF),
        ug.reshape(2, 128, FF),
        mn,
        m1,
        m2,
    )


def solution(mesh):
    torus = Mesh(
        mesh.devices.reshape(NY, NX, NZ, NC, mesh.shape["rep"]),
        ("dp_0", "dp_1", "dp_2", "dp_3", "rep"),
    )
    return jax.shard_map(
        on_device,
        mesh=torus,
        in_specs=(
            P(None, DP, "rep"),
            P(None, DP, "rep"),
            P(None, DP, None),
            P(DP, "rep"),
            P(DP, "rep"),
            P(DP, "rep"),
        ),
        out_specs=(
            P(None, DP, "rep"),
            P(None, DP, "rep"),
            P(None, DP, "rep"),
            P(DP, "rep"),
            P(DP, "rep"),
            P(DP, "rep"),
        ),
        check_vma=False,
    )
```

```python
import math

import jax
import jax.numpy as jnp
from jax import lax
from jax.experimental import pallas as pl
from jax.experimental.pallas import tpu as pltpu
from jax.sharding import Mesh
from jax.sharding import PartitionSpec as P

DP = ("dp_0", "dp_1", "dp_2", "dp_3")
NY, NX, NZ, NC = 4, 2, 8, 2

first_power = 2.6561398887587544e-05
second_power = 0.005920529220333997

F32 = jnp.float32
BF = jnp.bfloat16
D = 1024
FF = 2816
HALF = 1408
TOK = 256
A = (0, 512)
B = (512, 512)
C = (1024, 384)
BC = (512, 896)


def cols(r):
    return pl.ds(r[0], r[1])


class Names:
    def __getattr__(self, word):
        return word


K = Names()

ORDER = (
    K.init, K.hidO_, K.hid2_, K.gp, K.gC, K.RC1, K.A1, K.gB, K.RB1, K.gA, K.RA1, K.BC1, K.A2,
    K.RA3R1, K.RA2L1, K.A3_1R1, K.A3_1L0, K.A3_1R0, K.RA3R0, K.A3_1L1, K.RA2L0, K.C2L, K.A3_2L0,
    K.C2R, K.B2, K.A3_2L1, K.RB2L, K.B3R, K.RA4R0, K.A3_3L0, K.RB2R, K.RA3L0, K.A3_3L1, K.B3L,
    K.A3_2R1, K.A3_2R0, K.RA3L1, K.RC2, K.C3, K.RB3, K.RA4R1, K.RA4L0, K.C4, K.lo_cC, K.A6,
    K.B4, K.lo_cB, K.RC2b, K.RA4L1, K.lo_cA, K.lo_oC, K.RC2c, K.lo_oA, K.RB4, K.lo_oB, K.losend,
    K.RC3R, K.RC3L, K.RA5, K.RC4, K.hg_oB0, K.hg_oB1, K.hg_oA1, K.hg_oC1, K.hg_cC0, K.hg_cA1,
    K.RA6, K.hg_oC0, K.hg_cB0, K.hg_oA0, K.hg_cC1, K.hg_cB1, K.hg_cA0, K.RB5, K.RC5, K.RA7,
    K.fin_, K.lofin, K.adam,
)
ORDS = {
    K.init: (K.Zd3, K.Zd5, K.Zd7, K.og, K.Zd4, K.Ax, K.Zd6, K.Zd2, K.Zd1,),
    K.A1: (K.Ay3, K.Ay1, K.Ay2,),
    K.A2: (K.Az1R1, K.DA0, K.Az1L0, K.Az1R0, K.Az1L1,),
    K.A3_1R0: (K.Az2R0, K.DA1R0,),
    K.A3_1R1: (K.DA1R1, K.Az2R1,),
    K.A3_1L0: (K.Az2L0, K.DA1L0,),
    K.A3_1L1: (K.Az2L1, K.DA1L1,),
    K.A3_2R0: (K.DA2R0, K.Az3R0,),
    K.A3_2R1: (K.DA2R1, K.Az3R1,),
    K.A3_2L0: (K.DA2L0, K.Az3L0,),
    K.A3_2L1: (K.Az3L1, K.DA2L1,),
    K.A3_3L0: (K.DA3L0, K.Az4L0,),
    K.A3_3L1: (K.Az4L1, K.DA3L1,),
    K.BC1: (K.DC0, K.Bx, K.Cx0, K.Cy1L, K.Cy1R, K.DB0, K.By1Rx, K.By1Lx,),
    K.B2: (K.By1Ro, K.DB1, K.By1Lo,),
    K.B3R: (K.By2R, K.DB2,),
    K.B3L: (K.By2L, K.DB3,),
    K.C2R: (K.Cx3, K.Cy2R, K.DC3,),
    K.C2L: (K.DC1, K.Cx1, K.Cy2L,),
    K.C3: (K.Cx2, K.DC2,),
    K.RC1: (K.rCx3, K.rCx2, K.rCx1, K.rCx0,),
    K.RB1: (K.rB1R, K.rB2R1, K.rB2L1, K.rB1L,),
    K.RA1: (K.rA2R1, K.rA2R0, K.rA1L0, K.rA1L1,),
    K.RA5: (K.rAy1, K.rAy2, K.rAy3,),
    K.RB4: (K.rBz3, K.rBz5, K.rBz7, K.rBz6, K.rBz2, K.rBz1, K.rBz4,),
    K.RC2: (K.rCy1R, K.rCy1L,),
    K.RC4: (K.rCz4, K.rCz3, K.rCz1, K.rCz7, K.rCz6, K.rCz2, K.rCz5,),
}


def kernel(
    gate_hbm, up_hbm, og_hbm, master_hbm, one_hbm, two_hbm,
    out_ref, gg_ref, ug_ref, master_out, one_out, two_out,
    gate_ref, up_ref, og_ref, master_ref, one_ref, two_ref,
    W, G, hid2, hidO, ogP, ogT, mP, hg, acc, fin, finP, lo_s, lo_r,
    sa1, ra1, sa2, ra2, sa3, ra3, sa4, ra4,
    sb1, rb1, sb2, rb2, sb3, rb3, sb4, rb4,
    sc1, rc1, sc2, rc2, sc3, rc3, sc4, rc4,
    space, ssem, rsem, lsem,
):
    y = lax.axis_index(K.dp_0)
    x = lax.axis_index(K.dp_1)
    z = lax.axis_index(K.dp_2)
    c = lax.axis_index(K.dp_3)
    r = lax.axis_index(K.rep)
    oc = 1 - c
    ox = 1 - x

    def dy(o):
        return {K.dp_0: lax.rem(y + (o % NY), NY)}

    def dz(o):
        return {K.dp_2: lax.rem(z + (o % NZ), NZ)}

    def zz(o):
        return lax.rem(z + (o % NZ), NZ)

    def yy(o):
        return lax.rem(y + (o % NY), NY)

    dx = {K.dp_1: ox}
    dc = {K.dp_3: oc}
    dr = {K.rep: 1 - r}
    allr = slice(None)

    peers = [dc, dx, dr] + [dy(o) for o in range(1, NY)] + [dz(o) for o in range(1, NZ)]
    bar = pltpu.get_barrier_semaphore()
    for p in peers:
        pl.semaphore_signal(bar, inc=1, device_id=p, device_id_type=pl.DeviceIdType.MESH)

    loc = {}

    def local(name, src, dst):
        d = pltpu.make_async_copy(src, dst, lsem.at[len(loc)])
        d.start()
        loc[name] = d

    local(K.master, master_hbm, master_ref)
    local(K.og, og_hbm, og_ref)
    local(K.gate, gate_hbm, gate_ref)
    local(K.up, up_hbm, up_ref)
    local(K.one, one_hbm, one_ref)
    local(K.two, two_hbm, two_ref)

    slots, sent, arriving = {}, {}, {}

    def size(ref):
        return math.prod(ref.shape) * ref.dtype.itemsize

    def rc(name, src, dst, dev):
        group = group_of(name)
        k = slots.setdefault(group, len(slots))
        sent.setdefault(size(src), 0)
        return pltpu.make_async_remote_copy(
            src_ref=src, dst_ref=dst, send_sem=ssem.at[list(sent).index(size(src))],
            recv_sem=rsem.at[k], device_id=dev, device_id_type=pl.DeviceIdType.MESH,
        )

    def tiles(total):
        return space.at[pl.ds(0, total // 4096)]

    def recv_all(group):
        n = arriving[group]
        with jax.named_scope(K.wait_ + group):
            rc(group, tiles(n), tiles(n), dc).wait_recv()

    def sends(step, items):
        names = ORDS.get(step, tuple(i[0] for i in items))
        table = {i[0]: i for i in items}
        for n in names:
            table[n]
        for name in list(names) + [n for n in table if n not in names]:
            _, src, dst, dev = table[name]
            rc(name, src, dst, dev).start()
            sent[size(src)] += 1
            arriving[group_of(name)] = arriving.get(group_of(name), 0) + size(dst)

    def recv(name, dst, dev):
        with jax.named_scope(K.wait_ + name):
            rc(name, dst, dst, dev).wait_recv()

    def hidden_rows(half, out):
        off = pl.multiple_of(half * HALF, 128)

        def body(i, _):
            rows = pl.ds(pl.multiple_of(i * 16, 16), 16)
            g = gate_ref[rows, pl.ds(off, HALF)].astype(F32)
            u = up_ref[rows, pl.ds(off, HALF)].astype(F32)
            s = jax.nn.sigmoid(g)
            out[rows, :] = (g * s * u).astype(BF)
            return 0

        lax.fori_loop(0, TOK // 16, body, 0)

    def Wb(*idx):
        return W.at[(c,) + idx]

    def same(name, ref, dev):
        return (name, ref, ref, dev)

    S = {}

    def step(f):
        S[f.__name__] = f
        return f

    @step
    def init():
        sends(K.i0, [(K.m, master_ref.at[:, pl.ds(pl.multiple_of(oc * HALF, 128), HALF)], mP, dc)])
        recv(K.m, mP, dc)
        mine = master_ref[:, pl.ds(pl.multiple_of(c * HALF, 128), HALF)]
        theirs = mP[...]
        first_core = c == 0
        W[c, y, x, z] = jnp.concatenate(
            [jnp.where(first_core, mine, theirs), jnp.where(first_core, theirs, mine)], axis=0
        ).astype(BF)
        loc[K.og].wait()
        items = [
            (K.og, og_ref, ogP, dc),
            same(K.Ax, Wb(y, x, z, allr, cols(A)), dx),
        ]
        for o in (4, 3, 5, 2, 6, 1, 7):
            items.append(same(f"Zd{o}", Wb(y, x, z, allr, cols(BC)), dz(o)))
        sends(K.init, items)

    @step
    def hidO_():
        loc[K.gate].wait()
        loc[K.up].wait()
        hidden_rows(oc, hidO)
        sends(K.h, [(K.h, hidO, hid2.at[pl.ds(TOK, TOK)], dc)])

    @step
    def hid2_():
        hidden_rows(c, hid2)
        for b in range(4):
            ogT[b, :, 0:TOK] = og_ref[:, b * 256 : (b + 1) * 256].T

    @step
    def A1():
        recv(K.Ax, Wb(y, ox, z, allr, cols(A)), dx)
        ref = Wb(y, allr, z, allr, cols(A))
        sends(K.A1, [same(f"Ay{o}", ref, dy(o)) for o in (2, 1, 3)])

    def az(h, zi):
        return Wb(pl.ds(2 * h, 2), allr, zi, allr, cols(A))

    @step
    def A2():
        recv_all(K.Ay)
        sends(K.A2, [
            same(K.Az1L0, az(0, z), dz(-1)),
            same(K.Az1R0, az(0, z), dz(1)),
            same(K.Az1L1, az(1, z), dz(-1)),
            same(K.Az1R1, az(1, z), dz(1)),
            same(K.DA0, Wb(allr, allr, z, allr, cols(A)), dc),
        ])

    def a3(s, sd, h):
        sg = 1 if sd == K.R else -1
        ref = az(h, zz(-sg * s))
        nm = f"{s}{sd}{h}"

        def f():
            recv(K.Az + nm, ref, dz(-sg))
            sends(K.A3_ + nm, [same(f"Az{s + 1}{sd}{h}", ref, dz(sg)), same(K.DA + nm, ref, dc)])

        S[K.A3_ + nm] = f

    last_a = (("3R0", 0, -3), ("3R1", 1, -3), ("4L0", 0, 4), ("4L1", 1, 4))
    for s in (1, 2, 3):
        for h in (0, 1):
            a3(s, K.L, h)
            if s < 3:
                a3(s, K.R, h)

    @step
    def A6():
        recv_all(K.Az9)
        sends(K.A6, [same(K.DA + nm, az(h, zz(o)), dc) for nm, h, o in last_a])

    def bref(yi, xi):
        return Wb(yi, xi, allr, allr, cols(B))

    def cref(yi, xi, zs=allr):
        return Wb(yi, xi, zs, allr, cols(C))

    @step
    def BC1():
        recv_all(K.Zd)
        b, cc = bref(y, x), cref(y, x)
        sends(K.BC1, [
            same(K.Bx, b, dx), same(K.By1Rx, b, dy(1)), same(K.By1Lx, b, dy(-1)),
            same(K.Cy1R, cc, dy(1)), same(K.Cy1L, cc, dy(-1)), same(K.Cx0, cc, dx),
            same(K.DB0, b, dc), same(K.DC0, cc, dc),
        ])

    @step
    def B2():
        b = bref(y, ox)
        recv(K.Bx, b, dx)
        sends(K.B2, [same(K.By1Ro, b, dy(1)), same(K.By1Lo, b, dy(-1)), same(K.DB1, b, dc)])

    @step
    def B3R():
        b = bref(yy(-1), x)
        recv(K.By1Rx, b, dy(-1))
        sends(K.B3R, [same(K.By2R, b, dy(1)), same(K.DB2, b, dc)])

    @step
    def B3L():
        b = bref(yy(1), ox)
        recv(K.By1Lo, b, dy(1))
        sends(K.B3L, [same(K.By2L, b, dy(-1)), same(K.DB3, b, dc)])

    last_b = ((K.By2R, 2, x, -1), (K.By2L, 2, ox, 1), (K.By1Ro, -1, ox, -1), (K.By1Lx, 1, x, 1))

    @step
    def B4():
        recv_all(K.By9)
        sends(K.B4, [same(K.D + nm, bref(yy(o), xi), dc) for nm, o, xi, d in last_b])

    lo4, hi4 = pl.ds(0, 4), pl.ds(4, 4)

    @step
    def C2R():
        recv(K.Cy1R, cref(yy(-1), x), dy(-1))
        sends(K.C2R, [
            same(K.Cy2R, cref(yy(-1), x, lo4), dy(1)),
            same(K.Cx3, cref(yy(-1), x), dx), same(K.DC3, cref(yy(-1), x), dc),
        ])

    @step
    def C2L():
        recv(K.Cy1L, cref(yy(1), x), dy(1))
        sends(K.C2L, [
            same(K.Cy2L, cref(yy(1), x, hi4), dy(-1)),
            same(K.Cx1, cref(yy(1), x), dx), same(K.DC1, cref(yy(1), x), dc),
        ])

    @step
    def C3():
        recv_all(K.Cy2)
        sends(K.C3, [same(K.Cx2, cref(yy(2), x), dx), same(K.DC2, cref(yy(2), x), dc)])

    @step
    def C4():
        recv_all(K.Cx)
        sends(K.C4, [same(f"DCx{o}", cref(yy(o), ox), dc) for o in (0, 1, 3, 2)])

    @step
    def gp():
        recv(K.og, ogP, dc)
        for b in range(4):
            ogT[b, :, TOK : 2 * TOK] = ogP[:, b * 256 : (b + 1) * 256].T
        recv(K.h, hid2.at[pl.ds(TOK, TOK)], dc)

    def grads(cr):
        for c0 in range(cr[0], cr[0] + cr[1], 256):
            n = min(256, cr[0] + cr[1] - c0)
            p = jnp.dot(
                ogT[...].reshape(D, 2 * TOK), hid2[:, pl.ds(c0, n)], preferred_element_type=F32
            )
            G[:, :, :, :, pl.ds(c0, n)] = p.reshape(NY, NX, NZ, 16, n)

    S[K.gA] = lambda: grads(A)
    S[K.gB] = lambda: grads(B)
    S[K.gC] = lambda: grads(C)

    def ga(h, zi):
        return G[2 * h : 2 * h + 2, :, zi, :, cols(A)]

    @step
    def RA1():
        for h in (0, 1):
            sa1[h] = ga(h, zz(4)).astype(BF)
            sa2[0, 0, h] = ga(h, zz(3)).astype(BF)
        sends(K.RA1, [
            (K.rA1L0, sa1.at[0], ra1.at[0], dz(-1)),
            (K.rA1L1, sa1.at[1], ra1.at[1], dz(-1)),
            (K.rA2R0, sa2.at[0, 0, 0], ra2.at[0, 0, 0], dz(1)),
            (K.rA2R1, sa2.at[0, 0, 1], ra2.at[0, 0, 1], dz(1)),
        ])

    def ra(s, sd, h):
        sg = 1 if sd == K.R else -1
        side = 0 if sd == K.R else 1

        def f():
            buf = ra1.at[h] if s == 2 else ra2.at[side, s - 3, h]
            recv(f"rA{s - 1}{sd}{h}", buf, dz(-sg))
            sa2[side, s - 2, h] = (ga(h, zz(sg * (5 - s))) + buf[...].astype(F32)).astype(BF)
            sends(K.RA, [(f"rA{s}{sd}{h}", sa2.at[side, s - 2, h], ra2.at[side, s - 2, h], dz(sg))])

        S[f"RA{s}{sd}{h}"] = f

    for sd in K.RL:
        for h in (0, 1):
            for s in range(2 if sd == K.L else 3, 5):
                ra(s, sd, h)

    @step
    def RA5():
        recv_all(K.rA4)
        for h in (0, 1):
            t = ga(h, z) + ra2[0, 2, h].astype(F32) + ra2[1, 2, h].astype(F32)
            G[2 * h : 2 * h + 2, :, z, :, cols(A)] = t
            sa3[2 * h : 2 * h + 2] = t.astype(BF)
        sends(K.RA5, [(f"rAy{o}", sa3.at[yy(o)], ra3.at[o - 1], dy(o)) for o in (2, 1, 3)])

    @step
    def RA6():
        recv_all(K.rAy)
        t = G[y, :, z, :, cols(A)]
        for o in (1, 2, 3):
            t = t + ra3[o - 1].astype(F32)
        G[y, :, z, :, cols(A)] = t
        sa4[...] = t.astype(BF)
        sends(K.RA6, [(K.rAx, sa4.at[ox], ra4, dx)])

    @step
    def RA7():
        recv(K.rAx, ra4, dx)
        fin[:, cols(A)] = G[y, x, z, :, cols(A)] + ra4[...].astype(F32)

    def gb(yi, xi):
        return G[yi, xi, :, :, cols(B)]

    @step
    def RB1():
        sb1[0] = gb(yy(2), x).astype(BF)
        sb1[1] = gb(yy(2), ox).astype(BF)
        sb2[0, 1] = gb(yy(1), ox).astype(BF)
        sb2[1, 0] = gb(yy(-1), x).astype(BF)
        sends(K.RB1, [
            (K.rB1R, sb1.at[0], rb1.at[0], dy(1)), (K.rB1L, sb1.at[1], rb1.at[1], dy(-1)),
            (K.rB2R1, sb2.at[0, 1], rb2.at[0, 1], dy(1)),
            (K.rB2L1, sb2.at[1, 0], rb2.at[1, 0], dy(-1)),
        ])

    @step
    def RB2R():
        recv(K.rB1R, rb1.at[0], dy(-1))
        sb2[0, 0] = (gb(yy(1), x) + rb1[0].astype(F32)).astype(BF)
        sends(K.RB2R, [(K.rB2R0, sb2.at[0, 0], rb2.at[0, 0], dy(1))])

    @step
    def RB2L():
        recv(K.rB1L, rb1.at[1], dy(1))
        sb2[1, 1] = (gb(yy(-1), ox) + rb1[1].astype(F32)).astype(BF)
        sends(K.RB2L, [(K.rB2L0, sb2.at[1, 1], rb2.at[1, 1], dy(-1))])

    @step
    def RB3():
        recv_all(K.rB3)
        sb3[...] = (gb(y, ox) + rb2[0, 1].astype(F32) + rb2[1, 1].astype(F32)).astype(BF)
        sends(K.RB3, [(K.rBx, sb3, rb3, dx)])

    @step
    def RB4():
        recv_all(K.rB4)
        t = gb(y, x) + rb2[0, 0].astype(F32) + rb2[1, 0].astype(F32) + rb3[...].astype(F32)
        G[y, x, :, :, cols(B)] = t
        sb4[...] = t.astype(BF)
        sends(K.RB4, [(f"rBz{o}", sb4.at[zz(o)], rb4.at[o - 1], dz(o)) for o in (4, 3, 5, 2, 6, 1, 7)])

    @step
    def RB5():
        t = G[y, x, z, :, cols(B)]
        recv_all(K.rBz)
        for o in range(1, NZ):
            t = t + rb4[o - 1].astype(F32)
        fin[:, cols(B)] = t

    def gc(yi, xi, zs=allr):
        return G[yi, xi, zs, :, cols(C)]

    @step
    def RC1():
        items = []
        for o in (2, 1, 3, 0):
            sc1[o] = gc(yy(o), ox).astype(BF)
            items.append((f"rCx{o}", sc1.at[o], rc1.at[o], dx))
        sends(K.RC1, items)

    @step
    def RC2():
        recv(K.rCx2, rc1.at[2], dx)
        sc2[...] = (gc(yy(2), x) + rc1[2].astype(F32)).astype(BF)
        sends(K.RC2, [
            (K.rCy1R, sc2.at[lo4], rc2.at[0], dy(1)), (K.rCy1L, sc2.at[hi4], rc2.at[1], dy(-1)),
        ])

    @step
    def RC2b():
        recv(K.rCx1, rc1.at[1], dx)
        t = gc(yy(1), x) + rc1[1].astype(F32)
        G[yy(1), x, :, :, cols(C)] = t
        sc3[0, 4:8] = t[4:8].astype(BF)
        sends(K.RC2b, [(K.rCy2R1, sc3.at[0, hi4], rc3.at[0, hi4], dy(1))])

    @step
    def RC2c():
        recv(K.rCx3, rc1.at[3], dx)
        t = gc(yy(3), x) + rc1[3].astype(F32)
        G[yy(3), x, :, :, cols(C)] = t
        sc3[1, 0:4] = t[0:4].astype(BF)
        sends(K.RC2c, [(K.rCy2L1, sc3.at[1, lo4], rc3.at[1, lo4], dy(-1))])

    @step
    def RC3R():
        recv(K.rCy1R, rc2.at[0], dy(-1))
        sc3[0, 0:4] = (gc(yy(1), x, slice(0, 4)) + rc2[0].astype(F32)).astype(BF)
        sends(K.RC3R, [(K.rCy2R0, sc3.at[0, lo4], rc3.at[0, lo4], dy(1))])

    @step
    def RC3L():
        recv(K.rCy1L, rc2.at[1], dy(1))
        sc3[1, 4:8] = (gc(yy(3), x, slice(4, 8)) + rc2[1].astype(F32)).astype(BF)
        sends(K.RC3L, [(K.rCy2L0, sc3.at[1, hi4], rc3.at[1, hi4], dy(-1))])

    @step
    def RC4():
        recv_all(K.rC4)
        t = gc(y, x) + rc1[0].astype(F32) + rc3[0].astype(F32) + rc3[1].astype(F32)
        G[y, x, :, :, cols(C)] = t
        sc4[...] = t.astype(BF)
        sends(K.RC4, [(f"rCz{o}", sc4.at[zz(o)], rc4.at[o - 1], dz(o)) for o in (4, 3, 5, 2, 6, 1, 7)])

    @step
    def RC5():
        t = G[y, x, z, :, cols(C)]
        recv_all(K.rCz)
        for o in range(1, NZ):
            t = t + rc4[o - 1].astype(F32)
        fin[:, cols(C)] = t

    ranges = {K.A: A, K.B: B, K.C: C}
    have = set()
    started = []

    def w_of(side, k, c0, n):
        if side == K.o and k not in have:
            have.add(k)
            recv_all(K.D + k)
        half = c if side == K.c else oc
        return W[half, :, :, :, :, pl.ds(c0, n)].reshape(D, n)

    def lo(side, k):
        w = w_of(side, k, *ranges[k])
        h = (hid2 if side == K.c else hidO)[0:TOK, cols(ranges[k])]
        part = lax.dot_general(h, w, (((1,), (1,)), ((), ())), preferred_element_type=F32)
        if started:
            acc[...] += part
        else:
            acc[...] = part
        started.append(1)

    def hgrad(side, k, j):
        c0 = ranges[k][0] + 256 * j
        n = min(256, ranges[k][1] - 256 * j)
        half = c if side == K.c else oc
        hg[:, 0:n] = jnp.dot(og_ref[...], w_of(side, k, c0, n), preferred_element_type=F32)
        cs = pl.ds(pl.multiple_of(half * HALF + c0, 128), n)

        def body(i, _):
            rows = pl.ds(pl.multiple_of(i * 16, 16), 16)
            g = gate_ref[rows, cs].astype(F32)
            u = up_ref[rows, cs].astype(F32)
            h = hg[rows, 0:n]
            s = jax.nn.sigmoid(g)
            gg_ref[rows, cs] = (h * u * s * (1.0 + g * (1.0 - s))).astype(BF)
            ug_ref[rows, cs] = (h * g * s).astype(BF)
            return 0

        lax.fori_loop(0, TOK // 16, body, 0)

    for side in K.co:
        for k in K.ABC:
            S[f"lo_{side}{k}"] = lambda side=side, k=k: lo(side, k)
            for j in range(-(-ranges[k][1] // 256)):
                S[f"hg_{side}{k}{j}"] = lambda side=side, k=k, j=j: hgrad(side, k, j)

    @step
    def losend():
        lo_s[...] = acc[:, pl.ds(pl.multiple_of((1 - r) * 512, 128), 512)].astype(BF)
        sends(K.losend, [(K.lo, lo_s, lo_r, dr)])

    @step
    def lofin():
        recv(K.lo, lo_r, dr)
        out_ref[...] = (
            acc[:, pl.ds(pl.multiple_of(r * 512, 128), 512)] + lo_r[...].astype(F32)
        ).astype(BF)

    def update(half, g):
        cs = pl.ds(pl.multiple_of(half * HALF, 128), HALF)
        g = g / jnp.float32(32768)
        m = master_ref[:, cs]
        first = 0.9 * one_ref[:, cs] + 0.1 * g
        second = 0.95 * two_ref[:, cs] + 0.05 * g * g
        upd = first / (1.0 - first_power) / (jnp.sqrt(second / (1.0 - second_power)) + 1e-08)
        master_out[:, cs] = m - 0.003 * (upd + 0.1 * m)
        one_out[:, cs] = first
        two_out[:, cs] = second

    @step
    def fin_():
        loc[K.one].wait()
        loc[K.two].wait()
        sends(K.fin, [(K.fin, fin.at[pl.ds(pl.multiple_of(oc * 8, 8), 8)], finP, dc)])
        update(c, fin[pl.ds(pl.multiple_of(c * 8, 8), 8), :])

    @step
    def adam():
        recv(K.fin, finP, dc)
        update(oc, finP[...])

    loc[K.master].wait()
    with jax.named_scope(K.barrier):
        pl.semaphore_wait(bar, len(peers))
    for n in ORDER:
        with jax.named_scope(n):
            S.pop(n)()
    assert not S, S.keys()
    with jax.named_scope(K.sends_done):
        for n, many in sent.items():
            if many:
                pltpu.make_async_remote_copy(
                    src_ref=tiles(n * many), dst_ref=tiles(n * many),
                    send_sem=ssem.at[list(sent).index(n)], recv_sem=rsem.at[0],
                    device_id=dc, device_id_type=pl.DeviceIdType.MESH,
                ).wait_send()
    assert len(slots) <= NRECV and len(sent) <= NSEND, (len(slots), len(sent))


NRECV, NSEND = 56, 20

GROUPS = {}
for _first, _names in (
    (K.Az9, (K.Az3R0, K.Az3R1, K.Az4L0, K.Az4L1)),
    (K.By9, (K.By2R, K.By2L, K.By1Ro, K.By1Lx)),
    (K.rB4, (K.rB2R0, K.rB2L1, K.rBx)),
    (K.rB3, (K.rB2R1, K.rB2L0)),
    (K.rC4, (K.rCx0, K.rCy2R0, K.rCy2R1, K.rCy2L0, K.rCy2L1)),
    (K.Cy2, (K.Cy2R, K.Cy2L)),
):
    for _n in _names:
        GROUPS[_n] = _first


def group_of(name):
    if name in GROUPS:
        return GROUPS[name]
    for p in (K.Zd, K.Ay, K.rAy, K.rBz, K.rCz, K.DA, K.DB, K.DC, K.Cx, K.rA4):
        if name.startswith(p):
            return p
    return name


def copy_kernel(*refs):
    src, dst, sem = refs[0:6], refs[6:12], refs[12]
    copies = [pltpu.make_async_copy(src[i], dst[i], sem.at[i]) for i in range(6)]
    for d in copies:
        d.start()
    for d in copies:
        d.wait()


def on_device(gate_pre, up_pre, out_grad, master, moment_one, moment_two):
    V = pltpu.VMEM

    def in_hbm(a):
        return pltpu.with_memory_space_constraint(a, pltpu.HBM)

    nA, nB, nC = A[1], B[1], C[1]
    outs = pl.pallas_call(
        kernel,
        out_shape=(
            V((TOK, 512), BF),
            V((TOK, FF), BF),
            V((TOK, FF), BF),
            V((8, FF), F32),
            V((8, FF), F32),
            V((8, FF), F32),
        ),
        in_specs=[pl.BlockSpec(memory_space=pltpu.HBM)] * 6,
        out_specs=[pl.BlockSpec(memory_space=V)] * 6,
        scratch_shapes=[
            V((TOK, FF), BF), V((TOK, FF), BF), V((TOK, D), BF),
            V((8, FF), F32), V((8, FF), F32), V((8, FF), F32),
            V((NC, NY, NX, NZ, 16, HALF), BF),
            V((NY, NX, NZ, 16, HALF), F32),
            V((2 * TOK, HALF), BF),
            V((TOK, HALF), BF),
            V((TOK, D), BF),
            V((4, 256, 2 * TOK), BF),
            V((8, HALF), F32),
            V((TOK, 512), F32),
            V((TOK, D), F32),
            V((16, HALF), F32),
            V((8, HALF), F32),
            V((TOK, 512), BF),
            V((TOK, 512), BF),
            V((2, 2, NX, 16, nA), BF), V((2, 2, NX, 16, nA), BF),
            V((2, 3, 2, 2, NX, 16, nA), BF), V((2, 3, 2, 2, NX, 16, nA), BF),
            V((NY, NX, 16, nA), BF), V((3, NX, 16, nA), BF),
            V((NX, 16, nA), BF), V((16, nA), BF),
            V((NX, NZ, 16, nB), BF), V((2, NZ, 16, nB), BF),
            V((2, NX, NZ, 16, nB), BF), V((2, NX, NZ, 16, nB), BF),
            V((NZ, 16, nB), BF), V((NZ, 16, nB), BF),
            V((NZ, 16, nB), BF), V((7, 16, nB), BF),
            V((NY, NZ, 16, nC), BF), V((NY, NZ, 16, nC), BF),
            V((NZ, 16, nC), BF), V((2, 4, 16, nC), BF),
            V((2, NZ, 16, nC), BF), V((2, NZ, 16, nC), BF),
            V((NZ, 16, nC), BF), V((7, 16, nC), BF),
            V((768, 16, 128), BF),
            pltpu.SemaphoreType.DMA((NSEND,)),
            pltpu.SemaphoreType.DMA((NRECV,)),
            pltpu.SemaphoreType.DMA((6,)),
        ],
        compiler_params=pltpu.CompilerParams(
            collective_id=0, has_side_effects=True, vmem_limit_bytes=48_000_000
        ),
    )(
        in_hbm(gate_pre.reshape(TOK, FF)),
        in_hbm(up_pre.reshape(TOK, FF)),
        in_hbm(out_grad.reshape(TOK, D)),
        in_hbm(master),
        in_hbm(moment_one),
        in_hbm(moment_two),
    )
    outs = pl.pallas_call(
        copy_kernel,
        out_shape=tuple(jax.ShapeDtypeStruct(o.shape, o.dtype) for o in outs),
        in_specs=[pl.BlockSpec(memory_space=V)] * 6,
        out_specs=[pl.BlockSpec(memory_space=pl.ANY)] * 6,
        scratch_shapes=[pltpu.SemaphoreType.DMA((6,))],
    )(*[pltpu.with_memory_space_constraint(o, V) for o in outs])
    lo, gg, ug, mn, m1, m2 = outs
    return (
        lo.reshape(2, 128, 512),
        gg.reshape(2, 128, FF),
        ug.reshape(2, 128, FF),
        mn,
        m1,
        m2,
    )


def solution(mesh):
    torus = Mesh(
        mesh.devices.reshape(NY, NX, NZ, NC, mesh.shape["rep"]),
        ("dp_0", "dp_1", "dp_2", "dp_3", "rep"),
    )
    return jax.shard_map(
        on_device,
        mesh=torus,
        in_specs=(
            P(None, DP, "rep"),
            P(None, DP, "rep"),
            P(None, DP, None),
            P(DP, "rep"),
            P(DP, "rep"),
            P(DP, "rep"),
        ),
        out_specs=(
            P(None, DP, "rep"),
            P(None, DP, "rep"),
            P(None, DP, "rep"),
            P(DP, "rep"),
            P(DP, "rep"),
            P(DP, "rep"),
        ),
        check_vma=False,
    )
```

```python
import math

import jax
import jax.numpy as jnp
from jax import lax
from jax.experimental import pallas as pl
from jax.experimental.pallas import tpu as pltpu
from jax.sharding import Mesh
from jax.sharding import PartitionSpec as P

DP = ("dp_0", "dp_1", "dp_2", "dp_3")
NY, NX, NZ, NC = 4, 2, 8, 2

first_power = 2.6561398887587544e-05
second_power = 0.005920529220333997

F32 = jnp.float32
BF = jnp.bfloat16
D = 1024
FF = 2816
HALF = 1408
TOK = 256
A = (0, 512)
B = (512, 512)
C = (1024, 384)
BC = (512, 896)


def cols(r):
    return pl.ds(r[0], r[1])


class Names:
    def __getattr__(self, word):
        return word


K = Names()

ORDER = (
    K.init, K.hidO_, K.hid2_, K.gp, K.gC0, K.gC1, K.RC1, K.A1, K.gB0, K.gB1, K.RB1, K.gA0,
    K.gA1, K.RA1, K.A2, K.RA2L0, K.BC1, K.RA3R1, K.A3_1L0, K.A3_1R1, K.RA2L1, K.RA3L0, K.A3_1R0,
    K.C2R, K.C2L, K.fc, K.A3_1L1, K.B2, K.RA3R0, K.RB2L, K.A3_2L0, K.A3_2L1, K.A3_2R1, K.RA4R0,
    K.A3_2R0, K.B3R, K.B3L, K.RC2, K.C3, K.A3_3L0, K.fo, K.A3_3L1, K.RA3L1, K.RB2R, K.RB3,
    K.RC2b, K.RC2c, K.C4, K.hg_cC0, K.RA4R1, K.lo_cC, K.RC3R, K.RA4L0, K.A6, K.B4, K.lo_oC,
    K.lo_cA, K.RA4L1, K.lo_cB, K.lo_oA, K.RB4, K.lo_oB, K.losend, K.RC3L, K.hg_oB0, K.hg_oA1,
    K.RA5, K.RC4, K.hg_cA1, K.hg_oB1, K.hg_cB0, K.hg_oC0, K.hg_cC1, K.RA6, K.hg_cA0, K.hg_cB1,
    K.RB5, K.hg_oA0, K.RA7, K.RC5, K.fin_, K.hg_oC1, K.lofin, K.adam,
)
ORDS = {
    K.init: (K.Zd7, K.Zd5, K.Zd6, K.Zd1, K.Ax, K.og, K.Zd3, K.Zd4, K.Zd2,),
    K.A1: (K.Ay3, K.Ay1, K.Ay2,),
    K.A2: (K.Az1L0, K.DA0, K.Az1R1, K.Az1L1, K.Az1R0,),
    K.A3_1R0: (K.DA1R0, K.Az2R0,),
    K.A3_1R1: (K.DA1R1, K.Az2R1,),
    K.A3_1L0: (K.DA1L0, K.Az2L0,),
    K.A3_1L1: (K.Az2L1, K.DA1L1,),
    K.A3_2R0: (K.Az3R0, K.DA2R0,),
    K.A3_2R1: (K.Az3R1, K.DA2R1,),
    K.A3_2L0: (K.DA2L0, K.Az3L0,),
    K.A3_2L1: (K.DA2L1, K.Az3L1,),
    K.A3_3L0: (K.Az4L0, K.DA3L0,),
    K.A3_3L1: (K.Az4L1, K.DA3L1,),
    K.BC1: (K.Bx, K.Cy1L, K.DC0, K.Cx0, K.DB0, K.By1Lx, K.Cy1R, K.By1Rx,),
    K.B2: (K.By1Ro, K.DB1, K.By1Lo,),
    K.B3R: (K.By2R, K.DB2,),
    K.B3L: (K.By2L, K.DB3,),
    K.C2R: (K.Cx3, K.DC3, K.Cy2R,),
    K.C2L: (K.DC1, K.Cy2L, K.Cx1,),
    K.C3: (K.Cx2, K.DC2,),
    K.RC1: (K.rCx0, K.rCx2, K.rCx1, K.rCx3,),
    K.RB1: (K.rB1L, K.rB2R1, K.rB2L1, K.rB1R,),
    K.RA1: (K.rA1L0, K.rA2R1, K.rA1L1, K.rA2R0,),
    K.RA5: (K.rAy2, K.rAy1, K.rAy3,),
    K.RB4: (K.rBz1, K.rBz5, K.rBz6, K.rBz7, K.rBz2, K.rBz3, K.rBz4,),
    K.RC2: (K.rCy1R, K.rCy1L,),
    K.RC4: (K.rCz7, K.rCz6, K.rCz4, K.rCz3, K.rCz1, K.rCz2, K.rCz5,),
}
HORDER = (K.C, K.B, K.A)


def kernel(
    gate_hbm, up_hbm, og_hbm, master_hbm, one_hbm, two_hbm,
    out_ref, gg_ref, ug_ref, master_out, one_out, two_out,
    gate_ref, up_ref, og_ref, master_ref, one_ref, two_ref,
    W, G, hid2, hidO, ogP, ogT, mP, fg, fu, acc, fin, finP, lo_s, lo_r,
    sa1, ra1, sa2, ra2, sa3, ra3, sa4, ra4,
    sb1, rb1, sb2, rb2, sb3, rb3, sb4, rb4,
    sc1, rc1, sc2, rc2, sc3, rc3, sc4, rc4,
    space, ssem, rsem, lsem,
):
    y = lax.axis_index(K.dp_0)
    x = lax.axis_index(K.dp_1)
    z = lax.axis_index(K.dp_2)
    c = lax.axis_index(K.dp_3)
    r = lax.axis_index(K.rep)
    oc = 1 - c
    ox = 1 - x

    def dy(o):
        return {K.dp_0: lax.rem(y + (o % NY), NY)}

    def dz(o):
        return {K.dp_2: lax.rem(z + (o % NZ), NZ)}

    def zz(o):
        return lax.rem(z + (o % NZ), NZ)

    def yy(o):
        return lax.rem(y + (o % NY), NY)

    dx = {K.dp_1: ox}
    dc = {K.dp_3: oc}
    dr = {K.rep: 1 - r}
    allr = slice(None)

    peers = [dc, dx, dr] + [dy(o) for o in range(1, NY)] + [dz(o) for o in range(1, NZ)]
    bar = pltpu.get_barrier_semaphore()
    for p in peers:
        pl.semaphore_signal(bar, inc=1, device_id=p, device_id_type=pl.DeviceIdType.MESH)

    loc = {}

    def local(name, src, dst):
        d = pltpu.make_async_copy(src, dst, lsem.at[len(loc)])
        d.start()
        loc[name] = d

    local(K.master, master_hbm, master_ref)
    local(K.og, og_hbm, og_ref)
    local(K.gate, gate_hbm, gate_ref)
    local(K.up, up_hbm, up_ref)
    local(K.one, one_hbm, one_ref)
    local(K.two, two_hbm, two_ref)

    slots, sent, arriving = {}, {}, {}

    def size(ref):
        return math.prod(ref.shape) * ref.dtype.itemsize

    def rc(name, src, dst, dev):
        group = group_of(name)
        k = slots.setdefault(group, len(slots))
        sent.setdefault(size(src), 0)
        return pltpu.make_async_remote_copy(
            src_ref=src, dst_ref=dst, send_sem=ssem.at[list(sent).index(size(src))],
            recv_sem=rsem.at[k], device_id=dev, device_id_type=pl.DeviceIdType.MESH,
        )

    def tiles(total):
        return space.at[pl.ds(0, total // 4096)]

    def recv_all(group):
        n = arriving[group]
        with jax.named_scope(K.wait_ + group):
            rc(group, tiles(n), tiles(n), dc).wait_recv()

    def sends(step, items):
        names = ORDS.get(step, tuple(i[0] for i in items))
        table = {i[0]: i for i in items}
        for n in names:
            table[n]
        for name in list(names) + [n for n in table if n not in names]:
            _, src, dst, dev = table[name]
            rc(name, src, dst, dev).start()
            sent[size(src)] += 1
            arriving[group_of(name)] = arriving.get(group_of(name), 0) + size(dst)

    def recv(name, dst, dev):
        with jax.named_scope(K.wait_ + name):
            rc(name, dst, dst, dev).wait_recv()

    def hidden_rows(half, out, cr):
        cs = pl.ds(pl.multiple_of(half * HALF + cr[0], 128), cr[1])

        def body(i, _):
            rows = pl.ds(pl.multiple_of(i * 32, 32), 32)
            g = gate_ref[rows, cs].astype(F32)
            u = up_ref[rows, cs].astype(F32)
            s = jax.nn.sigmoid(g)
            out[rows, cols(cr)] = (g * s * u).astype(BF)
            return 0

        lax.fori_loop(0, TOK // 32, body, 0)

    def factor_rows(half):
        cs = pl.ds(pl.multiple_of(half * HALF, 128), HALF)

        def body(i, _):
            rows = pl.ds(pl.multiple_of(i * 16, 16), 16)
            g = gate_ref[rows, cs].astype(F32)
            u = up_ref[rows, cs].astype(F32)
            s = jax.nn.sigmoid(g)
            fg[half, rows, :] = u * s * (1.0 + g * (1.0 - s))
            fu[half, rows, :] = g * s
            return 0

        lax.fori_loop(0, TOK // 16, body, 0)

    def Wb(*idx):
        return W.at[(c,) + idx]

    def same(name, ref, dev):
        return (name, ref, ref, dev)

    ranges = {K.A: A, K.B: B, K.C: C}
    S = {}

    def step(f):
        S[f.__name__] = f
        return f

    @step
    def init():
        sends(K.i0, [(K.m, master_ref.at[:, pl.ds(pl.multiple_of(oc * HALF, 128), HALF)], mP, dc)])
        recv(K.m, mP, dc)
        mine = master_ref[:, pl.ds(pl.multiple_of(c * HALF, 128), HALF)]
        theirs = mP[...]
        first_core = c == 0
        W[c, y, x, z] = jnp.concatenate(
            [jnp.where(first_core, mine, theirs), jnp.where(first_core, theirs, mine)], axis=0
        ).astype(BF)
        loc[K.og].wait()
        items = [
            (K.og, og_ref, ogP, dc),
            same(K.Ax, Wb(y, x, z, allr, cols(A)), dx),
        ]
        for o in (4, 3, 5, 2, 6, 1, 7):
            items.append(same(f"Zd{o}", Wb(y, x, z, allr, cols(BC)), dz(o)))
        sends(K.init, items)

    @step
    def hidO_():
        loc[K.gate].wait()
        loc[K.up].wait()
        for k in HORDER:
            cr = ranges[k]
            hidden_rows(oc, hidO, cr)
            sends(K.h, [(K.h + k, hidO.at[:, cols(cr)], hid2.at[pl.ds(TOK, TOK), cols(cr)], dc)])

    @step
    def hid2_():
        for k in HORDER:
            hidden_rows(c, hid2, ranges[k])
        for b in range(4):
            ogT[b, :, 0:TOK] = og_ref[:, b * 256 : (b + 1) * 256].T

    S[K.fo] = lambda: factor_rows(oc)
    S[K.fc] = lambda: factor_rows(c)

    @step
    def A1():
        recv(K.Ax, Wb(y, ox, z, allr, cols(A)), dx)
        ref = Wb(y, allr, z, allr, cols(A))
        sends(K.A1, [same(f"Ay{o}", ref, dy(o)) for o in (2, 1, 3)])

    def az(h, zi):
        return Wb(pl.ds(2 * h, 2), allr, zi, allr, cols(A))

    @step
    def A2():
        recv_all(K.Ay)
        sends(K.A2, [
            same(K.Az1L0, az(0, z), dz(-1)),
            same(K.Az1R0, az(0, z), dz(1)),
            same(K.Az1L1, az(1, z), dz(-1)),
            same(K.Az1R1, az(1, z), dz(1)),
            same(K.DA0, Wb(allr, allr, z, allr, cols(A)), dc),
        ])

    def a3(s, sd, h):
        sg = 1 if sd == K.R else -1
        ref = az(h, zz(-sg * s))
        nm = f"{s}{sd}{h}"

        def f():
            recv(K.Az + nm, ref, dz(-sg))
            sends(K.A3_ + nm, [same(f"Az{s + 1}{sd}{h}", ref, dz(sg)), same(K.DA + nm, ref, dc)])

        S[K.A3_ + nm] = f

    last_a = (("3R0", 0, -3), ("3R1", 1, -3), ("4L0", 0, 4), ("4L1", 1, 4))
    for s in (1, 2, 3):
        for h in (0, 1):
            a3(s, K.L, h)
            if s < 3:
                a3(s, K.R, h)

    @step
    def A6():
        recv_all(K.Az9)
        sends(K.A6, [same(K.DA + nm, az(h, zz(o)), dc) for nm, h, o in last_a])

    def bref(yi, xi):
        return Wb(yi, xi, allr, allr, cols(B))

    def cref(yi, xi, zs=allr):
        return Wb(yi, xi, zs, allr, cols(C))

    @step
    def BC1():
        recv_all(K.Zd)
        b, cc = bref(y, x), cref(y, x)
        sends(K.BC1, [
            same(K.Bx, b, dx), same(K.By1Rx, b, dy(1)), same(K.By1Lx, b, dy(-1)),
            same(K.Cy1R, cc, dy(1)), same(K.Cy1L, cc, dy(-1)), same(K.Cx0, cc, dx),
            same(K.DB0, b, dc), same(K.DC0, cc, dc),
        ])

    @step
    def B2():
        b = bref(y, ox)
        recv(K.Bx, b, dx)
        sends(K.B2, [same(K.By1Ro, b, dy(1)), same(K.By1Lo, b, dy(-1)), same(K.DB1, b, dc)])

    @step
    def B3R():
        b = bref(yy(-1), x)
        recv(K.By1Rx, b, dy(-1))
        sends(K.B3R, [same(K.By2R, b, dy(1)), same(K.DB2, b, dc)])

    @step
    def B3L():
        b = bref(yy(1), ox)
        recv(K.By1Lo, b, dy(1))
        sends(K.B3L, [same(K.By2L, b, dy(-1)), same(K.DB3, b, dc)])

    last_b = ((K.By2R, 2, x, -1), (K.By2L, 2, ox, 1), (K.By1Ro, -1, ox, -1), (K.By1Lx, 1, x, 1))

    @step
    def B4():
        recv_all(K.By9)
        sends(K.B4, [same(K.D + nm, bref(yy(o), xi), dc) for nm, o, xi, d in last_b])

    lo4, hi4 = pl.ds(0, 4), pl.ds(4, 4)

    @step
    def C2R():
        recv(K.Cy1R, cref(yy(-1), x), dy(-1))
        sends(K.C2R, [
            same(K.Cy2R, cref(yy(-1), x, lo4), dy(1)),
            same(K.Cx3, cref(yy(-1), x), dx), same(K.DC3, cref(yy(-1), x), dc),
        ])

    @step
    def C2L():
        recv(K.Cy1L, cref(yy(1), x), dy(1))
        sends(K.C2L, [
            same(K.Cy2L, cref(yy(1), x, hi4), dy(-1)),
            same(K.Cx1, cref(yy(1), x), dx), same(K.DC1, cref(yy(1), x), dc),
        ])

    @step
    def C3():
        recv_all(K.Cy2)
        sends(K.C3, [same(K.Cx2, cref(yy(2), x), dx), same(K.DC2, cref(yy(2), x), dc)])

    @step
    def C4():
        recv_all(K.Cx)
        sends(K.C4, [same(f"DCx{o}", cref(yy(o), ox), dc) for o in (0, 1, 3, 2)])

    @step
    def gp():
        recv(K.og, ogP, dc)
        for b in range(4):
            ogT[b, :, TOK : 2 * TOK] = ogP[:, b * 256 : (b + 1) * 256].T

    def grads(k, j):
        cr = ranges[k]
        if j == 0:
            recv(K.h + k, hid2.at[pl.ds(TOK, TOK), cols(cr)], dc)
        c0 = cr[0] + 256 * j
        n = min(256, cr[1] - 256 * j)
        p = jnp.dot(
            ogT[...].reshape(D, 2 * TOK), hid2[:, pl.ds(c0, n)], preferred_element_type=F32
        )
        G[:, :, :, :, pl.ds(c0, n)] = p.reshape(NY, NX, NZ, 16, n)

    for k in K.ABC:
        for j in range(-(-ranges[k][1] // 256)):
            S[f"g{k}{j}"] = lambda k=k, j=j: grads(k, j)

    def ga(h, zi):
        return G[2 * h : 2 * h + 2, :, zi, :, cols(A)]

    @step
    def RA1():
        for h in (0, 1):
            sa1[h] = ga(h, zz(4)).astype(BF)
            sa2[0, 0, h] = ga(h, zz(3)).astype(BF)
        sends(K.RA1, [
            (K.rA1L0, sa1.at[0], ra1.at[0], dz(-1)),
            (K.rA1L1, sa1.at[1], ra1.at[1], dz(-1)),
            (K.rA2R0, sa2.at[0, 0, 0], ra2.at[0, 0, 0], dz(1)),
            (K.rA2R1, sa2.at[0, 0, 1], ra2.at[0, 0, 1], dz(1)),
        ])

    def ra(s, sd, h):
        sg = 1 if sd == K.R else -1
        side = 0 if sd == K.R else 1

        def f():
            buf = ra1.at[h] if s == 2 else ra2.at[side, s - 3, h]
            recv(f"rA{s - 1}{sd}{h}", buf, dz(-sg))
            sa2[side, s - 2, h] = (ga(h, zz(sg * (5 - s))) + buf[...].astype(F32)).astype(BF)
            sends(K.RA, [(f"rA{s}{sd}{h}", sa2.at[side, s - 2, h], ra2.at[side, s - 2, h], dz(sg))])

        S[f"RA{s}{sd}{h}"] = f

    for sd in K.RL:
        for h in (0, 1):
            for s in range(2 if sd == K.L else 3, 5):
                ra(s, sd, h)

    @step
    def RA5():
        recv_all(K.rA4)
        for h in (0, 1):
            t = ga(h, z) + ra2[0, 2, h].astype(F32) + ra2[1, 2, h].astype(F32)
            G[2 * h : 2 * h + 2, :, z, :, cols(A)] = t
            sa3[2 * h : 2 * h + 2] = t.astype(BF)
        sends(K.RA5, [(f"rAy{o}", sa3.at[yy(o)], ra3.at[o - 1], dy(o)) for o in (2, 1, 3)])

    @step
    def RA6():
        recv_all(K.rAy)
        t = G[y, :, z, :, cols(A)]
        for o in (1, 2, 3):
            t = t + ra3[o - 1].astype(F32)
        G[y, :, z, :, cols(A)] = t
        sa4[...] = t.astype(BF)
        sends(K.RA6, [(K.rAx, sa4.at[ox], ra4, dx)])

    @step
    def RA7():
        recv(K.rAx, ra4, dx)
        fin[:, cols(A)] = G[y, x, z, :, cols(A)] + ra4[...].astype(F32)

    def gb(yi, xi):
        return G[yi, xi, :, :, cols(B)]

    @step
    def RB1():
        sb1[0] = gb(yy(2), x).astype(BF)
        sb1[1] = gb(yy(2), ox).astype(BF)
        sb2[0, 1] = gb(yy(1), ox).astype(BF)
        sb2[1, 0] = gb(yy(-1), x).astype(BF)
        sends(K.RB1, [
            (K.rB1R, sb1.at[0], rb1.at[0], dy(1)), (K.rB1L, sb1.at[1], rb1.at[1], dy(-1)),
            (K.rB2R1, sb2.at[0, 1], rb2.at[0, 1], dy(1)),
            (K.rB2L1, sb2.at[1, 0], rb2.at[1, 0], dy(-1)),
        ])

    @step
    def RB2R():
        recv(K.rB1R, rb1.at[0], dy(-1))
        sb2[0, 0] = (gb(yy(1), x) + rb1[0].astype(F32)).astype(BF)
        sends(K.RB2R, [(K.rB2R0, sb2.at[0, 0], rb2.at[0, 0], dy(1))])

    @step
    def RB2L():
        recv(K.rB1L, rb1.at[1], dy(1))
        sb2[1, 1] = (gb(yy(-1), ox) + rb1[1].astype(F32)).astype(BF)
        sends(K.RB2L, [(K.rB2L0, sb2.at[1, 1], rb2.at[1, 1], dy(-1))])

    @step
    def RB3():
        recv_all(K.rB3)
        sb3[...] = (gb(y, ox) + rb2[0, 1].astype(F32) + rb2[1, 1].astype(F32)).astype(BF)
        sends(K.RB3, [(K.rBx, sb3, rb3, dx)])

    @step
    def RB4():
        recv_all(K.rB4)
        t = gb(y, x) + rb2[0, 0].astype(F32) + rb2[1, 0].astype(F32) + rb3[...].astype(F32)
        G[y, x, :, :, cols(B)] = t
        sb4[...] = t.astype(BF)
        sends(K.RB4, [(f"rBz{o}", sb4.at[zz(o)], rb4.at[o - 1], dz(o)) for o in (4, 3, 5, 2, 6, 1, 7)])

    @step
    def RB5():
        t = G[y, x, z, :, cols(B)]
        recv_all(K.rBz)
        for o in range(1, NZ):
            t = t + rb4[o - 1].astype(F32)
        fin[:, cols(B)] = t

    def gc(yi, xi, zs=allr):
        return G[yi, xi, zs, :, cols(C)]

    @step
    def RC1():
        items = []
        for o in (2, 1, 3, 0):
            sc1[o] = gc(yy(o), ox).astype(BF)
            items.append((f"rCx{o}", sc1.at[o], rc1.at[o], dx))
        sends(K.RC1, items)

    @step
    def RC2():
        recv(K.rCx2, rc1.at[2], dx)
        sc2[...] = (gc(yy(2), x) + rc1[2].astype(F32)).astype(BF)
        sends(K.RC2, [
            (K.rCy1R, sc2.at[lo4], rc2.at[0], dy(1)), (K.rCy1L, sc2.at[hi4], rc2.at[1], dy(-1)),
        ])

    @step
    def RC2b():
        recv(K.rCx1, rc1.at[1], dx)
        t = gc(yy(1), x) + rc1[1].astype(F32)
        G[yy(1), x, :, :, cols(C)] = t
        sc3[0, 4:8] = t[4:8].astype(BF)
        sends(K.RC2b, [(K.rCy2R1, sc3.at[0, hi4], rc3.at[0, hi4], dy(1))])

    @step
    def RC2c():
        recv(K.rCx3, rc1.at[3], dx)
        t = gc(yy(3), x) + rc1[3].astype(F32)
        G[yy(3), x, :, :, cols(C)] = t
        sc3[1, 0:4] = t[0:4].astype(BF)
        sends(K.RC2c, [(K.rCy2L1, sc3.at[1, lo4], rc3.at[1, lo4], dy(-1))])

    @step
    def RC3R():
        recv(K.rCy1R, rc2.at[0], dy(-1))
        sc3[0, 0:4] = (gc(yy(1), x, slice(0, 4)) + rc2[0].astype(F32)).astype(BF)
        sends(K.RC3R, [(K.rCy2R0, sc3.at[0, lo4], rc3.at[0, lo4], dy(1))])

    @step
    def RC3L():
        recv(K.rCy1L, rc2.at[1], dy(1))
        sc3[1, 4:8] = (gc(yy(3), x, slice(4, 8)) + rc2[1].astype(F32)).astype(BF)
        sends(K.RC3L, [(K.rCy2L0, sc3.at[1, hi4], rc3.at[1, hi4], dy(-1))])

    @step
    def RC4():
        recv_all(K.rC4)
        t = gc(y, x) + rc1[0].astype(F32) + rc3[0].astype(F32) + rc3[1].astype(F32)
        G[y, x, :, :, cols(C)] = t
        sc4[...] = t.astype(BF)
        sends(K.RC4, [(f"rCz{o}", sc4.at[zz(o)], rc4.at[o - 1], dz(o)) for o in (4, 3, 5, 2, 6, 1, 7)])

    @step
    def RC5():
        t = G[y, x, z, :, cols(C)]
        recv_all(K.rCz)
        for o in range(1, NZ):
            t = t + rc4[o - 1].astype(F32)
        fin[:, cols(C)] = t

    have = set()
    started = []

    def w_of(side, k, c0, n):
        if side == K.o and k not in have:
            have.add(k)
            recv_all(K.D + k)
        half = c if side == K.c else oc
        return W[half, :, :, :, :, pl.ds(c0, n)].reshape(D, n)

    def lo(side, k):
        w = w_of(side, k, *ranges[k])
        h = (hid2 if side == K.c else hidO)[0:TOK, cols(ranges[k])]
        part = lax.dot_general(h, w, (((1,), (1,)), ((), ())), preferred_element_type=F32)
        if started:
            acc[...] += part
        else:
            acc[...] = part
        started.append(1)

    def hgrad(side, k, j):
        c0 = ranges[k][0] + 256 * j
        n = min(256, ranges[k][1] - 256 * j)
        half = c if side == K.c else oc
        cs = pl.ds(pl.multiple_of(half * HALF + c0, 128), n)
        h = jnp.dot(og_ref[...], w_of(side, k, c0, n), preferred_element_type=F32)
        gg_ref[:, cs] = (h * fg[half, :, pl.ds(c0, n)]).astype(BF)
        ug_ref[:, cs] = (h * fu[half, :, pl.ds(c0, n)]).astype(BF)

    for side in K.co:
        for k in K.ABC:
            S[f"lo_{side}{k}"] = lambda side=side, k=k: lo(side, k)
            for j in range(-(-ranges[k][1] // 256)):
                S[f"hg_{side}{k}{j}"] = lambda side=side, k=k, j=j: hgrad(side, k, j)

    @step
    def losend():
        lo_s[...] = acc[:, pl.ds(pl.multiple_of((1 - r) * 512, 128), 512)].astype(BF)
        sends(K.losend, [(K.lo, lo_s, lo_r, dr)])

    @step
    def lofin():
        recv(K.lo, lo_r, dr)
        out_ref[...] = (
            acc[:, pl.ds(pl.multiple_of(r * 512, 128), 512)] + lo_r[...].astype(F32)
        ).astype(BF)

    def update(half, g):
        cs = pl.ds(pl.multiple_of(half * HALF, 128), HALF)
        g = g / jnp.float32(32768)
        m = master_ref[:, cs]
        first = 0.9 * one_ref[:, cs] + 0.1 * g
        second = 0.95 * two_ref[:, cs] + 0.05 * g * g
        upd = first / (1.0 - first_power) / (jnp.sqrt(second / (1.0 - second_power)) + 1e-08)
        master_out[:, cs] = m - 0.003 * (upd + 0.1 * m)
        one_out[:, cs] = first
        two_out[:, cs] = second

    @step
    def fin_():
        loc[K.one].wait()
        loc[K.two].wait()
        sends(K.fin, [(K.fin, fin.at[pl.ds(pl.multiple_of(oc * 8, 8), 8)], finP, dc)])
        update(c, fin[pl.ds(pl.multiple_of(c * 8, 8), 8), :])

    @step
    def adam():
        recv(K.fin, finP, dc)
        update(oc, finP[...])

    loc[K.master].wait()
    with jax.named_scope(K.barrier):
        pl.semaphore_wait(bar, len(peers))
    for n in ORDER:
        with jax.named_scope(n):
            S.pop(n)()
    assert not S, S.keys()
    with jax.named_scope(K.sends_done):
        for n, many in sent.items():
            if many:
                pltpu.make_async_remote_copy(
                    src_ref=tiles(n * many), dst_ref=tiles(n * many),
                    send_sem=ssem.at[list(sent).index(n)], recv_sem=rsem.at[0],
                    device_id=dc, device_id_type=pl.DeviceIdType.MESH,
                ).wait_send()
    assert len(slots) <= NRECV and len(sent) <= NSEND, (len(slots), len(sent))


NRECV, NSEND = 58, 20

GROUPS = {}
for _first, _names in (
    (K.Az9, (K.Az3R0, K.Az3R1, K.Az4L0, K.Az4L1)),
    (K.By9, (K.By2R, K.By2L, K.By1Ro, K.By1Lx)),
    (K.rB4, (K.rB2R0, K.rB2L1, K.rBx)),
    (K.rB3, (K.rB2R1, K.rB2L0)),
    (K.rC4, (K.rCx0, K.rCy2R0, K.rCy2R1, K.rCy2L0, K.rCy2L1)),
    (K.Cy2, (K.Cy2R, K.Cy2L)),
):
    for _n in _names:
        GROUPS[_n] = _first


def group_of(name):
    if name in GROUPS:
        return GROUPS[name]
    for p in (K.Zd, K.Ay, K.rAy, K.rBz, K.rCz, K.DA, K.DB, K.DC, K.Cx, K.rA4):
        if name.startswith(p):
            return p
    return name


def copy_kernel(*refs):
    src, dst, sem = refs[0:6], refs[6:12], refs[12]
    copies = [pltpu.make_async_copy(src[i], dst[i], sem.at[i]) for i in range(6)]
    for d in copies:
        d.start()
    for d in copies:
        d.wait()


def on_device(gate_pre, up_pre, out_grad, master, moment_one, moment_two):
    V = pltpu.VMEM

    def in_hbm(a):
        return pltpu.with_memory_space_constraint(a, pltpu.HBM)

    nA, nB, nC = A[1], B[1], C[1]
    outs = pl.pallas_call(
        kernel,
        out_shape=(
            V((TOK, 512), BF),
            V((TOK, FF), BF),
            V((TOK, FF), BF),
            V((8, FF), F32),
            V((8, FF), F32),
            V((8, FF), F32),
        ),
        in_specs=[pl.BlockSpec(memory_space=pltpu.HBM)] * 6,
        out_specs=[pl.BlockSpec(memory_space=V)] * 6,
        scratch_shapes=[
            V((TOK, FF), BF), V((TOK, FF), BF), V((TOK, D), BF),
            V((8, FF), F32), V((8, FF), F32), V((8, FF), F32),
            V((NC, NY, NX, NZ, 16, HALF), BF),
            V((NY, NX, NZ, 16, HALF), F32),
            V((2 * TOK, HALF), BF),
            V((TOK, HALF), BF),
            V((TOK, D), BF),
            V((4, 256, 2 * TOK), BF),
            V((8, HALF), F32),
            V((2, TOK, HALF), F32),
            V((2, TOK, HALF), F32),
            V((TOK, D), F32),
            V((16, HALF), F32),
            V((8, HALF), F32),
            V((TOK, 512), BF),
            V((TOK, 512), BF),
            V((2, 2, NX, 16, nA), BF), V((2, 2, NX, 16, nA), BF),
            V((2, 3, 2, 2, NX, 16, nA), BF), V((2, 3, 2, 2, NX, 16, nA), BF),
            V((NY, NX, 16, nA), BF), V((3, NX, 16, nA), BF),
            V((NX, 16, nA), BF), V((16, nA), BF),
            V((NX, NZ, 16, nB), BF), V((2, NZ, 16, nB), BF),
            V((2, NX, NZ, 16, nB), BF), V((2, NX, NZ, 16, nB), BF),
            V((NZ, 16, nB), BF), V((NZ, 16, nB), BF),
            V((NZ, 16, nB), BF), V((7, 16, nB), BF),
            V((NY, NZ, 16, nC), BF), V((NY, NZ, 16, nC), BF),
            V((NZ, 16, nC), BF), V((2, 4, 16, nC), BF),
            V((2, NZ, 16, nC), BF), V((2, NZ, 16, nC), BF),
            V((NZ, 16, nC), BF), V((7, 16, nC), BF),
            V((768, 16, 128), BF),
            pltpu.SemaphoreType.DMA((NSEND,)),
            pltpu.SemaphoreType.DMA((NRECV,)),
            pltpu.SemaphoreType.DMA((6,)),
        ],
        compiler_params=pltpu.CompilerParams(
            collective_id=0, has_side_effects=True, vmem_limit_bytes=56_000_000
        ),
    )(
        in_hbm(gate_pre.reshape(TOK, FF)),
        in_hbm(up_pre.reshape(TOK, FF)),
        in_hbm(out_grad.reshape(TOK, D)),
        in_hbm(master),
        in_hbm(moment_one),
        in_hbm(moment_two),
    )
    outs = pl.pallas_call(
        copy_kernel,
        out_shape=tuple(jax.ShapeDtypeStruct(o.shape, o.dtype) for o in outs),
        in_specs=[pl.BlockSpec(memory_space=V)] * 6,
        out_specs=[pl.BlockSpec(memory_space=pl.ANY)] * 6,
        scratch_shapes=[pltpu.SemaphoreType.DMA((6,))],
    )(*[pltpu.with_memory_space_constraint(o, V) for o in outs])
    lo, gg, ug, mn, m1, m2 = outs
    return (
        lo.reshape(2, 128, 512),
        gg.reshape(2, 128, FF),
        ug.reshape(2, 128, FF),
        mn,
        m1,
        m2,
    )


def solution(mesh):
    torus = Mesh(
        mesh.devices.reshape(NY, NX, NZ, NC, mesh.shape["rep"]),
        ("dp_0", "dp_1", "dp_2", "dp_3", "rep"),
    )
    return jax.shard_map(
        on_device,
        mesh=torus,
        in_specs=(
            P(None, DP, "rep"),
            P(None, DP, "rep"),
            P(None, DP, None),
            P(DP, "rep"),
            P(DP, "rep"),
            P(DP, "rep"),
        ),
        out_specs=(
            P(None, DP, "rep"),
            P(None, DP, "rep"),
            P(None, DP, "rep"),
            P(DP, "rep"),
            P(DP, "rep"),
            P(DP, "rep"),
        ),
        check_vma=False,
    )
```

```python
import math

import jax
import jax.numpy as jnp
from jax import lax
from jax.experimental import pallas as pl
from jax.experimental.pallas import tpu as pltpu
from jax.sharding import Mesh
from jax.sharding import PartitionSpec as P

DP = ("dp_0", "dp_1", "dp_2", "dp_3")
NY, NX, NZ, NC = 4, 2, 8, 2

first_power = 2.6561398887587544e-05
second_power = 0.005920529220333997

F32 = jnp.float32
BF = jnp.bfloat16
D = 1024
FF = 2816
HALF = 1408
TOK = 256
A = (0, 512)
B = (512, 512)
C = (1024, 384)
BC = (512, 896)


def cols(r):
    return pl.ds(r[0], r[1])


class Names:
    def __getattr__(self, word):
        return word


K = Names()

ORDER = (
    K.init, K.hidO_, K.hid2_, K.gp, K.gB0, K.A1, K.gC0, K.gC1, K.RC1, K.gB1, K.RB1, K.gA0,
    K.gA1, K.RA1, K.A2, K.BC1N, K.A3_1L0, K.A3_1L1, K.RA2L0, K.BC1F, K.A3_2L0, K.RB2L, K.A3_1R0,
    K.A3_1R1, K.B2N, K.RA3R0, K.fo, K.C2RF, K.A3_2L1, K.C2RN, K.C2LN, K.RA2L1, K.A3_2R0, K.B3RF,
    K.C2LF, K.A3_3L0, K.A3_3L1, K.B2F, K.B3RN, K.fc, K.RA3L0, K.A3_2R1, K.RA3R1, K.C3N, K.RA4R0,
    K.B3LN, K.C3F, K.RB2R, K.RB3, K.B3LF, K.RA3L1, K.A6, K.RC2, K.lo_cA, K.C4, K.lo_cC,
    K.hg_cC0, K.RA4L0, K.B4, K.lo_cB, K.lo_oA, K.RA4R1, K.RC2b, K.hg_cC1, K.RC2c, K.RA4L1,
    K.lo_oC, K.lo_oB, K.RB4, K.losend, K.RC3R, K.RC3L, K.hg_cA1, K.hg_cB1, K.hg_cA0, K.hg_oB1,
    K.hg_oA1, K.RA5, K.RC4, K.RA6, K.hg_cB0, K.hg_oC1, K.hg_oC0, K.RB5, K.hg_oA0, K.hg_oB0,
    K.RA7, K.RC5, K.fin_, K.lofin, K.adam,
)
ORDS = {
    K.init: (K.Zd4, K.Ax, K.Zd5, K.Zd2, K.Zd1, K.Zd3, K.Zd7, K.Zd6, K.og,),
    K.A1: (K.Ay1, K.Ay2, K.Ay3,),
    K.A2: (K.Az1R0, K.DA0, K.Az1L0, K.Az1L1, K.Az1R1,),
    K.A3_1R0: (K.DA1R0, K.Az2R0,),
    K.A3_1R1: (K.DA1R1, K.Az2R1,),
    K.A3_1L0: (K.DA1L0, K.Az2L0,),
    K.A3_1L1: (K.DA1L1, K.Az2L1,),
    K.A3_2R0: (K.DA2R0, K.Az3R0,),
    K.A3_2R1: (K.Az3R1, K.DA2R1,),
    K.A3_2L0: (K.DA2L0, K.Az3L0,),
    K.A3_2L1: (K.DA2L1, K.Az3L1,),
    K.A3_3L0: (K.Az4L0, K.DA3L0,),
    K.A3_3L1: (K.DA3L1, K.Az4L1,),
    K.BC1N: (K.DB0N, K.Cy1RN, K.Cy1LN, K.DC0N, K.BxN, K.By1LxN, K.Cx0N, K.By1RxN,),
    K.B2N: (K.By1LoN, K.DB1N, K.By1RoN,),
    K.B3RN: (K.By2RN, K.DB2N,),
    K.B3LN: (K.DB3N, K.By2LN,),
    K.C2RN: (K.Cx3N, K.DC3N, K.Cy2RN,),
    K.C2LN: (K.Cx1N, K.DC1N,),
    K.C3N: (K.Cx2N, K.DC2N,),
    K.BC1F: (K.BxF, K.Cy1RF, K.DC0F, K.Cx0F, K.By1RxF, K.DB0F, K.By1LxF, K.Cy1LF,),
    K.B2F: (K.By1LoF, K.DB1F, K.By1RoF,),
    K.B3RF: (K.DB2F, K.By2RF,),
    K.B3LF: (K.DB3F, K.By2LF,),
    K.C2RF: (K.Cx3F, K.DC3F,),
    K.C2LF: (K.Cx1F, K.DC1F, K.Cy2LF,),
    K.C3F: (K.Cx2F, K.DC2F,),
    K.RC1: (K.rCx1, K.rCx2, K.rCx0, K.rCx3,),
    K.RB1: (K.rB2L1, K.rB1L, K.rB1R, K.rB2R1,),
    K.RA1: (K.rA2R0, K.rA1L0, K.rA1L1, K.rA2R1,),
    K.RA5: (K.rAy2, K.rAy1, K.rAy3,),
    K.RB4: (K.rBz6, K.rBz3, K.rBz2, K.rBz7, K.rBz1, K.rBz4, K.rBz5,),
    K.RC2: (K.rCy1L, K.rCy1R,),
    K.RC4: (K.rCz4, K.rCz6, K.rCz7, K.rCz3, K.rCz2, K.rCz1, K.rCz5,),
}
HORDER = (K.B, K.C, K.A)


def kernel(
    gate_hbm, up_hbm, og_hbm, master_hbm, one_hbm, two_hbm,
    out_ref, gg_ref, ug_ref, master_out, one_out, two_out,
    gate_ref, up_ref, og_ref, master_ref, one_ref, two_ref,
    W, G, hid2, hidO, ogP, ogT, mP, fg, fu, acc, fin, finP, lo_s, lo_r,
    sa1, ra1, sa2, ra2, sa3, ra3, sa4, ra4,
    sb1, rb1, sb2, rb2, sb3, rb3, sb4, rb4,
    sc1, rc1, sc2, rc2, sc3, rc3, sc4, rc4,
    space, ssem, rsem, lsem,
):
    y = lax.axis_index(K.dp_0)
    x = lax.axis_index(K.dp_1)
    z = lax.axis_index(K.dp_2)
    c = lax.axis_index(K.dp_3)
    r = lax.axis_index(K.rep)
    oc = 1 - c
    ox = 1 - x

    def dy(o):
        return {K.dp_0: lax.rem(y + (o % NY), NY)}

    def dz(o):
        return {K.dp_2: lax.rem(z + (o % NZ), NZ)}

    def zz(o):
        return lax.rem(z + (o % NZ), NZ)

    def yy(o):
        return lax.rem(y + (o % NY), NY)

    dx = {K.dp_1: ox}
    dc = {K.dp_3: oc}
    dr = {K.rep: 1 - r}
    allr = slice(None)

    peers = [dc, dx, dr] + [dy(o) for o in range(1, NY)] + [dz(o) for o in range(1, NZ)]
    bar = pltpu.get_barrier_semaphore()
    for p in peers:
        pl.semaphore_signal(bar, inc=1, device_id=p, device_id_type=pl.DeviceIdType.MESH)

    loc = {}

    def local(name, src, dst):
        d = pltpu.make_async_copy(src, dst, lsem.at[len(loc)])
        d.start()
        loc[name] = d

    local(K.master, master_hbm, master_ref)
    local(K.og, og_hbm, og_ref)
    local(K.gate, gate_hbm, gate_ref)
    local(K.up, up_hbm, up_ref)
    local(K.one, one_hbm, one_ref)
    local(K.two, two_hbm, two_ref)

    slots, sent, arriving = {}, {}, {}

    def size(ref):
        return math.prod(ref.shape) * ref.dtype.itemsize

    def rc(name, src, dst, dev):
        group = group_of(name)
        k = slots.setdefault(group, len(slots))
        sent.setdefault(size(src), 0)
        return pltpu.make_async_remote_copy(
            src_ref=src, dst_ref=dst, send_sem=ssem.at[list(sent).index(size(src))],
            recv_sem=rsem.at[k], device_id=dev, device_id_type=pl.DeviceIdType.MESH,
        )

    def tiles(total):
        return space.at[pl.ds(0, total // 4096)]

    def recv_all(group):
        n = arriving[group]
        with jax.named_scope(K.wait_ + group):
            rc(group, tiles(n), tiles(n), dc).wait_recv()

    def sends(step, items):
        names = ORDS.get(step, tuple(i[0] for i in items))
        table = {i[0]: i for i in items}
        for n in names:
            table[n]
        for name in list(names) + [n for n in table if n not in names]:
            _, srcs, dsts, dev = table[name]
            if not isinstance(srcs, list):
                srcs, dsts = [srcs], [dsts]
            for src, dst in zip(srcs, dsts):
                rc(name, src, dst, dev).start()
                sent[size(src)] += 1
                arriving[group_of(name)] = arriving.get(group_of(name), 0) + size(dst)

    def recv(name, dst, dev):
        with jax.named_scope(K.wait_ + name):
            rc(name, dst, dst, dev).wait_recv()

    def hidden_rows(half, out, cr):
        cs = pl.ds(pl.multiple_of(half * HALF + cr[0], 128), cr[1])

        def body(i, _):
            rows = pl.ds(pl.multiple_of(i * 32, 32), 32)
            g = gate_ref[rows, cs].astype(F32)
            u = up_ref[rows, cs].astype(F32)
            s = jax.nn.sigmoid(g)
            out[rows, cols(cr)] = (g * s * u).astype(BF)
            return 0

        lax.fori_loop(0, TOK // 32, body, 0)

    def factor_rows(half):
        cs = pl.ds(pl.multiple_of(half * HALF, 128), HALF)

        def body(i, _):
            rows = pl.ds(pl.multiple_of(i * 16, 16), 16)
            g = gate_ref[rows, cs].astype(F32)
            u = up_ref[rows, cs].astype(F32)
            s = jax.nn.sigmoid(g)
            fg[half, rows, :] = u * s * (1.0 + g * (1.0 - s))
            fu[half, rows, :] = g * s
            return 0

        lax.fori_loop(0, TOK // 16, body, 0)

    def Wb(*idx):
        return W.at[(c,) + idx]

    def same(name, ref, dev):
        return (name, ref, ref, dev)

    ranges = {K.A: A, K.B: B, K.C: C}
    S = {}

    def step(f):
        S[f.__name__] = f
        return f

    @step
    def init():
        sends(K.i0, [(K.m, master_ref.at[:, pl.ds(pl.multiple_of(oc * HALF, 128), HALF)], mP, dc)])
        recv(K.m, mP, dc)
        mine = master_ref[:, pl.ds(pl.multiple_of(c * HALF, 128), HALF)]
        theirs = mP[...]
        first_core = c == 0
        W[c, y, x, z] = jnp.concatenate(
            [jnp.where(first_core, mine, theirs), jnp.where(first_core, theirs, mine)], axis=0
        ).astype(BF)
        loc[K.og].wait()
        items = [
            (K.og, og_ref, ogP, dc),
            same(K.Ax, Wb(y, x, z, allr, cols(A)), dx),
        ]
        for o in (4, 3, 5, 2, 6, 1, 7):
            items.append(same(f"Zd{o}", Wb(y, x, z, allr, cols(BC)), dz(o)))
        sends(K.init, items)

    @step
    def hidO_():
        loc[K.gate].wait()
        loc[K.up].wait()
        for k in HORDER:
            cr = ranges[k]
            hidden_rows(oc, hidO, cr)
            sends(K.h, [(K.h + k, hidO.at[:, cols(cr)], hid2.at[pl.ds(TOK, TOK), cols(cr)], dc)])

    @step
    def hid2_():
        for k in HORDER:
            hidden_rows(c, hid2, ranges[k])
        for b in range(4):
            ogT[b, :, 0:TOK] = og_ref[:, b * 256 : (b + 1) * 256].T

    S[K.fo] = lambda: factor_rows(oc)
    S[K.fc] = lambda: factor_rows(c)

    @step
    def A1():
        recv(K.Ax, Wb(y, ox, z, allr, cols(A)), dx)
        ref = Wb(y, allr, z, allr, cols(A))
        sends(K.A1, [same(f"Ay{o}", ref, dy(o)) for o in (2, 1, 3)])

    def az(h, zi):
        return Wb(pl.ds(2 * h, 2), allr, zi, allr, cols(A))

    @step
    def A2():
        recv_all(K.Ay)
        sends(K.A2, [
            same(K.Az1L0, az(0, z), dz(-1)),
            same(K.Az1R0, az(0, z), dz(1)),
            same(K.Az1L1, az(1, z), dz(-1)),
            same(K.Az1R1, az(1, z), dz(1)),
            same(K.DA0, Wb(allr, allr, z, allr, cols(A)), dc),
        ])

    def a3(s, sd, h):
        sg = 1 if sd == K.R else -1
        ref = az(h, zz(-sg * s))
        nm = f"{s}{sd}{h}"

        def f():
            recv(K.Az + nm, ref, dz(-sg))
            sends(K.A3_ + nm, [same(f"Az{s + 1}{sd}{h}", ref, dz(sg)), same(K.DA + nm, ref, dc)])

        S[K.A3_ + nm] = f

    last_a = (("3R0", 0, -3), ("3R1", 1, -3), ("4L0", 0, 4), ("4L1", 1, 4))
    for s in (1, 2, 3):
        for h in (0, 1):
            a3(s, K.L, h)
            if s < 3:
                a3(s, K.R, h)

    @step
    def A6():
        recv_all(K.Az9)
        sends(K.A6, [same(K.DA + nm, az(h, zz(o)), dc) for nm, h, o in last_a])

    def bref(yi, xi):
        return Wb(yi, xi, allr, allr, cols(B))

    def cref(yi, xi, zs=allr):
        return Wb(yi, xi, zs, allr, cols(C))

    zones = {K.N: (0, 1, -1, 2, -2), K.F: (3, -3, 4)}

    def bblk(yi, xi, p):
        return [Wb(yi, xi, zz(o), allr, cols(B)) for o in zones[p]]

    def cblk(yi, xi, p):
        return [Wb(yi, xi, zz(o), allr, cols(C)) for o in zones[p]]

    def bc_steps(p):
        def BC1():
            recv_all(K.Zd + p)
            b, cc = bblk(y, x, p), cblk(y, x, p)
            sends(K.BC1 + p, [
                same(K.Bx + p, b, dx), same(K.By1Rx + p, b, dy(1)), same(K.By1Lx + p, b, dy(-1)),
                same(K.Cy1R + p, cc, dy(1)), same(K.Cy1L + p, cc, dy(-1)), same(K.Cx0 + p, cc, dx),
                same(K.DB0 + p, b, dc), same(K.DC0 + p, cc, dc),
            ])

        def B2():
            recv_all(K.Bx + p)
            b = bblk(y, ox, p)
            sends(K.B2 + p, [
                same(K.By1Ro + p, b, dy(1)), same(K.By1Lo + p, b, dy(-1)), same(K.DB1 + p, b, dc),
            ])

        def B3R():
            recv_all(K.By1Rx + p)
            b = bblk(yy(-1), x, p)
            sends(K.B3R + p, [same(K.By2R + p, b, dy(1)), same(K.DB2 + p, b, dc)])

        def B3L():
            recv_all(K.By1Lo + p)
            b = bblk(yy(1), ox, p)
            sends(K.B3L + p, [same(K.By2L + p, b, dy(-1)), same(K.DB3 + p, b, dc)])

        def C2R():
            recv_all(K.Cy1R + p)
            cc = cblk(yy(-1), x, p)
            on = [same(K.Cy2RN, cc, dy(1))] if p == K.N else []
            sends(K.C2R + p, on + [same(K.Cx3 + p, cc, dx), same(K.DC3 + p, cc, dc)])

        def C2L():
            recv_all(K.Cy1L + p)
            cc = cblk(yy(1), x, p)
            on = [same(K.Cy2LF, cc, dy(-1))] if p == K.F else []
            sends(K.C2L + p, on + [same(K.Cx1 + p, cc, dx), same(K.DC1 + p, cc, dc)])

        def C3():
            recv_all(K.Cy2RN if p == K.N else K.Cy2LF)
            cc = cblk(yy(2), x, p)
            sends(K.C3 + p, [same(K.Cx2 + p, cc, dx), same(K.DC2 + p, cc, dc)])

        for f in (BC1, B2, B3R, B3L, C2R, C2L, C3):
            S[f.__name__ + p] = f

    bc_steps(K.N)
    bc_steps(K.F)
    last_b = ((K.By2R, 2, x), (K.By2L, 2, ox), (K.By1Ro, -1, ox), (K.By1Lx, 1, x))
    lo4, hi4 = pl.ds(0, 4), pl.ds(4, 4)

    @step
    def B4():
        recv_all(K.By9)
        sends(K.B4, [same(K.D + nm, bref(yy(o), xi), dc) for nm, o, xi in last_b])

    @step
    def C4():
        recv_all(K.Cx)
        sends(K.C4, [same(f"DCx{o}", cref(yy(o), ox), dc) for o in (0, 1, 3, 2)])

    @step
    def gp():
        recv(K.og, ogP, dc)
        for b in range(4):
            ogT[b, :, TOK : 2 * TOK] = ogP[:, b * 256 : (b + 1) * 256].T

    def grads(k, j):
        cr = ranges[k]
        if j == 0:
            recv(K.h + k, hid2.at[pl.ds(TOK, TOK), cols(cr)], dc)
        c0 = cr[0] + 256 * j
        n = min(256, cr[1] - 256 * j)
        p = jnp.dot(
            ogT[...].reshape(D, 2 * TOK), hid2[:, pl.ds(c0, n)], preferred_element_type=F32
        )
        G[:, :, :, :, pl.ds(c0, n)] = p.reshape(NY, NX, NZ, 16, n)

    for k in K.ABC:
        for j in range(-(-ranges[k][1] // 256)):
            S[f"g{k}{j}"] = lambda k=k, j=j: grads(k, j)

    def ga(h, zi):
        return G[2 * h : 2 * h + 2, :, zi, :, cols(A)]

    @step
    def RA1():
        for h in (0, 1):
            sa1[h] = ga(h, zz(4)).astype(BF)
            sa2[0, 0, h] = ga(h, zz(3)).astype(BF)
        sends(K.RA1, [
            (K.rA1L0, sa1.at[0], ra1.at[0], dz(-1)),
            (K.rA1L1, sa1.at[1], ra1.at[1], dz(-1)),
            (K.rA2R0, sa2.at[0, 0, 0], ra2.at[0, 0, 0], dz(1)),
            (K.rA2R1, sa2.at[0, 0, 1], ra2.at[0, 0, 1], dz(1)),
        ])

    def ra(s, sd, h):
        sg = 1 if sd == K.R else -1
        side = 0 if sd == K.R else 1

        def f():
            buf = ra1.at[h] if s == 2 else ra2.at[side, s - 3, h]
            recv(f"rA{s - 1}{sd}{h}", buf, dz(-sg))
            sa2[side, s - 2, h] = (ga(h, zz(sg * (5 - s))) + buf[...].astype(F32)).astype(BF)
            sends(K.RA, [(f"rA{s}{sd}{h}", sa2.at[side, s - 2, h], ra2.at[side, s - 2, h], dz(sg))])

        S[f"RA{s}{sd}{h}"] = f

    for sd in K.RL:
        for h in (0, 1):
            for s in range(2 if sd == K.L else 3, 5):
                ra(s, sd, h)

    @step
    def RA5():
        recv_all(K.rA4)
        for h in (0, 1):
            t = ga(h, z) + ra2[0, 2, h].astype(F32) + ra2[1, 2, h].astype(F32)
            G[2 * h : 2 * h + 2, :, z, :, cols(A)] = t
            sa3[2 * h : 2 * h + 2] = t.astype(BF)
        sends(K.RA5, [(f"rAy{o}", sa3.at[yy(o)], ra3.at[o - 1], dy(o)) for o in (2, 1, 3)])

    @step
    def RA6():
        recv_all(K.rAy)
        t = G[y, :, z, :, cols(A)]
        for o in (1, 2, 3):
            t = t + ra3[o - 1].astype(F32)
        G[y, :, z, :, cols(A)] = t
        sa4[...] = t.astype(BF)
        sends(K.RA6, [(K.rAx, sa4.at[ox], ra4, dx)])

    @step
    def RA7():
        recv(K.rAx, ra4, dx)
        fin[:, cols(A)] = G[y, x, z, :, cols(A)] + ra4[...].astype(F32)

    def gb(yi, xi):
        return G[yi, xi, :, :, cols(B)]

    @step
    def RB1():
        sb1[0] = gb(yy(2), x).astype(BF)
        sb1[1] = gb(yy(2), ox).astype(BF)
        sb2[0, 1] = gb(yy(1), ox).astype(BF)
        sb2[1, 0] = gb(yy(-1), x).astype(BF)
        sends(K.RB1, [
            (K.rB1R, sb1.at[0], rb1.at[0], dy(1)), (K.rB1L, sb1.at[1], rb1.at[1], dy(-1)),
            (K.rB2R1, sb2.at[0, 1], rb2.at[0, 1], dy(1)),
            (K.rB2L1, sb2.at[1, 0], rb2.at[1, 0], dy(-1)),
        ])

    @step
    def RB2R():
        recv(K.rB1R, rb1.at[0], dy(-1))
        sb2[0, 0] = (gb(yy(1), x) + rb1[0].astype(F32)).astype(BF)
        sends(K.RB2R, [(K.rB2R0, sb2.at[0, 0], rb2.at[0, 0], dy(1))])

    @step
    def RB2L():
        recv(K.rB1L, rb1.at[1], dy(1))
        sb2[1, 1] = (gb(yy(-1), ox) + rb1[1].astype(F32)).astype(BF)
        sends(K.RB2L, [(K.rB2L0, sb2.at[1, 1], rb2.at[1, 1], dy(-1))])

    @step
    def RB3():
        recv_all(K.rB3)
        sb3[...] = (gb(y, ox) + rb2[0, 1].astype(F32) + rb2[1, 1].astype(F32)).astype(BF)
        sends(K.RB3, [(K.rBx, sb3, rb3, dx)])

    @step
    def RB4():
        recv_all(K.rB4)
        t = gb(y, x) + rb2[0, 0].astype(F32) + rb2[1, 0].astype(F32) + rb3[...].astype(F32)
        G[y, x, :, :, cols(B)] = t
        sb4[...] = t.astype(BF)
        sends(K.RB4, [(f"rBz{o}", sb4.at[zz(o)], rb4.at[o - 1], dz(o)) for o in (4, 3, 5, 2, 6, 1, 7)])

    @step
    def RB5():
        t = G[y, x, z, :, cols(B)]
        recv_all(K.rBz)
        for o in range(1, NZ):
            t = t + rb4[o - 1].astype(F32)
        fin[:, cols(B)] = t

    def gc(yi, xi, zs=allr):
        return G[yi, xi, zs, :, cols(C)]

    @step
    def RC1():
        items = []
        for o in (2, 1, 3, 0):
            sc1[o] = gc(yy(o), ox).astype(BF)
            items.append((f"rCx{o}", sc1.at[o], rc1.at[o], dx))
        sends(K.RC1, items)

    @step
    def RC2():
        recv(K.rCx2, rc1.at[2], dx)
        sc2[...] = (gc(yy(2), x) + rc1[2].astype(F32)).astype(BF)
        sends(K.RC2, [
            (K.rCy1R, sc2.at[lo4], rc2.at[0], dy(1)), (K.rCy1L, sc2.at[hi4], rc2.at[1], dy(-1)),
        ])

    @step
    def RC2b():
        recv(K.rCx1, rc1.at[1], dx)
        t = gc(yy(1), x) + rc1[1].astype(F32)
        G[yy(1), x, :, :, cols(C)] = t
        sc3[0, 4:8] = t[4:8].astype(BF)
        sends(K.RC2b, [(K.rCy2R1, sc3.at[0, hi4], rc3.at[0, hi4], dy(1))])

    @step
    def RC2c():
        recv(K.rCx3, rc1.at[3], dx)
        t = gc(yy(3), x) + rc1[3].astype(F32)
        G[yy(3), x, :, :, cols(C)] = t
        sc3[1, 0:4] = t[0:4].astype(BF)
        sends(K.RC2c, [(K.rCy2L1, sc3.at[1, lo4], rc3.at[1, lo4], dy(-1))])

    @step
    def RC3R():
        recv(K.rCy1R, rc2.at[0], dy(-1))
        sc3[0, 0:4] = (gc(yy(1), x, slice(0, 4)) + rc2[0].astype(F32)).astype(BF)
        sends(K.RC3R, [(K.rCy2R0, sc3.at[0, lo4], rc3.at[0, lo4], dy(1))])

    @step
    def RC3L():
        recv(K.rCy1L, rc2.at[1], dy(1))
        sc3[1, 4:8] = (gc(yy(3), x, slice(4, 8)) + rc2[1].astype(F32)).astype(BF)
        sends(K.RC3L, [(K.rCy2L0, sc3.at[1, hi4], rc3.at[1, hi4], dy(-1))])

    @step
    def RC4():
        recv_all(K.rC4)
        t = gc(y, x) + rc1[0].astype(F32) + rc3[0].astype(F32) + rc3[1].astype(F32)
        G[y, x, :, :, cols(C)] = t
        sc4[...] = t.astype(BF)
        sends(K.RC4, [(f"rCz{o}", sc4.at[zz(o)], rc4.at[o - 1], dz(o)) for o in (4, 3, 5, 2, 6, 1, 7)])

    @step
    def RC5():
        t = G[y, x, z, :, cols(C)]
        recv_all(K.rCz)
        for o in range(1, NZ):
            t = t + rc4[o - 1].astype(F32)
        fin[:, cols(C)] = t

    have = set()
    started = []

    def w_of(side, k, c0, n):
        if side == K.o and k not in have:
            have.add(k)
            recv_all(K.D + k)
        half = c if side == K.c else oc
        return W[half, :, :, :, :, pl.ds(c0, n)].reshape(D, n)

    def lo(side, k):
        w = w_of(side, k, *ranges[k])
        h = (hid2 if side == K.c else hidO)[0:TOK, cols(ranges[k])]
        part = lax.dot_general(h, w, (((1,), (1,)), ((), ())), preferred_element_type=F32)
        if started:
            acc[...] += part
        else:
            acc[...] = part
        started.append(1)

    def hgrad(side, k, j):
        c0 = ranges[k][0] + 256 * j
        n = min(256, ranges[k][1] - 256 * j)
        half = c if side == K.c else oc
        cs = pl.ds(pl.multiple_of(half * HALF + c0, 128), n)
        h = jnp.dot(og_ref[...], w_of(side, k, c0, n), preferred_element_type=F32)
        gg_ref[:, cs] = (h * fg[half, :, pl.ds(c0, n)]).astype(BF)
        ug_ref[:, cs] = (h * fu[half, :, pl.ds(c0, n)]).astype(BF)

    for side in K.co:
        for k in K.ABC:
            S[f"lo_{side}{k}"] = lambda side=side, k=k: lo(side, k)
            for j in range(-(-ranges[k][1] // 256)):
                S[f"hg_{side}{k}{j}"] = lambda side=side, k=k, j=j: hgrad(side, k, j)

    @step
    def losend():
        lo_s[...] = acc[:, pl.ds(pl.multiple_of((1 - r) * 512, 128), 512)].astype(BF)
        sends(K.losend, [(K.lo, lo_s, lo_r, dr)])

    @step
    def lofin():
        recv(K.lo, lo_r, dr)
        out_ref[...] = (
            acc[:, pl.ds(pl.multiple_of(r * 512, 128), 512)] + lo_r[...].astype(F32)
        ).astype(BF)

    def update(half, g):
        cs = pl.ds(pl.multiple_of(half * HALF, 128), HALF)
        g = g / jnp.float32(32768)
        m = master_ref[:, cs]
        first = 0.9 * one_ref[:, cs] + 0.1 * g
        second = 0.95 * two_ref[:, cs] + 0.05 * g * g
        upd = first / (1.0 - first_power) / (jnp.sqrt(second / (1.0 - second_power)) + 1e-08)
        master_out[:, cs] = m - 0.003 * (upd + 0.1 * m)
        one_out[:, cs] = first
        two_out[:, cs] = second

    @step
    def fin_():
        loc[K.one].wait()
        loc[K.two].wait()
        sends(K.fin, [(K.fin, fin.at[pl.ds(pl.multiple_of(oc * 8, 8), 8)], finP, dc)])
        update(c, fin[pl.ds(pl.multiple_of(c * 8, 8), 8), :])

    @step
    def adam():
        recv(K.fin, finP, dc)
        update(oc, finP[...])

    loc[K.master].wait()
    with jax.named_scope(K.barrier):
        pl.semaphore_wait(bar, len(peers))
    for n in ORDER:
        with jax.named_scope(n):
            S.pop(n)()
    assert not S, S.keys()
    with jax.named_scope(K.sends_done):
        for n, many in sent.items():
            if many:
                pltpu.make_async_remote_copy(
                    src_ref=tiles(n * many), dst_ref=tiles(n * many),
                    send_sem=ssem.at[list(sent).index(n)], recv_sem=rsem.at[0],
                    device_id=dc, device_id_type=pl.DeviceIdType.MESH,
                ).wait_send()
    assert len(slots) <= NRECV and len(sent) <= NSEND, (len(slots), len(sent))


NRECV, NSEND = 64, 21

GROUPS = {}
for _first, _names in (
    (K.Az9, (K.Az3R0, K.Az3R1, K.Az4L0, K.Az4L1)),
    (K.By9, tuple(a + b for a in (K.By2R, K.By2L, K.By1Ro, K.By1Lx) for b in K.NF)),
    (K.ZdN, (K.Zd1, K.Zd2, K.Zd6, K.Zd7)),
    (K.ZdF, (K.Zd3, K.Zd4, K.Zd5)),
    (K.rB4, (K.rB2R0, K.rB2L1, K.rBx)),
    (K.rB3, (K.rB2R1, K.rB2L0)),
    (K.rC4, (K.rCx0, K.rCy2R0, K.rCy2R1, K.rCy2L0, K.rCy2L1)),
):
    for _n in _names:
        GROUPS[_n] = _first


def group_of(name):
    if name in GROUPS:
        return GROUPS[name]
    for p in (K.Ay, K.rAy, K.rBz, K.rCz, K.DA, K.DB, K.DC, K.Cx, K.rA4):
        if name.startswith(p):
            return p
    return name


def copy_kernel(*refs):
    src, dst, sem = refs[0:6], refs[6:12], refs[12]
    copies = [pltpu.make_async_copy(src[i], dst[i], sem.at[i]) for i in range(6)]
    for d in copies:
        d.start()
    for d in copies:
        d.wait()


def on_device(gate_pre, up_pre, out_grad, master, moment_one, moment_two):
    V = pltpu.VMEM

    def in_hbm(a):
        return pltpu.with_memory_space_constraint(a, pltpu.HBM)

    nA, nB, nC = A[1], B[1], C[1]
    outs = pl.pallas_call(
        kernel,
        out_shape=(
            V((TOK, 512), BF),
            V((TOK, FF), BF),
            V((TOK, FF), BF),
            V((8, FF), F32),
            V((8, FF), F32),
            V((8, FF), F32),
        ),
        in_specs=[pl.BlockSpec(memory_space=pltpu.HBM)] * 6,
        out_specs=[pl.BlockSpec(memory_space=V)] * 6,
        scratch_shapes=[
            V((TOK, FF), BF), V((TOK, FF), BF), V((TOK, D), BF),
            V((8, FF), F32), V((8, FF), F32), V((8, FF), F32),
            V((NC, NY, NX, NZ, 16, HALF), BF),
            V((NY, NX, NZ, 16, HALF), F32),
            V((2 * TOK, HALF), BF),
            V((TOK, HALF), BF),
            V((TOK, D), BF),
            V((4, 256, 2 * TOK), BF),
            V((8, HALF), F32),
            V((2, TOK, HALF), F32),
            V((2, TOK, HALF), F32),
            V((TOK, D), F32),
            V((16, HALF), F32),
            V((8, HALF), F32),
            V((TOK, 512), BF),
            V((TOK, 512), BF),
            V((2, 2, NX, 16, nA), BF), V((2, 2, NX, 16, nA), BF),
            V((2, 3, 2, 2, NX, 16, nA), BF), V((2, 3, 2, 2, NX, 16, nA), BF),
            V((NY, NX, 16, nA), BF), V((3, NX, 16, nA), BF),
            V((NX, 16, nA), BF), V((16, nA), BF),
            V((NX, NZ, 16, nB), BF), V((2, NZ, 16, nB), BF),
            V((2, NX, NZ, 16, nB), BF), V((2, NX, NZ, 16, nB), BF),
            V((NZ, 16, nB), BF), V((NZ, 16, nB), BF),
            V((NZ, 16, nB), BF), V((7, 16, nB), BF),
            V((NY, NZ, 16, nC), BF), V((NY, NZ, 16, nC), BF),
            V((NZ, 16, nC), BF), V((2, 4, 16, nC), BF),
            V((2, NZ, 16, nC), BF), V((2, NZ, 16, nC), BF),
            V((NZ, 16, nC), BF), V((7, 16, nC), BF),
            V((768, 16, 128), BF),
            pltpu.SemaphoreType.DMA((NSEND,)),
            pltpu.SemaphoreType.DMA((NRECV,)),
            pltpu.SemaphoreType.DMA((6,)),
        ],
        compiler_params=pltpu.CompilerParams(
            collective_id=0, has_side_effects=True, vmem_limit_bytes=56_000_000
        ),
    )(
        in_hbm(gate_pre.reshape(TOK, FF)),
        in_hbm(up_pre.reshape(TOK, FF)),
        in_hbm(out_grad.reshape(TOK, D)),
        in_hbm(master),
        in_hbm(moment_one),
        in_hbm(moment_two),
    )
    outs = pl.pallas_call(
        copy_kernel,
        out_shape=tuple(jax.ShapeDtypeStruct(o.shape, o.dtype) for o in outs),
        in_specs=[pl.BlockSpec(memory_space=V)] * 6,
        out_specs=[pl.BlockSpec(memory_space=pl.ANY)] * 6,
        scratch_shapes=[pltpu.SemaphoreType.DMA((6,))],
    )(*[pltpu.with_memory_space_constraint(o, V) for o in outs])
    lo, gg, ug, mn, m1, m2 = outs
    return (
        lo.reshape(2, 128, 512),
        gg.reshape(2, 128, FF),
        ug.reshape(2, 128, FF),
        mn,
        m1,
        m2,
    )


def solution(mesh):
    torus = Mesh(
        mesh.devices.reshape(NY, NX, NZ, NC, mesh.shape["rep"]),
        ("dp_0", "dp_1", "dp_2", "dp_3", "rep"),
    )
    return jax.shard_map(
        on_device,
        mesh=torus,
        in_specs=(
            P(None, DP, "rep"),
            P(None, DP, "rep"),
            P(None, DP, None),
            P(DP, "rep"),
            P(DP, "rep"),
            P(DP, "rep"),
        ),
        out_specs=(
            P(None, DP, "rep"),
            P(None, DP, "rep"),
            P(None, DP, "rep"),
            P(DP, "rep"),
            P(DP, "rep"),
            P(DP, "rep"),
        ),
        check_vma=False,
    )
```

```python
import math

import jax
import jax.numpy as jnp
from jax import lax
from jax.experimental import pallas as pl
from jax.experimental.pallas import tpu as pltpu
from jax.sharding import Mesh
from jax.sharding import PartitionSpec as P

DP = ("dp_0", "dp_1", "dp_2", "dp_3")
NY, NX, NZ, NC = 4, 2, 8, 2

first_power = 2.6561398887587544e-05
second_power = 0.005920529220333997

F32 = jnp.float32
BF = jnp.bfloat16
D = 1024
FF = 2816
HALF = 1408
TOK = 256
A = (0, 512)
B = (512, 512)
C = (1024, 384)
BC = (512, 896)


def cols(r):
    return pl.ds(r[0], r[1])


class Names:
    def __getattr__(self, word):
        return word


K = Names()

ORDER = (
    K.init, K.hidO_, K.hid2_, K.gp, K.gC0, K.RC1, K.A1, K.gB0, K.RB1, K.gA0, K.RA1, K.A2,
    K.RA2L0, K.BC1, K.RA3R1, K.A3_1L0, K.A3_1R1, K.RA2L1, K.RA3L0, K.A3_1R0, K.C2R, K.C2L, K.fc,
    K.A3_1L1, K.B2, K.RA3R0, K.RB2L, K.A3_2L0, K.A3_2L1, K.A3_2R1, K.RA4R0, K.A3_2R0, K.B3R,
    K.B3L, K.RC2, K.C3, K.A3_3L0, K.fo, K.A3_3L1, K.RA3L1, K.RB2R, K.RB3, K.RC2b, K.RC2c, K.C4,
    K.RA4R1, K.lo_cC, K.RC3R, K.RA4L0, K.A6, K.B4, K.lo_oC, K.lo_cA, K.RA4L1, K.lo_cB, K.lo_oA,
    K.RB4, K.lo_oB, K.losend, K.RC3L, K.hg_oB0, K.hg_oA0, K.RA5, K.RC4, K.hg_cA0, K.hg_cB0,
    K.hg_oC0, K.hg_cC0, K.RA6, K.RB5, K.RA7, K.RC5, K.fin_, K.lofin, K.adam,
)
ORDS = {
    K.init: (K.Zd7, K.Zd5, K.Zd6, K.Zd1, K.Ax, K.og, K.Zd3, K.Zd4, K.Zd2,),
    K.A1: (K.Ay3, K.Ay1, K.Ay2,),
    K.A2: (K.Az1L0, K.DA0, K.Az1R1, K.Az1L1, K.Az1R0,),
    K.A3_1R0: (K.DA1R0, K.Az2R0,),
    K.A3_1R1: (K.DA1R1, K.Az2R1,),
    K.A3_1L0: (K.DA1L0, K.Az2L0,),
    K.A3_1L1: (K.Az2L1, K.DA1L1,),
    K.A3_2R0: (K.Az3R0, K.DA2R0,),
    K.A3_2R1: (K.Az3R1, K.DA2R1,),
    K.A3_2L0: (K.DA2L0, K.Az3L0,),
    K.A3_2L1: (K.DA2L1, K.Az3L1,),
    K.A3_3L0: (K.Az4L0, K.DA3L0,),
    K.A3_3L1: (K.Az4L1, K.DA3L1,),
    K.BC1: (K.Bx, K.Cy1L, K.DC0, K.Cx0, K.DB0, K.By1Lx, K.Cy1R, K.By1Rx,),
    K.B2: (K.By1Ro, K.DB1, K.By1Lo,),
    K.B3R: (K.By2R, K.DB2,),
    K.B3L: (K.By2L, K.DB3,),
    K.C2R: (K.Cx3, K.DC3, K.Cy2R,),
    K.C2L: (K.DC1, K.Cy2L, K.Cx1,),
    K.C3: (K.Cx2, K.DC2,),
    K.RC1: (K.rCx0, K.rCx2, K.rCx1, K.rCx3,),
    K.RB1: (K.rB1L, K.rB2R1, K.rB2L1, K.rB1R,),
    K.RA1: (K.rA1L0, K.rA2R1, K.rA1L1, K.rA2R0,),
    K.RA5: (K.rAy2, K.rAy1, K.rAy3,),
    K.RB4: (K.rBz1, K.rBz5, K.rBz6, K.rBz7, K.rBz2, K.rBz3, K.rBz4,),
    K.RC2: (K.rCy1R, K.rCy1L,),
    K.RC4: (K.rCz7, K.rCz6, K.rCz4, K.rCz3, K.rCz1, K.rCz2, K.rCz5,),
}
HORDER = (K.C, K.B, K.A)


def kernel(
    gate_hbm, up_hbm, og_hbm, master_hbm, one_hbm, two_hbm,
    out_ref, gg_ref, ug_ref, master_out, one_out, two_out,
    gate_ref, up_ref, og_ref, master_ref, one_ref, two_ref,
    W, G, hid2, hidO, ogP, ogT, mP, fg, fu, acc, fin, finP, lo_s, lo_r,
    sa1, ra1, sa2, ra2, sa3, ra3, sa4, ra4,
    sb1, rb1, sb2, rb2, sb3, rb3, sb4, rb4,
    sc1, rc1, sc2, rc2, sc3, rc3, sc4, rc4,
    space, ssem, rsem, lsem,
):
    y = lax.axis_index(K.dp_0)
    x = lax.axis_index(K.dp_1)
    z = lax.axis_index(K.dp_2)
    c = lax.axis_index(K.dp_3)
    r = lax.axis_index(K.rep)
    oc = 1 - c
    ox = 1 - x

    def dy(o):
        return {K.dp_0: lax.rem(y + (o % NY), NY)}

    def dz(o):
        return {K.dp_2: lax.rem(z + (o % NZ), NZ)}

    def zz(o):
        return lax.rem(z + (o % NZ), NZ)

    def yy(o):
        return lax.rem(y + (o % NY), NY)

    dx = {K.dp_1: ox}
    dc = {K.dp_3: oc}
    dr = {K.rep: 1 - r}
    allr = slice(None)

    peers = [dc, dx, dr] + [dy(o) for o in range(1, NY)] + [dz(o) for o in range(1, NZ)]
    bar = pltpu.get_barrier_semaphore()
    for p in peers:
        pl.semaphore_signal(bar, inc=1, device_id=p, device_id_type=pl.DeviceIdType.MESH)

    loc = {}

    def local(name, src, dst):
        d = pltpu.make_async_copy(src, dst, lsem.at[len(loc)])
        d.start()
        loc[name] = d

    local(K.master, master_hbm, master_ref)
    local(K.og, og_hbm, og_ref)
    local(K.gate, gate_hbm, gate_ref)
    local(K.up, up_hbm, up_ref)
    local(K.one, one_hbm, one_ref)
    local(K.two, two_hbm, two_ref)

    slots, sent, arriving = {}, {}, {}

    def size(ref):
        return math.prod(ref.shape) * ref.dtype.itemsize

    def rc(name, src, dst, dev):
        group = group_of(name)
        k = slots.setdefault(group, len(slots))
        sent.setdefault(size(src), 0)
        return pltpu.make_async_remote_copy(
            src_ref=src, dst_ref=dst, send_sem=ssem.at[list(sent).index(size(src))],
            recv_sem=rsem.at[k], device_id=dev, device_id_type=pl.DeviceIdType.MESH,
        )

    def tiles(total):
        return space.at[pl.ds(0, total // 4096)]

    def recv_all(group):
        n = arriving[group]
        with jax.named_scope(K.wait_ + group):
            rc(group, tiles(n), tiles(n), dc).wait_recv()

    def sends(step, items):
        names = ORDS.get(step, tuple(i[0] for i in items))
        table = {i[0]: i for i in items}
        for n in names:
            table[n]
        for name in list(names) + [n for n in table if n not in names]:
            _, src, dst, dev = table[name]
            rc(name, src, dst, dev).start()
            sent[size(src)] += 1
            arriving[group_of(name)] = arriving.get(group_of(name), 0) + size(dst)

    def recv(name, dst, dev):
        with jax.named_scope(K.wait_ + name):
            rc(name, dst, dst, dev).wait_recv()

    def hidden_rows(half, out, cr):
        cs = pl.ds(pl.multiple_of(half * HALF + cr[0], 128), cr[1])

        def body(i, _):
            rows = pl.ds(pl.multiple_of(i * 32, 32), 32)
            g = gate_ref[rows, cs].astype(F32)
            u = up_ref[rows, cs].astype(F32)
            s = jax.nn.sigmoid(g)
            out[rows, cols(cr)] = (g * s * u).astype(BF)
            return 0

        lax.fori_loop(0, TOK // 32, body, 0)

    def factor_rows(half):
        cs = pl.ds(pl.multiple_of(half * HALF, 128), HALF)

        def body(i, _):
            rows = pl.ds(pl.multiple_of(i * 16, 16), 16)
            g = gate_ref[rows, cs].astype(F32)
            u = up_ref[rows, cs].astype(F32)
            s = jax.nn.sigmoid(g)
            fg[half, rows, :] = u * s * (1.0 + g * (1.0 - s))
            fu[half, rows, :] = g * s
            return 0

        lax.fori_loop(0, TOK // 16, body, 0)

    def Wb(*idx):
        return W.at[(c,) + idx]

    def same(name, ref, dev):
        return (name, ref, ref, dev)

    ranges = {K.A: A, K.B: B, K.C: C}
    S = {}

    def step(f):
        S[f.__name__] = f
        return f

    @step
    def init():
        sends(K.i0, [(K.m, master_ref.at[:, pl.ds(pl.multiple_of(oc * HALF, 128), HALF)], mP, dc)])
        recv(K.m, mP, dc)
        mine = master_ref[:, pl.ds(pl.multiple_of(c * HALF, 128), HALF)]
        theirs = mP[...]
        first_core = c == 0
        W[c, y, x, z] = jnp.concatenate(
            [jnp.where(first_core, mine, theirs), jnp.where(first_core, theirs, mine)], axis=0
        ).astype(BF)
        loc[K.og].wait()
        items = [
            (K.og, og_ref, ogP, dc),
            same(K.Ax, Wb(y, x, z, allr, cols(A)), dx),
        ]
        for o in (4, 3, 5, 2, 6, 1, 7):
            items.append(same(f"Zd{o}", Wb(y, x, z, allr, cols(BC)), dz(o)))
        sends(K.init, items)

    @step
    def hidO_():
        loc[K.gate].wait()
        loc[K.up].wait()
        for k in HORDER:
            cr = ranges[k]
            hidden_rows(oc, hidO, cr)
            sends(K.h, [(K.h + k, hidO.at[:, cols(cr)], hid2.at[pl.ds(TOK, TOK), cols(cr)], dc)])

    @step
    def hid2_():
        for k in HORDER:
            hidden_rows(c, hid2, ranges[k])
        for b in range(4):
            ogT[b, :, 0:TOK] = og_ref[:, b * 256 : (b + 1) * 256].T

    S[K.fo] = lambda: factor_rows(oc)
    S[K.fc] = lambda: factor_rows(c)

    @step
    def A1():
        recv(K.Ax, Wb(y, ox, z, allr, cols(A)), dx)
        ref = Wb(y, allr, z, allr, cols(A))
        sends(K.A1, [same(f"Ay{o}", ref, dy(o)) for o in (2, 1, 3)])

    def az(h, zi):
        return Wb(pl.ds(2 * h, 2), allr, zi, allr, cols(A))

    @step
    def A2():
        recv_all(K.Ay)
        sends(K.A2, [
            same(K.Az1L0, az(0, z), dz(-1)),
            same(K.Az1R0, az(0, z), dz(1)),
            same(K.Az1L1, az(1, z), dz(-1)),
            same(K.Az1R1, az(1, z), dz(1)),
            same(K.DA0, Wb(allr, allr, z, allr, cols(A)), dc),
        ])

    def a3(s, sd, h):
        sg = 1 if sd == K.R else -1
        ref = az(h, zz(-sg * s))
        nm = f"{s}{sd}{h}"

        def f():
            recv(K.Az + nm, ref, dz(-sg))
            sends(K.A3_ + nm, [same(f"Az{s + 1}{sd}{h}", ref, dz(sg)), same(K.DA + nm, ref, dc)])

        S[K.A3_ + nm] = f

    last_a = (("3R0", 0, -3), ("3R1", 1, -3), ("4L0", 0, 4), ("4L1", 1, 4))
    for s in (1, 2, 3):
        for h in (0, 1):
            a3(s, K.L, h)
            if s < 3:
                a3(s, K.R, h)

    @step
    def A6():
        recv_all(K.Az9)
        sends(K.A6, [same(K.DA + nm, az(h, zz(o)), dc) for nm, h, o in last_a])

    def bref(yi, xi):
        return Wb(yi, xi, allr, allr, cols(B))

    def cref(yi, xi, zs=allr):
        return Wb(yi, xi, zs, allr, cols(C))

    @step
    def BC1():
        recv_all(K.Zd)
        b, cc = bref(y, x), cref(y, x)
        sends(K.BC1, [
            same(K.Bx, b, dx), same(K.By1Rx, b, dy(1)), same(K.By1Lx, b, dy(-1)),
            same(K.Cy1R, cc, dy(1)), same(K.Cy1L, cc, dy(-1)), same(K.Cx0, cc, dx),
            same(K.DB0, b, dc), same(K.DC0, cc, dc),
        ])

    @step
    def B2():
        b = bref(y, ox)
        recv(K.Bx, b, dx)
        sends(K.B2, [same(K.By1Ro, b, dy(1)), same(K.By1Lo, b, dy(-1)), same(K.DB1, b, dc)])

    @step
    def B3R():
        b = bref(yy(-1), x)
        recv(K.By1Rx, b, dy(-1))
        sends(K.B3R, [same(K.By2R, b, dy(1)), same(K.DB2, b, dc)])

    @step
    def B3L():
        b = bref(yy(1), ox)
        recv(K.By1Lo, b, dy(1))
        sends(K.B3L, [same(K.By2L, b, dy(-1)), same(K.DB3, b, dc)])

    last_b = ((K.By2R, 2, x, -1), (K.By2L, 2, ox, 1), (K.By1Ro, -1, ox, -1), (K.By1Lx, 1, x, 1))

    @step
    def B4():
        recv_all(K.By9)
        sends(K.B4, [same(K.D + nm, bref(yy(o), xi), dc) for nm, o, xi, d in last_b])

    lo4, hi4 = pl.ds(0, 4), pl.ds(4, 4)

    @step
    def C2R():
        recv(K.Cy1R, cref(yy(-1), x), dy(-1))
        sends(K.C2R, [
            same(K.Cy2R, cref(yy(-1), x, lo4), dy(1)),
            same(K.Cx3, cref(yy(-1), x), dx), same(K.DC3, cref(yy(-1), x), dc),
        ])

    @step
    def C2L():
        recv(K.Cy1L, cref(yy(1), x), dy(1))
        sends(K.C2L, [
            same(K.Cy2L, cref(yy(1), x, hi4), dy(-1)),
            same(K.Cx1, cref(yy(1), x), dx), same(K.DC1, cref(yy(1), x), dc),
        ])

    @step
    def C3():
        recv_all(K.Cy2)
        sends(K.C3, [same(K.Cx2, cref(yy(2), x), dx), same(K.DC2, cref(yy(2), x), dc)])

    @step
    def C4():
        recv_all(K.Cx)
        sends(K.C4, [same(f"DCx{o}", cref(yy(o), ox), dc) for o in (0, 1, 3, 2)])

    @step
    def gp():
        recv(K.og, ogP, dc)
        for b in range(4):
            ogT[b, :, TOK : 2 * TOK] = ogP[:, b * 256 : (b + 1) * 256].T

    def grads(k, j):
        cr = ranges[k]
        if j == 0:
            recv(K.h + k, hid2.at[pl.ds(TOK, TOK), cols(cr)], dc)
        c0 = cr[0] + 512 * j
        n = min(512, cr[1] - 512 * j)
        p = jnp.dot(
            ogT[...].reshape(D, 2 * TOK), hid2[:, pl.ds(c0, n)], preferred_element_type=F32
        )
        G[:, :, :, :, pl.ds(c0, n)] = p.reshape(NY, NX, NZ, 16, n)

    for k in K.ABC:
        for j in range(-(-ranges[k][1] // 512)):
            S[f"g{k}{j}"] = lambda k=k, j=j: grads(k, j)

    def ga(h, zi):
        return G[2 * h : 2 * h + 2, :, zi, :, cols(A)]

    @step
    def RA1():
        for h in (0, 1):
            sa1[h] = ga(h, zz(4)).astype(BF)
            sa2[0, 0, h] = ga(h, zz(3)).astype(BF)
        sends(K.RA1, [
            (K.rA1L0, sa1.at[0], ra1.at[0], dz(-1)),
            (K.rA1L1, sa1.at[1], ra1.at[1], dz(-1)),
            (K.rA2R0, sa2.at[0, 0, 0], ra2.at[0, 0, 0], dz(1)),
            (K.rA2R1, sa2.at[0, 0, 1], ra2.at[0, 0, 1], dz(1)),
        ])

    def ra(s, sd, h):
        sg = 1 if sd == K.R else -1
        side = 0 if sd == K.R else 1

        def f():
            buf = ra1.at[h] if s == 2 else ra2.at[side, s - 3, h]
            recv(f"rA{s - 1}{sd}{h}", buf, dz(-sg))
            sa2[side, s - 2, h] = (ga(h, zz(sg * (5 - s))) + buf[...].astype(F32)).astype(BF)
            sends(K.RA, [(f"rA{s}{sd}{h}", sa2.at[side, s - 2, h], ra2.at[side, s - 2, h], dz(sg))])

        S[f"RA{s}{sd}{h}"] = f

    for sd in K.RL:
        for h in (0, 1):
            for s in range(2 if sd == K.L else 3, 5):
                ra(s, sd, h)

    @step
    def RA5():
        recv_all(K.rA4)
        for h in (0, 1):
            t = ga(h, z) + ra2[0, 2, h].astype(F32) + ra2[1, 2, h].astype(F32)
            G[2 * h : 2 * h + 2, :, z, :, cols(A)] = t
            sa3[2 * h : 2 * h + 2] = t.astype(BF)
        sends(K.RA5, [(f"rAy{o}", sa3.at[yy(o)], ra3.at[o - 1], dy(o)) for o in (2, 1, 3)])

    @step
    def RA6():
        recv_all(K.rAy)
        t = G[y, :, z, :, cols(A)]
        for o in (1, 2, 3):
            t = t + ra3[o - 1].astype(F32)
        G[y, :, z, :, cols(A)] = t
        sa4[...] = t.astype(BF)
        sends(K.RA6, [(K.rAx, sa4.at[ox], ra4, dx)])

    @step
    def RA7():
        recv(K.rAx, ra4, dx)
        fin[:, cols(A)] = G[y, x, z, :, cols(A)] + ra4[...].astype(F32)

    def gb(yi, xi):
        return G[yi, xi, :, :, cols(B)]

    @step
    def RB1():
        sb1[0] = gb(yy(2), x).astype(BF)
        sb1[1] = gb(yy(2), ox).astype(BF)
        sb2[0, 1] = gb(yy(1), ox).astype(BF)
        sb2[1, 0] = gb(yy(-1), x).astype(BF)
        sends(K.RB1, [
            (K.rB1R, sb1.at[0], rb1.at[0], dy(1)), (K.rB1L, sb1.at[1], rb1.at[1], dy(-1)),
            (K.rB2R1, sb2.at[0, 1], rb2.at[0, 1], dy(1)),
            (K.rB2L1, sb2.at[1, 0], rb2.at[1, 0], dy(-1)),
        ])

    @step
    def RB2R():
        recv(K.rB1R, rb1.at[0], dy(-1))
        sb2[0, 0] = (gb(yy(1), x) + rb1[0].astype(F32)).astype(BF)
        sends(K.RB2R, [(K.rB2R0, sb2.at[0, 0], rb2.at[0, 0], dy(1))])

    @step
    def RB2L():
        recv(K.rB1L, rb1.at[1], dy(1))
        sb2[1, 1] = (gb(yy(-1), ox) + rb1[1].astype(F32)).astype(BF)
        sends(K.RB2L, [(K.rB2L0, sb2.at[1, 1], rb2.at[1, 1], dy(-1))])

    @step
    def RB3():
        recv_all(K.rB3)
        sb3[...] = (gb(y, ox) + rb2[0, 1].astype(F32) + rb2[1, 1].astype(F32)).astype(BF)
        sends(K.RB3, [(K.rBx, sb3, rb3, dx)])

    @step
    def RB4():
        recv_all(K.rB4)
        t = gb(y, x) + rb2[0, 0].astype(F32) + rb2[1, 0].astype(F32) + rb3[...].astype(F32)
        G[y, x, :, :, cols(B)] = t
        sb4[...] = t.astype(BF)
        sends(K.RB4, [(f"rBz{o}", sb4.at[zz(o)], rb4.at[o - 1], dz(o)) for o in (4, 3, 5, 2, 6, 1, 7)])

    @step
    def RB5():
        t = G[y, x, z, :, cols(B)]
        recv_all(K.rBz)
        for o in range(1, NZ):
            t = t + rb4[o - 1].astype(F32)
        fin[:, cols(B)] = t

    def gc(yi, xi, zs=allr):
        return G[yi, xi, zs, :, cols(C)]

    @step
    def RC1():
        items = []
        for o in (2, 1, 3, 0):
            sc1[o] = gc(yy(o), ox).astype(BF)
            items.append((f"rCx{o}", sc1.at[o], rc1.at[o], dx))
        sends(K.RC1, items)

    @step
    def RC2():
        recv(K.rCx2, rc1.at[2], dx)
        sc2[...] = (gc(yy(2), x) + rc1[2].astype(F32)).astype(BF)
        sends(K.RC2, [
            (K.rCy1R, sc2.at[lo4], rc2.at[0], dy(1)), (K.rCy1L, sc2.at[hi4], rc2.at[1], dy(-1)),
        ])

    @step
    def RC2b():
        recv(K.rCx1, rc1.at[1], dx)
        t = gc(yy(1), x) + rc1[1].astype(F32)
        G[yy(1), x, :, :, cols(C)] = t
        sc3[0, 4:8] = t[4:8].astype(BF)
        sends(K.RC2b, [(K.rCy2R1, sc3.at[0, hi4], rc3.at[0, hi4], dy(1))])

    @step
    def RC2c():
        recv(K.rCx3, rc1.at[3], dx)
        t = gc(yy(3), x) + rc1[3].astype(F32)
        G[yy(3), x, :, :, cols(C)] = t
        sc3[1, 0:4] = t[0:4].astype(BF)
        sends(K.RC2c, [(K.rCy2L1, sc3.at[1, lo4], rc3.at[1, lo4], dy(-1))])

    @step
    def RC3R():
        recv(K.rCy1R, rc2.at[0], dy(-1))
        sc3[0, 0:4] = (gc(yy(1), x, slice(0, 4)) + rc2[0].astype(F32)).astype(BF)
        sends(K.RC3R, [(K.rCy2R0, sc3.at[0, lo4], rc3.at[0, lo4], dy(1))])

    @step
    def RC3L():
        recv(K.rCy1L, rc2.at[1], dy(1))
        sc3[1, 4:8] = (gc(yy(3), x, slice(4, 8)) + rc2[1].astype(F32)).astype(BF)
        sends(K.RC3L, [(K.rCy2L0, sc3.at[1, hi4], rc3.at[1, hi4], dy(-1))])

    @step
    def RC4():
        recv_all(K.rC4)
        t = gc(y, x) + rc1[0].astype(F32) + rc3[0].astype(F32) + rc3[1].astype(F32)
        G[y, x, :, :, cols(C)] = t
        sc4[...] = t.astype(BF)
        sends(K.RC4, [(f"rCz{o}", sc4.at[zz(o)], rc4.at[o - 1], dz(o)) for o in (4, 3, 5, 2, 6, 1, 7)])

    @step
    def RC5():
        t = G[y, x, z, :, cols(C)]
        recv_all(K.rCz)
        for o in range(1, NZ):
            t = t + rc4[o - 1].astype(F32)
        fin[:, cols(C)] = t

    have = set()
    started = []

    def w_of(side, k, c0, n):
        if side == K.o and k not in have:
            have.add(k)
            recv_all(K.D + k)
        half = c if side == K.c else oc
        return W[half, :, :, :, :, pl.ds(c0, n)].reshape(D, n)

    def lo(side, k):
        w = w_of(side, k, *ranges[k])
        h = (hid2 if side == K.c else hidO)[0:TOK, cols(ranges[k])]
        part = lax.dot_general(h, w, (((1,), (1,)), ((), ())), preferred_element_type=F32)
        if started:
            acc[...] += part
        else:
            acc[...] = part
        started.append(1)

    def hgrad(side, k, j):
        c0 = ranges[k][0] + 512 * j
        n = min(512, ranges[k][1] - 512 * j)
        half = c if side == K.c else oc
        cs = pl.ds(pl.multiple_of(half * HALF + c0, 128), n)
        h = jnp.dot(og_ref[...], w_of(side, k, c0, n), preferred_element_type=F32)
        gg_ref[:, cs] = (h * fg[half, :, pl.ds(c0, n)]).astype(BF)
        ug_ref[:, cs] = (h * fu[half, :, pl.ds(c0, n)]).astype(BF)

    for side in K.co:
        for k in K.ABC:
            S[f"lo_{side}{k}"] = lambda side=side, k=k: lo(side, k)
            for j in range(-(-ranges[k][1] // 512)):
                S[f"hg_{side}{k}{j}"] = lambda side=side, k=k, j=j: hgrad(side, k, j)

    @step
    def losend():
        lo_s[...] = acc[:, pl.ds(pl.multiple_of((1 - r) * 512, 128), 512)].astype(BF)
        sends(K.losend, [(K.lo, lo_s, lo_r, dr)])

    @step
    def lofin():
        recv(K.lo, lo_r, dr)
        out_ref[...] = (
            acc[:, pl.ds(pl.multiple_of(r * 512, 128), 512)] + lo_r[...].astype(F32)
        ).astype(BF)

    def update(half, g):
        cs = pl.ds(pl.multiple_of(half * HALF, 128), HALF)
        g = g / jnp.float32(32768)
        m = master_ref[:, cs]
        first = 0.9 * one_ref[:, cs] + 0.1 * g
        second = 0.95 * two_ref[:, cs] + 0.05 * g * g
        upd = first / (1.0 - first_power) / (jnp.sqrt(second / (1.0 - second_power)) + 1e-08)
        master_out[:, cs] = m - 0.003 * (upd + 0.1 * m)
        one_out[:, cs] = first
        two_out[:, cs] = second

    @step
    def fin_():
        loc[K.one].wait()
        loc[K.two].wait()
        sends(K.fin, [(K.fin, fin.at[pl.ds(pl.multiple_of(oc * 8, 8), 8)], finP, dc)])
        update(c, fin[pl.ds(pl.multiple_of(c * 8, 8), 8), :])

    @step
    def adam():
        recv(K.fin, finP, dc)
        update(oc, finP[...])

    loc[K.master].wait()
    with jax.named_scope(K.barrier):
        pl.semaphore_wait(bar, len(peers))
    for n in ORDER:
        with jax.named_scope(n):
            S.pop(n)()
    assert not S, S.keys()
    with jax.named_scope(K.sends_done):
        for n, many in sent.items():
            if many:
                pltpu.make_async_remote_copy(
                    src_ref=tiles(n * many), dst_ref=tiles(n * many),
                    send_sem=ssem.at[list(sent).index(n)], recv_sem=rsem.at[0],
                    device_id=dc, device_id_type=pl.DeviceIdType.MESH,
                ).wait_send()
    assert len(slots) <= NRECV and len(sent) <= NSEND, (len(slots), len(sent))


NRECV, NSEND = 58, 20

GROUPS = {}
for _first, _names in (
    (K.Az9, (K.Az3R0, K.Az3R1, K.Az4L0, K.Az4L1)),
    (K.By9, (K.By2R, K.By2L, K.By1Ro, K.By1Lx)),
    (K.rB4, (K.rB2R0, K.rB2L1, K.rBx)),
    (K.rB3, (K.rB2R1, K.rB2L0)),
    (K.rC4, (K.rCx0, K.rCy2R0, K.rCy2R1, K.rCy2L0, K.rCy2L1)),
    (K.Cy2, (K.Cy2R, K.Cy2L)),
):
    for _n in _names:
        GROUPS[_n] = _first


def group_of(name):
    if name in GROUPS:
        return GROUPS[name]
    for p in (K.Zd, K.Ay, K.rAy, K.rBz, K.rCz, K.DA, K.DB, K.DC, K.Cx, K.rA4):
        if name.startswith(p):
            return p
    return name


def copy_kernel(*refs):
    src, dst, sem = refs[0:6], refs[6:12], refs[12]
    copies = [pltpu.make_async_copy(src[i], dst[i], sem.at[i]) for i in range(6)]
    for d in copies:
        d.start()
    for d in copies:
        d.wait()


def on_device(gate_pre, up_pre, out_grad, master, moment_one, moment_two):
    V = pltpu.VMEM

    def in_hbm(a):
        return pltpu.with_memory_space_constraint(a, pltpu.HBM)

    nA, nB, nC = A[1], B[1], C[1]
    outs = pl.pallas_call(
        kernel,
        out_shape=(
            V((TOK, 512), BF),
            V((TOK, FF), BF),
            V((TOK, FF), BF),
            V((8, FF), F32),
            V((8, FF), F32),
            V((8, FF), F32),
        ),
        in_specs=[pl.BlockSpec(memory_space=pltpu.HBM)] * 6,
        out_specs=[pl.BlockSpec(memory_space=V)] * 6,
        scratch_shapes=[
            V((TOK, FF), BF), V((TOK, FF), BF), V((TOK, D), BF),
            V((8, FF), F32), V((8, FF), F32), V((8, FF), F32),
            V((NC, NY, NX, NZ, 16, HALF), BF),
            V((NY, NX, NZ, 16, HALF), F32),
            V((2 * TOK, HALF), BF),
            V((TOK, HALF), BF),
            V((TOK, D), BF),
            V((4, 256, 2 * TOK), BF),
            V((8, HALF), F32),
            V((2, TOK, HALF), F32),
            V((2, TOK, HALF), F32),
            V((TOK, D), F32),
            V((16, HALF), F32),
            V((8, HALF), F32),
            V((TOK, 512), BF),
            V((TOK, 512), BF),
            V((2, 2, NX, 16, nA), BF), V((2, 2, NX, 16, nA), BF),
            V((2, 3, 2, 2, NX, 16, nA), BF), V((2, 3, 2, 2, NX, 16, nA), BF),
            V((NY, NX, 16, nA), BF), V((3, NX, 16, nA), BF),
            V((NX, 16, nA), BF), V((16, nA), BF),
            V((NX, NZ, 16, nB), BF), V((2, NZ, 16, nB), BF),
            V((2, NX, NZ, 16, nB), BF), V((2, NX, NZ, 16, nB), BF),
            V((NZ, 16, nB), BF), V((NZ, 16, nB), BF),
            V((NZ, 16, nB), BF), V((7, 16, nB), BF),
            V((NY, NZ, 16, nC), BF), V((NY, NZ, 16, nC), BF),
            V((NZ, 16, nC), BF), V((2, 4, 16, nC), BF),
            V((2, NZ, 16, nC), BF), V((2, NZ, 16, nC), BF),
            V((NZ, 16, nC), BF), V((7, 16, nC), BF),
            V((768, 16, 128), BF),
            pltpu.SemaphoreType.DMA((NSEND,)),
            pltpu.SemaphoreType.DMA((NRECV,)),
            pltpu.SemaphoreType.DMA((6,)),
        ],
        compiler_params=pltpu.CompilerParams(
            collective_id=0, has_side_effects=True, vmem_limit_bytes=56_000_000
        ),
    )(
        in_hbm(gate_pre.reshape(TOK, FF)),
        in_hbm(up_pre.reshape(TOK, FF)),
        in_hbm(out_grad.reshape(TOK, D)),
        in_hbm(master),
        in_hbm(moment_one),
        in_hbm(moment_two),
    )
    outs = pl.pallas_call(
        copy_kernel,
        out_shape=tuple(jax.ShapeDtypeStruct(o.shape, o.dtype) for o in outs),
        in_specs=[pl.BlockSpec(memory_space=V)] * 6,
        out_specs=[pl.BlockSpec(memory_space=pl.ANY)] * 6,
        scratch_shapes=[pltpu.SemaphoreType.DMA((6,))],
    )(*[pltpu.with_memory_space_constraint(o, V) for o in outs])
    lo, gg, ug, mn, m1, m2 = outs
    return (
        lo.reshape(2, 128, 512),
        gg.reshape(2, 128, FF),
        ug.reshape(2, 128, FF),
        mn,
        m1,
        m2,
    )


def solution(mesh):
    torus = Mesh(
        mesh.devices.reshape(NY, NX, NZ, NC, mesh.shape["rep"]),
        ("dp_0", "dp_1", "dp_2", "dp_3", "rep"),
    )
    return jax.shard_map(
        on_device,
        mesh=torus,
        in_specs=(
            P(None, DP, "rep"),
            P(None, DP, "rep"),
            P(None, DP, None),
            P(DP, "rep"),
            P(DP, "rep"),
            P(DP, "rep"),
        ),
        out_specs=(
            P(None, DP, "rep"),
            P(None, DP, "rep"),
            P(None, DP, "rep"),
            P(DP, "rep"),
            P(DP, "rep"),
            P(DP, "rep"),
        ),
        check_vma=False,
    )
```
